16 devices in a mesh: rep: 1, r: 2 (over z), s: 8 (over x, y, core).
Axes of the slice: x: 2, y: 2, z: 2, core: 2. Of those that a mesh axis runs over, the one named last changes fastest.
Arguments:
- x: bfloat16 [16, 2048, 1280], P(('rep', 'r', 's'))
- dy: bfloat16 [16, 2048, 1280], P(('rep', 'r', 's'))
- w_gate: bfloat16 [2, 1280, 4096], P(None, 's')
- w_up: bfloat16 [2, 1280, 4096], P(None, 's')
- w_down: bfloat16 [2, 4096, 1280], P(None, 's')
Outputs:
- output 1: bfloat16 [16, 2048, 1280], P(('rep', 'r', 's'))
- output 2: bfloat16 [2, 1280, 4096], P('rep', 's')
- output 3: bfloat16 [2, 1280, 4096], P('rep', 's')
- output 4: bfloat16 [2, 4096, 1280], P('rep', 's')
All inputs are finite; a program needn't handle non-finite values.
Results may differ from the reference program's by a relative error of at most 0.018.
Values are sent between devices in bfloat16 or wider.
A program may use at most 2 GiB of HBM per device.

```python
import jax
import jax.numpy as jnp
from jax import lax

SEQUENCES = 16
TOKENS = 2048
D = 1280
FF = 4096
LAYERS = 2
NAMES = ("w_gate", "w_up", "w_down")
SHAPES = {"w_gate": (LAYERS, D, FF), "w_up": (LAYERS, D, FF), "w_down": (LAYERS, FF, D)}


def bump(key, n, height):
    away = (jnp.arange(n, dtype=jnp.int32) - jax.random.randint(key, (), 0, n, jnp.int32)) % n
    return jnp.where(away < n // 8, height, 1.0)


def together(key, own, strength):
    shared = jax.random.normal(key, own.shape[1:], jnp.float32)
    return (own + strength * shared) * lax.rsqrt(1 + strength * strength)


def setup_inputs(seed: int = 0, part: int = 0) -> dict:
    kx, kdy, ka, kb, kz, kf, kh, kl, *kw = jax.random.split(jax.random.key(seed), 8 + len(NAMES))
    kx, kdy, ka, kb = (jax.random.fold_in(k, part) for k in (kx, kdy, ka, kb))
    shape = (SEQUENCES, TOKENS, D)
    much_x, much_dy = jax.random.uniform(kz, (2,), jnp.float32, 0.0, 1.0)
    layers = 2.0 ** jax.random.uniform(kl, (LAYERS, 1, 1), jnp.float32, -1.0, 1.0)
    x = together(ka, jax.random.normal(kx, shape, jnp.float32), much_x) * bump(kf, D, 4.0)
    dy = together(kb, jax.random.normal(kdy, shape, jnp.float32), much_dy)
    drawn = {"x": x.astype(jnp.bfloat16), "dy": (dy * (SEQUENCES * TOKENS) ** -0.5).astype(jnp.bfloat16)}
    for key, name in zip(kw, NAMES, strict=True):
        w = jax.random.normal(key, SHAPES[name], jnp.float32) * SHAPES[name][1] ** -0.5
        drawn[name] = (w * {"w_gate": 1.0, "w_up": bump(kh, FF, 4.0), "w_down": layers}[name]).astype(jnp.bfloat16)
    return drawn


def matmul(a, w):
    return jnp.dot(a, w, preferred_element_type=jnp.float32).astype(jnp.bfloat16)


def normed(h):
    wide = h.astype(jnp.float32)
    scale = lax.rsqrt(jnp.mean(wide**2, -1, keepdims=True) + 1e-6)
    return (wide * scale).astype(jnp.bfloat16)


def layer(h, w):
    a = normed(h)
    gate = jnp.dot(a, w["w_gate"], preferred_element_type=jnp.float32)
    up = jnp.dot(a, w["w_up"], preferred_element_type=jnp.float32)
    return h + matmul((jax.nn.silu(gate) * up).astype(jnp.bfloat16), w["w_down"])


def stack(weights, h):
    return lax.scan(lambda h, w: (layer(h, w), None), h, weights)[0]


def reference(x, dy, w_gate, w_up, w_down):
    weights = dict(zip(NAMES, (w_gate, w_up, w_down), strict=True))

    def take(so_far, sequence):
        h, by_y = sequence
        _, back = jax.vjp(stack, weights, h)
        by_weights, by_h = back(by_y)
        return jax.tree.map(lambda total, term: total + term.astype(jnp.float32), so_far, by_weights), by_h

    none_yet = {name: jnp.zeros(w.shape, jnp.float32) for name, w in weights.items()}
    by_weights, by_x = lax.scan(take, none_yet, (x, dy))
    return (by_x, *(by_weights[name].astype(jnp.bfloat16) for name in NAMES))
```

```python
import functools

import jax
import jax.numpy as jnp
from jax import lax
from jax.experimental import pallas as pl
from jax.experimental.pallas import tpu as pltpu
from jax.sharding import PartitionSpec as P

MESH = pl.DeviceIdType.MESH
BF, F32 = jnp.bfloat16, jnp.float32
NB = 8
LEAD = 8
TWO, THREE, FOUR = 2, 3, 4
STEPS = 11
LAST = TWO * STEPS


def nn(a, b):
    return lax.dot_general(a, b, (((1,), (0,)), ((), ())), preferred_element_type=F32)


def nt(a, b):
    return lax.dot_general(a, b, (((1,), (1,)), ((), ())), preferred_element_type=F32)


def rows_of(start, size):
    return pl.ds(start if isinstance(start, int) else pl.multiple_of(start, 16), size)


def cols_of(start, size):
    return pl.ds(start if isinstance(start, int) else pl.multiple_of(start, 128), size)


def odd(i):
    return lax.rem(i, TWO)


def copy(src, dst, sem):
    return pltpu.make_async_copy(src, dst, sem)


def done(ref, sem):
    pltpu.make_async_copy(ref, ref, sem).wait()


def both(a, b):
    return jnp.logical_and(a, b)


def either(a, b):
    return jnp.logical_or(a, b)


def vmem(*shape, dtype=BF):
    return pltpu.VMEM(shape, dtype)


def dmas(*shape):
    return pltpu.SemaphoreType.DMA(shape)


class Sizes:
    def __init__(self, T, D, F):
        self.T, self.D, self.F = T, D, F
        self.RB, self.FB, self.HB = D // NB, F // NB, D // TWO
        self.FC = self.FB
        self.UC, self.UD = self.FC // TWO, self.FB // FOUR
        self.NG, self.ND = F // self.UC, FOUR
        self.TM, self.TS = T // FOUR, T // NB
        self.PR = TWO * self.RB
        self.UNITS = TWO * (self.NG + self.ND)


class Here:
    def __init__(self):
        self.r, self.s = lax.axis_index("r"), lax.axis_index("s")
        rep, r, s = lax.axis_index("rep"), self.r, self.s
        self.c = c = odd(s)
        y, x = odd(lax.div(s, TWO)), lax.div(s, FOUR)
        self.xn, self.yn, partner = s + FOUR - NB * x, s + TWO - FOUR * y, s + 1 - TWO * c
        self.far = self.xn + self.yn - s
        self.over = self.yn + c * (self.xn - self.yn)
        self.u, self.v = x + c * (y - x), y + c * (x - y)
        n1 = self.xn + c * (self.yn - self.xn)
        n2 = self.xn + self.yn - n1
        self.to_p, self.to_x, self.to_y, self.to_z = (rep, r, partner), (rep, r, self.xn), (rep, r, self.yn), (rep, 1 - r, s)
        self.to_1, self.to_2 = (rep, r, n1), (rep, r, n2)
        self.z0, self.z1, self.c0, self.c1 = r == 0, r == 1, c == 0, c == 1

    def meet(self):
        barrier = pltpu.get_barrier_semaphore()
        for dev in (self.to_p, self.to_x, self.to_y, self.to_z):
            pl.semaphore_signal(barrier, inc=1, device_id=dev, device_id_type=MESH)
        pl.semaphore_wait(barrier, FOUR)


def remote(src, dst, ss, rs, dev):
    return pltpu.make_async_remote_copy(src, dst, ss, rs, device_id=dev, device_id_type=MESH)


def normed(h):
    wide = h.astype(F32)
    scale = lax.rsqrt(jnp.mean(wide * wide, -1, keepdims=True) + 1e-6)
    return (wide * scale).astype(BF)


def gather_of(z, me, k):
    segments = (
        (0, z.NG, "gu", 0),
        (z.NG, z.ND, "d", 0),
        (z.NG + z.ND, z.NG, "gu", 1),
        (z.UNITS - z.ND, z.ND, "d", 1),
    )

    def held(kind, l, n, d):
        if kind == "gu":
            return [G.at[l, rows_of(d * z.RB, z.RB), cols_of(n * z.UC, z.UC)] for G in (k.GG, k.GU)]
        return [k.GD.at[l, rows_of(d * z.FB + n * z.UD, z.UD), :]]

    def mine(kind, l, n):
        if kind == "gu":
            return [w.at[l, :, cols_of(n * z.UC, z.UC)] for w in (k.wg, k.wu)]
        return [k.wd.at[l, rows_of(n * z.UD, z.UD), :]]

    def got(kind, l, n, sem):
        done(k.GG.at[l, pl.ds(0, n * z.PR), pl.ds(0, z.UC)] if kind == "gu" else k.GD.at[l, pl.ds(0, n * z.UD), :], sem)

    def push(srcs, dsts, ss, rs, i, dev):
        for a, b in zip(srcs, dsts, strict=True):
            remote(a, b, ss.at[i], rs.at[i], dev).start()

    def pass_on(ref, i):
        push(ref, ref, k.gsp, k.grp, i, me.to_p)

    def stage_own(kind, l, n, i):
        own, there = mine(kind, l, n), held(kind, l, n, me.s)

        @pl.when(either(me.z0, me.c0))
        def _():
            push(own, there, k.gsx, k.grx, i, me.to_x)

        @pl.when(either(me.z0, me.c1))
        def _():
            push(own, there, k.gsy, k.gry, i, me.to_y)

        push(own, there, k.gsp, k.grp, i, me.to_p)

    def stage_1(kind, l, n, i):
        hx, hy = held(kind, l, n, me.xn), held(kind, l, n, me.yn)

        @pl.when(either(me.z0, me.c0))
        def _():
            got(kind, l, 1, k.grx.at[i])

        @pl.when(either(me.z0, me.c1))
        def _():
            got(kind, l, 1, k.gry.at[i])

        @pl.when(me.z0)
        def _():
            on = held(kind, l, n, me.over)
            push(on, on, k.gsz, k.grz, i, me.to_z)
            pass_on(hx, i)
            pass_on(hy, i)

        @pl.when(both(me.z1, me.c0))
        def _():
            push(hx, hx, k.gsy, k.gry, i, me.to_y)
            pass_on(hx, i)

        @pl.when(both(me.z1, me.c1))
        def _():
            push(hy, hy, k.gsx, k.grx, i, me.to_x)
            pass_on(hy, i)

    def stage_2(kind, l, n, i):
        @pl.when(me.z1)
        def _():
            far, over = held(kind, l, n, me.far), held(kind, l, n, me.over)

            @pl.when(me.c0)
            def _():
                got(kind, l, 1, k.gry.at[i])

            @pl.when(me.c1)
            def _():
                got(kind, l, 1, k.grx.at[i])

            push(far, far, k.gsz, k.grz, i, me.to_z)
            pass_on(far, i)
            got(kind, l, 1, k.grz.at[i])
            pass_on(over, i)

    def stage_3(kind, l, n, i):
        @pl.when(me.z0)
        def _():
            got(kind, l, 1, k.grz.at[i])
            pass_on(held(kind, l, n, me.far), i)

    def stage(fn, i, low, high):
        for start, n, kind, l in segments:
            a, b = max(start, low), min(start + n, high)
            if a < b:

                @pl.when(both(i >= a, i < b))
                def _(kind=kind, l=l, start=start):
                    fn(kind, l, i - start, i)

    def tick(t, low, high, first=0, last=z.UNITS):
        t = jnp.asarray(t, jnp.int32)
        stage(stage_own, t + LEAD, low + LEAD, high + LEAD)
        for lag, fn in enumerate((stage_1, stage_2, stage_3)):
            stage(fn, t - lag, max(first, low - lag), min(last, high - lag))

    def ready(l, kind, n):
        start = next(a for a, _, kd, ll in segments if kd == kind and ll == l)
        got(kind, l, FOUR, k.grp.at[start + n])

    def begin():
        @pl.loop(0, LEAD)
        def _(i):
            stage(stage_own, i, 0, LEAD)

    def end():
        for start, n, kind, l in segments:

            @pl.loop(0, n)
            def _(i, start=start, kind=kind, l=l):
                for sem in (k.gsx, k.gsy, k.gsz):
                    got(kind, l, 1, sem.at[start + i])
                got(kind, l, FOUR, k.gsp.at[start + i])

    return tick, ready, begin, end


def loads_of(z, me, k):
    def load_gu(l, j, WG, WU, sems):
        cols = cols_of(j * z.FC, z.FC)

        @pl.loop(0, NB)
        def _(d):
            rows = rows_of(d * z.RB, z.RB)
            for n, (W, own, G) in enumerate(((WG, k.wg, k.GG), (WU, k.wu, k.GU))):

                @pl.when(d == me.s)
                def _(n=n, W=W, own=own):
                    copy(own.at[l, :, cols], W.at[rows, :], sems.at[n]).start()

                @pl.when(d != me.s)
                def _(n=n, W=W, G=G):
                    copy(G.at[l, rows, cols], W.at[rows, :], sems.at[n]).start()

    def load_d(l, j, W, sem):
        @pl.when(j == me.s)
        def _():
            copy(k.wd.at[l], W, sem).start()

        @pl.when(j != me.s)
        def _():
            copy(k.GD.at[l, rows_of(j * z.FB, z.FB), :], W, sem).start()

    return load_gu, load_d


def forward(z, me, k):
    tick, ready, gather_begin, gather_end = gather_of(z, me, k)
    load_gu, load_d = loads_of(z, me, k)
    NS, U1 = NB, z.NG + z.ND

    def put_turned(ref, a):
        turned = a.T
        for d in range(NB):
            core, px, py = d % TWO, d // FOUR, (d // TWO) % TWO
            i = TWO * px + py if core == 0 else TWO * py + px
            ref[core * z.HB + i * z.RB : core * z.HB + (i + 1) * z.RB, :] = turned[d * z.RB : (d + 1) * z.RB, :]

    def turn(A):
        def body(xb, yb, ab, bb, si, sj, so, sp):
            def fetch(m, e):
                rows = rows_of(m * z.TS, z.TS)
                copy(k.x.at[0, rows, :], xb.at[e], si.at[e]).start()
                copy(k.dy.at[0, rows, :], yb.at[e], sj.at[e]).start()

            fetch(0, 0)

            def sent(e):
                done(ab.at[e], so.at[e])
                done(bb.at[e], sp.at[e])

            @pl.loop(0, NS)
            def _(m):
                e = odd(m)
                cols = cols_of(m * z.TS, z.TS)

                @pl.when(m + 1 < NS)
                def _():
                    fetch(m + 1, 1 - e)

                done(xb.at[e], si.at[e])
                done(yb.at[e], sj.at[e])
                a = normed(xb[e])
                A[rows_of(m * z.TS, z.TS), :] = a

                @pl.when(m >= TWO)
                def _():
                    sent(e)

                put_turned(ab.at[e], a)
                bb[e] = yb[e].T
                copy(ab.at[e], k.ATH.at[0, :, cols], so.at[e]).start()
                copy(bb.at[e], k.DYT.at[:, cols], sp.at[e]).start()

                @pl.when(e == 1)
                def _():
                    tick(lax.div(m, TWO), 0, FOUR)

            sent(0)
            sent(1)

        blocks = [vmem(TWO, z.TS, z.D)] * TWO + [vmem(TWO, z.D, z.TS)] * TWO
        pl.run_scoped(body, *blocks, *[dmas(TWO)] * FOUR)

    def gate_up(l, A, hook):
        def body(WG, WU, sb, tb, ab, ws, *so):
            kept = ((sb, k.SS), (tb, k.TT), (ab, k.ACT))

            def sent(e):
                for (b, _), sem in zip(kept, so, strict=True):
                    done(b.at[e], sem.at[e])

            def fetch(j, e):
                ready(l, "gu", TWO * j)
                ready(l, "gu", TWO * j + 1)
                load_gu(l, j, WG.at[e], WU.at[e], ws.at[e])

            fetch(0, 0)

            @pl.loop(0, NB)
            def _(j):
                slot = odd(j)
                cols = cols_of(j * z.FC, z.FC)
                done(WG.at[slot], ws.at[slot, 0])
                done(WU.at[slot], ws.at[slot, 1])

                @pl.loop(0, TWO)
                def _(m):
                    @pl.when(j + m > 0)
                    def _():
                        sent(0)
                        sent(1)

                    for e in range(TWO):
                        a = A[rows_of((TWO * m + e) * z.TM, z.TM), :]
                        gate = nn(a, WG[slot])
                        up = nn(a, WU[slot])
                        sig = lax.logistic(gate)
                        sl = gate * sig
                        sb[e] = sl
                        tb[e] = up * (sig + sl * (1.0 - sig))
                        ab[e] = (sl * up).astype(BF)
                    for e in range(TWO):
                        rows = rows_of((TWO * m + e) * z.TM, z.TM)
                        for (b, to), sem in zip(kept, so, strict=True):
                            copy(b.at[e], to.at[l, rows, cols], sem.at[e]).start()
                    hook(TWO * j + m)

                    @pl.when(both(m == 1, j + 1 < NB))
                    def _():
                        fetch(j + 1, 1 - slot)

            sent(0)
            sent(1)

        weights = [vmem(TWO, z.D, z.FC)] * TWO
        tiles = [vmem(TWO, z.TM, z.FC, dtype=F32)] * TWO + [vmem(TWO, z.TM, z.FC)]
        pl.run_scoped(body, *weights, *tiles, dmas(TWO, TWO), *[dmas(TWO)] * THREE)

    def down(A, hook):
        def body(W, ab, xb, hb, tb, ws, si, sj, so, sp):
            for n in range(z.ND):
                ready(0, "d", n)

            @pl.loop(0, NB)
            def _(d):
                load_d(0, d, W.at[rows_of(d * z.FB, z.FB), :], ws.at[0])

            def fetch(m, e):
                rows = rows_of(m * z.TS, z.TS)
                copy(k.ACT.at[0, rows, :], ab.at[e], si.at[e]).start()
                copy(k.x.at[0, rows, :], xb.at[e], sj.at[e]).start()

            fetch(0, 0)
            done(W, ws.at[0])

            def sent(e):
                done(hb.at[e], so.at[e])
                done(tb.at[e], sp.at[e])

            @pl.loop(0, NS)
            def _(m):
                e = odd(m)
                rows = rows_of(m * z.TS, z.TS)

                @pl.when(m + 1 < NS)
                def _():
                    fetch(m + 1, 1 - e)

                done(ab.at[e], si.at[e])
                done(xb.at[e], sj.at[e])
                low = nn(ab[e], W[...]).astype(BF)
                h = (xb[e].astype(F32) + low.astype(F32)).astype(BF)

                @pl.when(m >= TWO)
                def _():
                    sent(e)

                hb[e] = h
                a = normed(h)
                A[rows, :] = a
                put_turned(tb.at[e], a)
                copy(hb.at[e], k.H1.at[rows, :], so.at[e]).start()
                copy(tb.at[e], k.ATH.at[1, :, cols_of(m * z.TS, z.TS)], sp.at[e]).start()
                hook(m)

            sent(0)
            sent(1)

        tiles = [vmem(TWO, z.TS, z.F)] + [vmem(TWO, z.TS, z.D)] * TWO + [vmem(TWO, z.D, z.TS)]
        pl.run_scoped(body, vmem(z.F, z.D), *tiles, dmas(1), *[dmas(TWO)] * FOUR)

    def run(A):
        gather_begin()
        turn(A)
        gate_up(0, A, lambda n: tick(n + FOUR, FOUR, U1))
        for t in (U1, U1 + 1):
            tick(t, t, t + 1)
        t2, t3 = U1 + TWO, U1 + TWO + FOUR

        def in_down(m):
            @pl.when(odd(m) == 1)
            def _():
                tick(t2 + lax.div(m, TWO), t2, t3)

        down(A, in_down)
        gate_up(1, A, lambda n: tick(n + t3, t3, t3 + z.NG, 0, U1 + z.NG))
        for t in range(U1 + z.NG, z.UNITS + TWO):
            tick(t, t, t + 1, U1 + z.NG)
        for n in range(z.ND):
            ready(1, "d", n)
        gather_end()

    pl.run_scoped(run, vmem(z.T, z.D))


def backward(z, me, k):
    load_gu, load_d = loads_of(z, me, k)
    c, u, v = me.c, me.u, me.v
    RB, FC, HB, PR, TM = z.RB, z.FC, z.HB, z.PR, z.TM
    KINDS = range(THREE)

    def place(core, i):
        return i + core * (odd(i) * TWO + lax.div(i, TWO) - i)

    def block_of(g):
        q = lax.rem(g, STEPS)
        b = lax.div(q, THREE)
        return 1 - lax.div(g, STEPS), b, q - THREE * b + lax.div(b, THREE)

    def first_row(b):
        return jnp.minimum(THREE * b, NB - THREE)

    def has(g, n):
        _, b, t = block_of(g)
        inside = both(g >= 0, g < LAST)
        if n == 0:
            return both(inside, either(b < TWO, t > 0))
        return inside if n == 1 else both(inside, t == 0)

    def halves(slot, n):
        return remote(k.SP.at[n], k.LP.at[slot, n], k.d2ds.at[n], k.d2dr.at[slot, n], me.to_p)

    def first(slot, n):
        return remote(k.S1.at[slot, n], k.L1.at[slot, n], k.s1s.at[slot, n], k.s1r.at[slot, n], me.to_1)

    def second(slot, n):
        return remote(k.S2.at[slot, n], k.L2.at[slot, n], k.s2s.at[slot, n], k.s2r.at[slot, n], me.to_2)

    def third(slot, n):
        return remote(k.S3.at[slot, n], k.L3.at[slot, n], k.s3s.at[slot, n], k.s3r.at[slot, n], me.to_z)

    def sum_1(g):
        slot = odd(g)
        for n in KINDS:

            @pl.when(has(g - TWO, n))
            def _(n=n):
                second(slot, n).wait_send()

            @pl.when(has(g, n))
            def _(n=n):
                first(slot, n).wait_recv()
                away, home = rows_of((1 - v) * RB, RB), rows_of(v * RB, RB)
                k.S2[slot, n] = (k.K1[slot, n, away, :] + k.L1[slot, n, away, :].astype(F32)).astype(BF)
                k.K2[slot, n] = k.K1[slot, n, home, :] + k.L1[slot, n, home, :].astype(F32)
                second(slot, n).start()

        pl.semaphore_signal(k.credit, inc=1, device_id=me.to_1, device_id_type=MESH)

    def sum_2(g):
        slot = odd(g)
        for n in KINDS:

            @pl.when(has(g - TWO, n))
            def _(n=n):
                third(slot, n).wait_send()

            @pl.when(has(g, n))
            def _(n=n):
                second(slot, n).wait_recv()
                k.S3[slot, n] = (k.K2[slot, n] + k.L2[slot, n].astype(F32)).astype(BF)
                third(slot, n).start()

    def sum_3(g):
        slot = odd(g)
        l, b, t = block_of(g)
        for n in KINDS:

            @pl.when(has(g - TWO, n))
            def _(n=n):
                done(k.OUT.at[slot, n], k.osem.at[slot, n])

            @pl.when(has(g, n))
            def _(n=n):
                third(slot, n).wait_recv()
                k.OUT[slot, n] = (k.S3[slot, n].astype(F32) + k.L3[slot, n].astype(F32)).astype(BF)

                @pl.when(t == 0)
                def _():
                    copy(k.OUT.at[slot, n], k.dwdt.at[l, rows_of((first_row(b) + n) * RB, RB), :], k.osem.at[slot, n]).start()

                if n < TWO:

                    @pl.when(t > 0)
                    def _():
                        to = (k.dwg, k.dwu)[n].at[l, :, cols_of((TWO * b + t - 1) * FC, FC)]
                        copy(k.OUT.at[slot, n], to, k.osem.at[slot, n]).start()

    def sums(g):
        for lag, fn in ((FOUR, sum_3), (THREE, sum_2), (TWO, sum_1)):

            @pl.when(both(g >= lag, g < LAST + lag))
            def _(lag=lag, fn=fn):
                fn(g - lag)

    def first_sent(g):
        for n in KINDS:

            @pl.when(has(g, n))
            def _(n=n):
                first(odd(g), n).wait_send()

    def slots_free(g):
        first_sent(g - TWO)

        @pl.when(g >= TWO)
        def _():
            pl.semaphore_wait(k.credit, 1)

    def start_all(made, g):
        for n in KINDS:

            @pl.when(has(g, n))
            def _(n=n):
                made(n).start()

    def layer(it, AT, DA):
        l = 1 - it
        copy(k.ATH.at[l], AT, k.lsem.at[0]).start()

        def body(WG, WU, WD, stb, DGU, ws, si, sj, sa):
            def fetch(j, m, e):
                rows, cols = rows_of(m * TM, TM), cols_of(j * FC, FC)
                copy(k.SS.at[l, rows, cols], stb.at[0, e], si.at[e]).start()
                copy(k.TT.at[l, rows, cols], stb.at[1, e], sj.at[e]).start()

            def column(q):
                own = lax.rem(TWO * (1 - u) + q, FOUR)
                return jnp.where(q < FOUR, TWO * place(1 - c, q) + 1 - c, TWO * place(c, own) + c)

            def fetch_act(q):
                copy(k.ACT.at[l, :, cols_of(column(q) * FC, FC)], DGU.at[odd(q)], sa.at[odd(q)]).start()

            load_d(l, jnp.int32(0), WD, ws.at[TWO])
            load_gu(l, jnp.int32(0), WG, WU, ws)
            fetch(jnp.int32(0), jnp.int32(0), 0)

            @pl.loop(0, FOUR)
            def _(m):
                DA[rows_of(m * TM, TM), :] = jnp.zeros((TM, z.D), F32)

            done(AT, k.lsem.at[0])

            def product(b, q):
                @pl.when(q + 1 < NB)
                def _():
                    fetch_act(q + 1)

                done(DGU.at[odd(q)], sa.at[odd(q)])
                return nn(k.DHT[rows_of(first_row(b) * RB, THREE * RB), :], DGU[odd(q)])

            def down_step(b, g):
                slot = odd(g)

                @pl.loop(0, FOUR)
                def _(q):
                    val = product(b, q).astype(BF)
                    for n in KINDS:
                        k.SP[n, rows_of(q * RB, RB), :] = val[n * RB : (n + 1) * RB]

                start_all(lambda n: halves(slot, n), g)
                slots_free(g)
                for n in KINDS:

                    @pl.when(has(g, n))
                    def _(n=n):
                        halves(slot, n).wait_recv()

                @pl.loop(0, TWO)
                def _(e):
                    val, at = product(b, e + FOUR), rows_of((TWO * (1 - u) + e) * RB, RB)
                    for n in KINDS:
                        k.S1[slot, n, rows_of(e * RB, RB), :] = (
                            val[n * RB : (n + 1) * RB] + k.LP[slot, n, at, :].astype(F32)
                        ).astype(BF)

                start_all(lambda n: first(slot, n), g)

                @pl.loop(0, TWO)
                def _(e):
                    val, at = product(b, e + FOUR + TWO), rows_of((TWO * u + e) * RB, RB)
                    for n in KINDS:
                        k.K1[slot, n, rows_of(e * RB, RB), :] = val[n * RB : (n + 1) * RB] + k.LP[slot, n, at, :].astype(F32)

                for n in KINDS:

                    @pl.when(has(g, n))
                    def _(n=n):
                        halves(slot, n).wait_send()

            def gate_up_step(j, g):
                slot = odd(g)
                done(WD, ws.at[TWO])

                @pl.loop(0, FOUR)
                def _(m):
                    e = odd(m)
                    rows = rows_of(m * TM, TM)

                    @pl.when(m + 1 < FOUR)
                    def _():
                        fetch(j, m + 1, 1 - e)

                    @pl.when(both(m + 1 == FOUR, j + 1 < NB))
                    def _():
                        fetch(j + 1, jnp.int32(0), 1 - e)

                    done(stb.at[0, e], si.at[e])
                    done(stb.at[1, e], sj.at[e])
                    dact = nt(k.DH[rows, :], WD[...]).astype(BF).astype(F32)
                    DGU[0, rows, :] = (dact * stb[1, e]).astype(BF)
                    DGU[1, rows, :] = (dact * stb[0, e]).astype(BF)

                @pl.when(j + 1 < NB)
                def _():
                    load_d(l, j + 1, WD, ws.at[TWO])

                for n in range(TWO):
                    k.SP[n] = nn(AT[rows_of((1 - c) * HB, HB), :], DGU[n]).astype(BF)
                    halves(slot, n).start()
                slots_free(g)
                out, keep = TWO * (1 - u) * RB, TWO * u * RB
                for n in range(TWO):
                    halves(slot, n).wait_recv()
                    k.S1[slot, n] = (
                        nn(AT[rows_of(c * HB + out, PR), :], DGU[n]) + k.LP[slot, n, rows_of(out, PR), :].astype(F32)
                    ).astype(BF)
                    k.K1[slot, n] = nn(AT[rows_of(c * HB + keep, PR), :], DGU[n]) + k.LP[slot, n, rows_of(keep, PR), :].astype(F32)
                    first(slot, n).start()
                done(WG, ws.at[0])
                done(WU, ws.at[1])

                @pl.loop(0, FOUR)
                def _(m):
                    rows = rows_of(m * TM, TM)
                    DA[rows, :] += nt(DGU[0, rows, :], WG[...]) + nt(DGU[1, rows, :], WU[...])

                @pl.when(j + 1 < NB)
                def _():
                    load_gu(l, j + 1, WG, WU, ws)

                for n in range(TWO):
                    halves(slot, n).wait_send()

            @pl.loop(0, STEPS)
            def _(q):
                g = it * STEPS + q
                _, b, t = block_of(g)

                @pl.when(t == 0)
                def _():
                    fetch_act(jnp.int32(0))

                sums(g)

                @pl.when(t == 0)
                def _():
                    down_step(b, g)

                @pl.when(t > 0)
                def _():
                    gate_up_step(TWO * b + t - 1, g)

        weights = [vmem(z.D, FC)] * TWO + [vmem(z.FB, z.D)]
        tiles = [vmem(TWO, TWO, TM, FC, dtype=F32), vmem(TWO, z.T, FC)]
        pl.run_scoped(body, *weights, *tiles, dmas(THREE), *[dmas(TWO)] * THREE)
        norm_back(l, DA)

    def norm_back(l, DA):
        def body(hb, ob, si, so):
            def fetch(m, e):
                rows = rows_of(m * z.TS, z.TS)

                @pl.when(l == 1)
                def _():
                    copy(k.H1.at[rows, :], hb.at[e], si.at[e]).start()

                @pl.when(l == 0)
                def _():
                    copy(k.x.at[0, rows, :], hb.at[e], si.at[e]).start()

            fetch(jnp.int32(0), 0)

            @pl.loop(0, NB)
            def _(m):
                e = odd(m)
                rows = rows_of(m * z.TS, z.TS)

                @pl.when(m + 1 < NB)
                def _():
                    fetch(m + 1, 1 - e)

                done(hb.at[e], si.at[e])

                @pl.when(both(l == 0, m >= TWO))
                def _():
                    done(ob.at[e], so.at[e])

                wide = hb[e].astype(F32)
                da = DA[rows, :].astype(BF).astype(F32)
                scale = lax.rsqrt(jnp.mean(wide * wide, -1, keepdims=True) + 1e-6)
                along = jnp.mean(da * wide, -1, keepdims=True)
                dn = (da * scale - wide * (along * scale * scale * scale)).astype(BF)
                new = (k.DH[rows, :].astype(F32) + dn.astype(F32)).astype(BF)
                k.DH[rows, :] = new
                ob[e] = new

                @pl.when(l == 1)
                def _():
                    k.DHT[:, cols_of(m * z.TS, z.TS)] = ob[e].T

                @pl.when(l == 0)
                def _():
                    copy(ob.at[e], k.dx.at[0, rows, :], so.at[e]).start()

            @pl.when(l == 0)
            def _():
                for e in range(TWO):
                    done(ob.at[e], so.at[e])

        pl.run_scoped(body, *[vmem(TWO, z.TS, z.D)] * TWO, *[dmas(TWO)] * TWO)

    copy(k.dy.at[0], k.DH, k.lsem.at[0]).start()
    copy(k.DYT, k.DHT, k.lsem.at[1]).start()
    done(k.DH, k.lsem.at[0])
    done(k.DHT, k.lsem.at[1])

    @pl.loop(0, TWO)
    def _(it):
        pl.run_scoped(functools.partial(layer, it), vmem(z.D, z.T), vmem(z.T, z.D, dtype=F32))

    @pl.loop(LAST, LAST + FOUR)
    def _(g):
        sums(g)

    for g in (LAST - TWO, LAST - 1):
        first_sent(jnp.int32(g))
        for n in range(TWO):
            second(g % TWO, n).wait_send()
            third(g % TWO, n).wait_send()
            done(k.OUT.at[g % TWO, n], k.osem.at[g % TWO, n])
    pl.semaphore_wait(k.credit, TWO)


class Refs:
    def __init__(self, names, refs):
        for name, ref in zip(names, refs, strict=True):
            setattr(self, name, ref)


def call(name, z, fn, number, ins, outs, scratch, flops):
    names = [*ins, *outs, *scratch]

    def kernel(*refs):
        me, k = Here(), Refs(names, refs)
        me.meet()
        fn(z, me, k)

    hbm = pl.BlockSpec(memory_space=pl.ANY)
    made = pl.pallas_call(
        kernel,
        out_shape=[jax.ShapeDtypeStruct(*spec) for spec in outs.values()],
        in_specs=[hbm] * len(ins),
        out_specs=[hbm] * len(outs),
        scratch_shapes=list(scratch.values()),
        compiler_params=pltpu.CompilerParams(collective_id=number, has_side_effects=True, vmem_limit_bytes=67043328),
        cost_estimate=pl.CostEstimate(flops=flops, bytes_accessed=1 << 28, transcendentals=0),
        name=name,
    )(*ins.values())
    return dict(zip(outs, made, strict=True))


def solution(mesh):
    def step(x, dy, wg, wu, wd):
        _, T, D = x.shape
        F = wg.shape[TWO]
        z = Sizes(T, D, F)
        RB, FB, FC, L = z.RB, z.FB, z.FC, TWO
        ins = {"x": x, "dy": dy, "wg": wg, "wu": wu, "wd": wd}
        kept = {
            **{name: ((L, D, F), BF) for name in ("GG", "GU")},
            "GD": ((L, F, D), BF),
            **{name: ((L, T, F), F32) for name in ("SS", "TT")},
            "ACT": ((L, T, F), BF),
            "H1": ((T, D), BF),
            "ATH": ((L, D, T), BF),
            "DYT": ((D, T), BF),
        }
        results = {
            "dx": ((1, T, D), BF),
            **{name: ((L, RB, F), BF) for name in ("dwg", "dwu")},
            "dwdt": ((L, D, FB), BF),
        }
        gather = {name: dmas(z.UNITS) for name in ("gsx", "gsy", "gsz", "gsp", "grx", "gry", "grz", "grp")}
        item, pair = (TWO, THREE, RB, FC), (TWO, THREE, z.PR, FC)
        sums = {
            "DH": vmem(T, D),
            "DHT": vmem(D, T),
            "SP": vmem(THREE, z.HB, FC),
            "LP": vmem(TWO, THREE, z.HB, FC),
            **{name: vmem(*pair) for name in ("S1", "L1")},
            "K1": vmem(*pair, dtype=F32),
            **{name: vmem(*item) for name in ("S2", "L2", "S3", "L3", "OUT")},
            "K2": vmem(*item, dtype=F32),
            "d2ds": dmas(THREE),
            **{name: dmas(TWO, THREE) for name in ("d2dr", "s1s", "s1r", "s2s", "s2r", "s3s", "s3r", "osem")},
            "credit": pltpu.SemaphoreType.REGULAR,
            "lsem": dmas(TWO),
        }
        flops = TWO * T * D * F
        kept = call("forward", z, forward, 0, ins, kept, gather, flops * (FOUR + 1))
        made = call("backward", z, backward, 1, {**ins, **kept}, results, sums, flops * STEPS)
        return made["dx"], made["dwg"], made["dwu"], jnp.swapaxes(made["dwdt"], 1, TWO)

    states, cut = P(("rep", "r", "s"), None, None), P(None, "s", None)
    return jax.shard_map(
        step,
        mesh=mesh,
        in_specs=(states, states, cut, cut, cut),
        out_specs=(states, *[P("rep", "s", None)] * THREE),
        check_vma=False,
    )
```

```python
import functools

import jax
import jax.numpy as jnp
from jax import lax
from jax.experimental import pallas as pl
from jax.experimental.pallas import tpu as pltpu
from jax.sharding import PartitionSpec as P

MESH = pl.DeviceIdType.MESH
BF, F32 = jnp.bfloat16, jnp.float32
NB = 8
LEAD = 8
LAG = 2
TWO, THREE, FOUR = 2, 3, 4
STEPS = 11
LAST = TWO * STEPS


def nn(a, b):
    return lax.dot_general(a, b, (((1,), (0,)), ((), ())), preferred_element_type=F32)


def nt(a, b):
    return lax.dot_general(a, b, (((1,), (1,)), ((), ())), preferred_element_type=F32)


def rows_of(start, size):
    return pl.ds(start if isinstance(start, int) else pl.multiple_of(start, 16), size)


def cols_of(start, size):
    return pl.ds(start if isinstance(start, int) else pl.multiple_of(start, 128), size)


def odd(i):
    return lax.rem(i, TWO)


def copy(src, dst, sem):
    return pltpu.make_async_copy(src, dst, sem)


def done(ref, sem):
    pltpu.make_async_copy(ref, ref, sem).wait()


def both(a, b):
    return jnp.logical_and(a, b)


def either(a, b):
    return jnp.logical_or(a, b)


def vmem(*shape, dtype=BF):
    return pltpu.VMEM(shape, dtype)


def dmas(*shape):
    return pltpu.SemaphoreType.DMA(shape)


class Sizes:
    def __init__(self, T, D, F):
        self.T, self.D, self.F = T, D, F
        self.RB, self.FB, self.HB = D // NB, F // NB, D // TWO
        self.FC = self.FB
        self.UC, self.UD = self.FC // TWO, self.FB // FOUR
        self.NG, self.ND = F // self.UC, FOUR
        self.TM, self.TS = T // FOUR, T // NB
        self.PR = TWO * self.RB
        self.UNITS = TWO * (self.NG + self.ND)


class Here:
    def __init__(self):
        self.r, self.s = lax.axis_index("r"), lax.axis_index("s")
        rep, r, s = lax.axis_index("rep"), self.r, self.s
        self.c = c = odd(s)
        y, x = odd(lax.div(s, TWO)), lax.div(s, FOUR)
        self.xn, self.yn, partner = s + FOUR - NB * x, s + TWO - FOUR * y, s + 1 - TWO * c
        self.far = self.xn + self.yn - s
        self.over = self.yn + c * (self.xn - self.yn)
        self.u, self.v = x + c * (y - x), y + c * (x - y)
        n1 = self.xn + c * (self.yn - self.xn)
        n2 = self.xn + self.yn - n1
        self.to_p, self.to_x, self.to_y, self.to_z = (rep, r, partner), (rep, r, self.xn), (rep, r, self.yn), (rep, 1 - r, s)
        self.to_1, self.to_2 = (rep, r, n1), (rep, r, n2)
        self.z0, self.z1, self.c0, self.c1 = r == 0, r == 1, c == 0, c == 1

    def meet(self):
        barrier = pltpu.get_barrier_semaphore()
        for dev in (self.to_p, self.to_x, self.to_y, self.to_z):
            pl.semaphore_signal(barrier, inc=1, device_id=dev, device_id_type=MESH)
        pl.semaphore_wait(barrier, FOUR)


def remote(src, dst, ss, rs, dev):
    return pltpu.make_async_remote_copy(src, dst, ss, rs, device_id=dev, device_id_type=MESH)


def normed(h):
    wide = h.astype(F32)
    scale = lax.rsqrt(jnp.mean(wide * wide, -1, keepdims=True) + 1e-6)
    return (wide * scale).astype(BF)


def gather_of(z, me, k):
    segments = (
        (0, z.NG, "gu", 0),
        (z.NG, z.ND, "d", 0),
        (z.NG + z.ND, z.NG, "gu", 1),
        (z.UNITS - z.ND, z.ND, "d", 1),
    )

    def held(kind, l, n, d):
        if kind == "gu":
            return [G.at[l, rows_of(d * z.RB, z.RB), cols_of(n * z.UC, z.UC)] for G in (k.GG, k.GU)]
        return [k.GD.at[l, rows_of(d * z.FB + n * z.UD, z.UD), :]]

    def mine(kind, l, n):
        if kind == "gu":
            return [w.at[l, :, cols_of(n * z.UC, z.UC)] for w in (k.wg, k.wu)]
        return [k.wd.at[l, rows_of(n * z.UD, z.UD), :]]

    def got(kind, l, n, sem):
        done(k.GG.at[l, pl.ds(0, n * z.PR), pl.ds(0, z.UC)] if kind == "gu" else k.GD.at[l, pl.ds(0, n * z.UD), :], sem)

    def push(srcs, dsts, ss, rs, i, dev):
        for a, b in zip(srcs, dsts, strict=True):
            remote(a, b, ss.at[i], rs.at[i], dev).start()

    def pass_on(ref, i):
        push(ref, ref, k.gsp, k.grp, i, me.to_p)

    def stage_own(kind, l, n, i):
        own, there = mine(kind, l, n), held(kind, l, n, me.s)

        @pl.when(either(me.z0, me.c0))
        def _():
            push(own, there, k.gsx, k.grx, i, me.to_x)

        @pl.when(either(me.z0, me.c1))
        def _():
            push(own, there, k.gsy, k.gry, i, me.to_y)

        push(own, there, k.gsp, k.grp, i, me.to_p)

    def stage_1(kind, l, n, i):
        hx, hy = held(kind, l, n, me.xn), held(kind, l, n, me.yn)

        @pl.when(either(me.z0, me.c0))
        def _():
            got(kind, l, 1, k.grx.at[i])

        @pl.when(either(me.z0, me.c1))
        def _():
            got(kind, l, 1, k.gry.at[i])

        @pl.when(me.z0)
        def _():
            on = held(kind, l, n, me.over)
            push(on, on, k.gsz, k.grz, i, me.to_z)
            pass_on(hx, i)
            pass_on(hy, i)

        @pl.when(both(me.z1, me.c0))
        def _():
            push(hx, hx, k.gsy, k.gry, i, me.to_y)
            pass_on(hx, i)

        @pl.when(both(me.z1, me.c1))
        def _():
            push(hy, hy, k.gsx, k.grx, i, me.to_x)
            pass_on(hy, i)

    def stage_2(kind, l, n, i):
        @pl.when(me.z1)
        def _():
            far, over = held(kind, l, n, me.far), held(kind, l, n, me.over)

            @pl.when(me.c0)
            def _():
                got(kind, l, 1, k.gry.at[i])

            @pl.when(me.c1)
            def _():
                got(kind, l, 1, k.grx.at[i])

            push(far, far, k.gsz, k.grz, i, me.to_z)
            pass_on(far, i)
            got(kind, l, 1, k.grz.at[i])
            pass_on(over, i)

    def stage_3(kind, l, n, i):
        @pl.when(me.z0)
        def _():
            got(kind, l, 1, k.grz.at[i])
            pass_on(held(kind, l, n, me.far), i)

    def stage(fn, i, low, high):
        for start, n, kind, l in segments:
            a, b = max(start, low), min(start + n, high)
            if a < b:

                @pl.when(both(i >= a, i < b))
                def _(kind=kind, l=l, start=start):
                    fn(kind, l, i - start, i)

    def tick(t, low, high, first=0, last=z.UNITS):
        t = jnp.asarray(t, jnp.int32)
        stage(stage_own, t + LEAD, low + LEAD, high + LEAD)
        for n, fn in enumerate((stage_1, stage_2, stage_3)):
            lag = LAG * n
            stage(fn, t - lag, max(first, low - lag), min(last, high - lag))

    def ready(l, kind, n):
        start = next(a for a, _, kd, ll in segments if kd == kind and ll == l)
        got(kind, l, FOUR, k.grp.at[start + n])

    def begin():
        @pl.loop(0, LEAD)
        def _(i):
            stage(stage_own, i, 0, LEAD)

    def end():
        for start, n, kind, l in segments:

            @pl.loop(0, n)
            def _(i, start=start, kind=kind, l=l):
                for sem in (k.gsx, k.gsy, k.gsz):
                    got(kind, l, 1, sem.at[start + i])
                got(kind, l, FOUR, k.gsp.at[start + i])

    return tick, ready, begin, end


def loads_of(z, me, k):
    def load_gu(l, j, WG, WU, sems):
        cols = cols_of(j * z.FC, z.FC)

        @pl.loop(0, NB)
        def _(d):
            rows = rows_of(d * z.RB, z.RB)
            for n, (W, own, G) in enumerate(((WG, k.wg, k.GG), (WU, k.wu, k.GU))):

                @pl.when(d == me.s)
                def _(n=n, W=W, own=own):
                    copy(own.at[l, :, cols], W.at[rows, :], sems.at[n]).start()

                @pl.when(d != me.s)
                def _(n=n, W=W, G=G):
                    copy(G.at[l, rows, cols], W.at[rows, :], sems.at[n]).start()

    def load_d(l, j, W, sem):
        @pl.when(j == me.s)
        def _():
            copy(k.wd.at[l], W, sem).start()

        @pl.when(j != me.s)
        def _():
            copy(k.GD.at[l, rows_of(j * z.FB, z.FB), :], W, sem).start()

    return load_gu, load_d


def forward(z, me, k):
    tick, ready, gather_begin, gather_end = gather_of(z, me, k)
    load_gu, load_d = loads_of(z, me, k)
    NS, U1 = NB, z.NG + z.ND

    def put_turned(ref, a):
        turned = a.T
        for d in range(NB):
            core, px, py = d % TWO, d // FOUR, (d // TWO) % TWO
            i = TWO * px + py if core == 0 else TWO * py + px
            ref[core * z.HB + i * z.RB : core * z.HB + (i + 1) * z.RB, :] = turned[d * z.RB : (d + 1) * z.RB, :]

    def turn(A):
        def body(xb, yb, ab, si, sj, so):
            def fetch(m, e):
                rows = rows_of(m * z.TS, z.TS)
                copy(k.x.at[0, rows, :], xb.at[e], si.at[e]).start()
                copy(k.dy.at[0, rows, :], yb.at[e], sj.at[e]).start()

            fetch(0, 0)

            def sent(e):
                done(ab.at[e], so.at[e])

            @pl.loop(0, NS)
            def _(m):
                e = odd(m)
                cols = cols_of(m * z.TS, z.TS)

                @pl.when(m + 1 < NS)
                def _():
                    fetch(m + 1, 1 - e)

                done(xb.at[e], si.at[e])
                done(yb.at[e], sj.at[e])
                a = normed(xb[e])
                A[rows_of(m * z.TS, z.TS), :] = a

                @pl.when(m >= TWO)
                def _():
                    sent(e)

                put_turned(ab.at[e], a)
                copy(ab.at[e], k.ATH.at[0, :, cols], so.at[e]).start()
                k.DHT[:, cols] = yb[e].T

                @pl.when(e == 1)
                def _():
                    tick(lax.div(m, TWO), 0, FOUR)

            sent(0)
            sent(1)

        blocks = [vmem(TWO, z.TS, z.D)] * TWO + [vmem(TWO, z.D, z.TS)]
        pl.run_scoped(body, *blocks, *[dmas(TWO)] * THREE)

    def gate_up(l, A, hook):
        def body(WG, WU, sb, tb, ab, ws, *so):
            kept = ((sb, k.SS), (tb, k.TT), (ab, k.ACT))

            def sent(e):
                for (b, _), sem in zip(kept, so, strict=True):
                    done(b.at[e], sem.at[e])

            def fetch(j, e):
                ready(l, "gu", TWO * j)
                ready(l, "gu", TWO * j + 1)
                load_gu(l, j, WG.at[e], WU.at[e], ws.at[e])

            fetch(0, 0)

            @pl.loop(0, NB)
            def _(j):
                slot = odd(j)
                cols = cols_of(j * z.FC, z.FC)
                done(WG.at[slot], ws.at[slot, 0])
                done(WU.at[slot], ws.at[slot, 1])

                @pl.loop(0, TWO)
                def _(m):
                    @pl.when(j + m > 0)
                    def _():
                        sent(0)
                        sent(1)

                    for e in range(TWO):
                        a = A[rows_of((TWO * m + e) * z.TM, z.TM), :]
                        gate = nn(a, WG[slot])
                        up = nn(a, WU[slot])
                        sig = lax.logistic(gate)
                        sl = gate * sig
                        sb[e] = sl
                        tb[e] = up * (sig + sl * (1.0 - sig))
                        ab[e] = (sl * up).astype(BF)
                    for e in range(TWO):
                        rows = rows_of((TWO * m + e) * z.TM, z.TM)
                        for (b, to), sem in zip(kept, so, strict=True):
                            copy(b.at[e], to.at[l, rows, cols], sem.at[e]).start()
                    hook(TWO * j + m)

                    @pl.when(both(m == 1, j + 1 < NB))
                    def _():
                        fetch(j + 1, 1 - slot)

            sent(0)
            sent(1)

        weights = [vmem(TWO, z.D, z.FC)] * TWO
        tiles = [vmem(TWO, z.TM, z.FC, dtype=F32)] * TWO + [vmem(TWO, z.TM, z.FC)]
        pl.run_scoped(body, *weights, *tiles, dmas(TWO, TWO), *[dmas(TWO)] * THREE)

    def down(A, hook):
        def body(W, ab, xb, hb, tb, ws, si, sj, so, sp):
            for n in range(z.ND):
                ready(0, "d", n)

            @pl.loop(0, NB)
            def _(d):
                load_d(0, d, W.at[rows_of(d * z.FB, z.FB), :], ws.at[0])

            def fetch(m, e):
                rows = rows_of(m * z.TS, z.TS)
                copy(k.ACT.at[0, rows, :], ab.at[e], si.at[e]).start()
                copy(k.x.at[0, rows, :], xb.at[e], sj.at[e]).start()

            fetch(0, 0)
            done(W, ws.at[0])

            def sent(e):
                done(hb.at[e], so.at[e])
                done(tb.at[e], sp.at[e])

            @pl.loop(0, NS)
            def _(m):
                e = odd(m)
                rows = rows_of(m * z.TS, z.TS)

                @pl.when(m + 1 < NS)
                def _():
                    fetch(m + 1, 1 - e)

                done(ab.at[e], si.at[e])
                done(xb.at[e], sj.at[e])
                low = nn(ab[e], W[...]).astype(BF)
                h = (xb[e].astype(F32) + low.astype(F32)).astype(BF)

                @pl.when(m >= TWO)
                def _():
                    sent(e)

                hb[e] = h
                a = normed(h)
                A[rows, :] = a
                put_turned(tb.at[e], a)
                copy(hb.at[e], k.H1.at[rows, :], so.at[e]).start()
                copy(tb.at[e], k.ATH.at[1, :, cols_of(m * z.TS, z.TS)], sp.at[e]).start()
                hook(m)

            sent(0)
            sent(1)

        tiles = [vmem(TWO, z.TS, z.F)] + [vmem(TWO, z.TS, z.D)] * TWO + [vmem(TWO, z.D, z.TS)]
        pl.run_scoped(body, vmem(z.F, z.D), *tiles, dmas(1), *[dmas(TWO)] * FOUR)

    def run(A):
        gather_begin()
        copy(k.dy.at[0], k.DH, k.lsem.at[0]).start()
        turn(A)
        t1, t2, t3 = TWO * LAG + TWO, U1 + TWO * LAG, U1 + TWO * LAG + FOUR
        for t in range(FOUR, t1):
            tick(t, t, t + 1)
        gate_up(0, A, lambda n: tick(n + t1, t1, t1 + z.NG))
        for t in range(t1 + z.NG, t2):
            tick(t, t, t + 1)

        def in_down(m):
            @pl.when(odd(m) == 1)
            def _():
                tick(t2 + lax.div(m, TWO), t2, t3)

        down(A, in_down)
        gate_up(1, A, lambda n: tick(n + t3, t3, t3 + z.NG, 0, U1 + z.NG))

    def late(n):
        tick(n + U1 + z.NG, U1 + z.NG, U1 + z.NG + NB, U1 + z.NG)

    def all_there():
        for n in range(z.ND):
            ready(1, "d", n)

    pl.run_scoped(run, vmem(z.T, z.D))
    return late, all_there, gather_end


def backward(z, me, k, late, all_there):
    load_gu, load_d = loads_of(z, me, k)
    c, u, v = me.c, me.u, me.v
    RB, FC, HB, PR, TM = z.RB, z.FC, z.HB, z.PR, z.TM
    DR = THREE * RB
    KINDS = range(THREE)

    def place(core, i):
        return i + core * (odd(i) * TWO + lax.div(i, TWO) - i)

    def block_of(g):
        q = lax.rem(g, STEPS)
        b = lax.div(q, THREE)
        return 1 - lax.div(g, STEPS), b, q - THREE * b + lax.div(b, THREE)

    def first_row(b):
        return jnp.minimum(THREE * b, NB - THREE)

    def has(g, n):
        _, b, t = block_of(g)
        inside = both(g >= 0, g < LAST)
        if n == 0:
            return both(inside, either(b < TWO, t > 0))
        return inside if n == 1 else both(inside, t == 0)

    def halves(slot, n):
        rows = pl.ds(n * HB, HB)
        return remote(k.SP.at[rows, :], k.LP.at[slot, rows, :], k.d2ds.at[n], k.d2dr.at[slot, n], me.to_p)

    def block(slot, e):
        return remote(
            k.SP.at[rows_of(odd(e) * DR, DR), :], k.LP.at[slot, rows_of(e * DR, DR), :], k.b2ds.at[odd(e)], k.b2dr.at[slot, e], me.to_p
        )

    def first(slot, n):
        return remote(k.S1.at[slot, n], k.L1.at[slot, n], k.s1s.at[slot, n], k.s1r.at[slot, n], me.to_1)

    def second(slot, n):
        return remote(k.S2.at[slot, n], k.L2.at[slot, n], k.s2s.at[slot, n], k.s2r.at[slot, n], me.to_2)

    def third(slot, n):
        return remote(k.S3.at[slot, n], k.L3.at[slot, n], k.s3s.at[slot, n], k.s3r.at[slot, n], me.to_z)

    def sum_1(g):
        slot = odd(g)
        for n in KINDS:

            @pl.when(has(g - TWO, n))
            def _(n=n):
                second(slot, n).wait_send()

            @pl.when(has(g, n))
            def _(n=n):
                first(slot, n).wait_recv()
                away, home = rows_of((1 - v) * RB, RB), rows_of(v * RB, RB)
                k.S2[slot, n] = (k.K1[slot, n, away, :] + k.L1[slot, n, away, :].astype(F32)).astype(BF)
                k.K2[slot, n] = k.K1[slot, n, home, :] + k.L1[slot, n, home, :].astype(F32)
                second(slot, n).start()

        pl.semaphore_signal(k.credit, inc=1, device_id=me.to_1, device_id_type=MESH)

    def sum_2(g):
        slot = odd(g)
        for n in KINDS:

            @pl.when(has(g - TWO, n))
            def _(n=n):
                done(k.S3.at[slot, n], k.osem.at[slot, n])

            @pl.when(has(g, n))
            def _(n=n):
                second(slot, n).wait_recv()
                k.S3[slot, n] = (k.K2[slot, n] + k.L2[slot, n].astype(F32)).astype(BF)
                third(slot, n).start()

    def sum_3(g):
        slot = odd(g)
        l, b, t = block_of(g)
        for n in KINDS:

            @pl.when(has(g, n))
            def _(n=n):
                third(slot, n).wait()
                k.S3[slot, n] = (k.S3[slot, n].astype(F32) + k.L3[slot, n].astype(F32)).astype(BF)

                @pl.when(t == 0)
                def _():
                    copy(k.S3.at[slot, n], k.dwdt.at[l, rows_of((first_row(b) + n) * RB, RB), :], k.osem.at[slot, n]).start()

                if n < TWO:

                    @pl.when(t > 0)
                    def _():
                        to = (k.dwg, k.dwu)[n].at[l, :, cols_of((TWO * b + t - 1) * FC, FC)]
                        copy(k.S3.at[slot, n], to, k.osem.at[slot, n]).start()

    def sums(g):
        for lag, fn in ((FOUR, sum_3), (THREE, sum_2), (TWO, sum_1)):

            @pl.when(both(g >= lag, g < LAST + lag))
            def _(lag=lag, fn=fn):
                fn(g - lag)

    def first_sent(g):
        for n in KINDS:

            @pl.when(has(g, n))
            def _(n=n):
                first(odd(g), n).wait_send()

    def slots_free(g):
        first_sent(g - TWO)

        @pl.when(g >= TWO)
        def _():
            pl.semaphore_wait(k.credit, 1)

    def layer(it, AT, DA):
        l = 1 - it
        copy(k.ATH.at[l], AT, k.lsem.at[0]).start()

        def body(WG, WU, WD, stb, DGU, ws, si, sj, sa):
            def fetch(i):
                rows, cols = rows_of(lax.rem(i, FOUR) * TM, TM), cols_of(lax.div(i, FOUR) * FC, FC)
                e = lax.rem(i, THREE)
                copy(k.SS.at[l, rows, cols], stb.at[0, e], si.at[e]).start()
                copy(k.TT.at[l, rows, cols], stb.at[1, e], sj.at[e]).start()

            def column(q):
                theirs, own = lax.rem(TWO * (1 - v) + q, FOUR), lax.rem(TWO * (1 - u) + q, FOUR)
                return jnp.where(q < FOUR, TWO * place(1 - c, theirs) + 1 - c, TWO * place(c, own) + c)

            def fetch_act(q):
                e = lax.rem(q + TWO, THREE)
                copy(k.ACT.at[l, :, cols_of(column(q) * FC, FC)], DGU.at[e], sa.at[e]).start()

            load_gu(l, jnp.int32(0), WG, WU, ws)
            fetch_act(jnp.int32(0))
            fetch(jnp.int32(0))
            fetch(jnp.int32(1))

            @pl.loop(0, FOUR)
            def _(m):
                DA[rows_of(m * TM, TM), :] = jnp.zeros((TM, z.D), F32)

            done(AT, k.lsem.at[0])

            def product(b, q):
                e = lax.rem(q + TWO, THREE)

                @pl.when(both(q > 0, q + TWO < NB))
                def _():
                    fetch_act(q + TWO)

                @pl.when(both(it == 0, b == 0))
                def _():
                    late(q)

                done(DGU.at[e], sa.at[e])
                return nn(k.DHT[rows_of(first_row(b) * RB, DR), :], DGU[e])

            def down_step(b, g):
                slot = odd(g)
                fetch_act(jnp.int32(1))
                fetch_act(jnp.int32(TWO))

                @pl.loop(0, FOUR)
                def _(e):
                    val = product(b, e).astype(BF)

                    @pl.when(e >= TWO)
                    def _():
                        block(slot, e - TWO).wait_send()

                    k.SP[rows_of(odd(e) * DR, DR), :] = val
                    block(slot, e).start()

                slots_free(g)

                @pl.loop(0, TWO)
                def _(e):
                    block(slot, e).wait_recv()
                    val = (product(b, e + FOUR) + k.LP[slot, rows_of(e * DR, DR), :].astype(F32)).astype(BF)
                    for n in KINDS:
                        k.S1[slot, n, rows_of(e * RB, RB), :] = val[n * RB : (n + 1) * RB]

                for n in KINDS:

                    @pl.when(has(g, n))
                    def _(n=n):
                        first(slot, n).start()

                @pl.loop(0, TWO)
                def _(e):
                    block(slot, e + TWO).wait_recv()
                    val = product(b, e + FOUR + TWO) + k.LP[slot, rows_of((e + TWO) * DR, DR), :].astype(F32)
                    for n in KINDS:
                        k.K1[slot, n, rows_of(e * RB, RB), :] = val[n * RB : (n + 1) * RB]

                for e in range(TWO):
                    block(slot, e).wait_send()

                @pl.when(b == 0)
                def _():
                    @pl.when(it == 0)
                    def _():
                        all_there()

                    load_d(l, jnp.int32(0), WD, ws.at[TWO])

            def gate_up_step(j, g):
                slot = odd(g)
                done(WD, ws.at[TWO])

                @pl.loop(0, FOUR)
                def _(m):
                    i = j * FOUR + m
                    e = lax.rem(i, THREE)
                    rows = rows_of(m * TM, TM)

                    @pl.when(i + TWO < FOUR * NB)
                    def _():
                        fetch(i + TWO)

                    done(stb.at[0, e], si.at[e])
                    done(stb.at[1, e], sj.at[e])
                    dact = nt(k.DH[rows, :], WD[...]).astype(BF).astype(F32)
                    DGU[0, rows, :] = (dact * stb[1, e]).astype(BF)
                    DGU[1, rows, :] = (dact * stb[0, e]).astype(BF)

                @pl.when(j + 1 < NB)
                def _():
                    load_d(l, j + 1, WD, ws.at[TWO])

                for n in range(TWO):
                    k.SP[n * HB : (n + 1) * HB, :] = nn(AT[rows_of((1 - c) * HB, HB), :], DGU[n]).astype(BF)
                    halves(slot, n).start()
                slots_free(g)
                out, keep = TWO * (1 - u) * RB, TWO * u * RB
                for n in range(TWO):
                    halves(slot, n).wait_recv()
                    k.S1[slot, n] = (
                        nn(AT[rows_of(c * HB + out, PR), :], DGU[n]) + k.LP[slot, rows_of(n * HB + out, PR), :].astype(F32)
                    ).astype(BF)
                    k.K1[slot, n] = nn(AT[rows_of(c * HB + keep, PR), :], DGU[n]) + k.LP[slot, rows_of(n * HB + keep, PR), :].astype(F32)
                    first(slot, n).start()
                done(WG, ws.at[0])
                done(WU, ws.at[1])

                @pl.loop(0, FOUR)
                def _(m):
                    rows = rows_of(m * TM, TM)
                    DA[rows, :] += nt(DGU[0, rows, :], WG[...]) + nt(DGU[1, rows, :], WU[...])

                @pl.when(j + 1 < NB)
                def _():
                    load_gu(l, j + 1, WG, WU, ws)

                @pl.when(both(lax.rem(j, TWO) == 1, j + TWO + 1 < NB))
                def _():
                    fetch_act(jnp.int32(0))

                for n in range(TWO):
                    halves(slot, n).wait_send()

            @pl.loop(0, STEPS)
            def _(q):
                g = it * STEPS + q
                _, b, t = block_of(g)
                sums(g)

                @pl.when(t == 0)
                def _():
                    down_step(b, g)

                @pl.when(t > 0)
                def _():
                    gate_up_step(TWO * b + t - 1, g)

        weights = [vmem(z.D, FC)] * TWO + [vmem(z.FB, z.D)]
        tiles = [vmem(TWO, THREE, TM, FC, dtype=F32), vmem(THREE, z.T, FC)]
        pl.run_scoped(body, *weights, *tiles, *[dmas(THREE)] * FOUR)
        norm_back(l, DA)

    def norm_back(l, DA):
        def body(hb, ob, si, so):
            def fetch(m, e):
                rows = rows_of(m * z.TS, z.TS)

                @pl.when(l == 1)
                def _():
                    copy(k.H1.at[rows, :], hb.at[e], si.at[e]).start()

                @pl.when(l == 0)
                def _():
                    copy(k.x.at[0, rows, :], hb.at[e], si.at[e]).start()

            fetch(jnp.int32(0), 0)

            @pl.loop(0, NB)
            def _(m):
                e = odd(m)
                rows = rows_of(m * z.TS, z.TS)

                @pl.when(m + 1 < NB)
                def _():
                    fetch(m + 1, 1 - e)

                done(hb.at[e], si.at[e])

                @pl.when(both(l == 0, m >= TWO))
                def _():
                    done(ob.at[e], so.at[e])

                wide = hb[e].astype(F32)
                da = DA[rows, :].astype(BF).astype(F32)
                scale = lax.rsqrt(jnp.mean(wide * wide, -1, keepdims=True) + 1e-6)
                along = jnp.mean(da * wide, -1, keepdims=True)
                dn = (da * scale - wide * (along * scale * scale * scale)).astype(BF)
                new = (k.DH[rows, :].astype(F32) + dn.astype(F32)).astype(BF)
                k.DH[rows, :] = new
                ob[e] = new

                @pl.when(l == 1)
                def _():
                    k.DHT[:, cols_of(m * z.TS, z.TS)] = ob[e].T

                @pl.when(l == 0)
                def _():
                    copy(ob.at[e], k.dx.at[0, rows, :], so.at[e]).start()

            @pl.when(l == 0)
            def _():
                for e in range(TWO):
                    done(ob.at[e], so.at[e])

        pl.run_scoped(body, *[vmem(TWO, z.TS, z.D)] * TWO, *[dmas(TWO)] * TWO)

    done(k.DH, k.lsem.at[0])

    @pl.loop(0, TWO)
    def _(it):
        pl.run_scoped(functools.partial(layer, it), vmem(z.D, z.T), vmem(z.T, z.D, dtype=F32))

    @pl.loop(LAST, LAST + FOUR)
    def _(g):
        sums(g)

    for g in (LAST - TWO, LAST - 1):
        first_sent(jnp.int32(g))
        for n in range(TWO):
            second(g % TWO, n).wait_send()
            done(k.S3.at[g % TWO, n], k.osem.at[g % TWO, n])
    pl.semaphore_wait(k.credit, TWO)


class Refs:
    def __init__(self, names, refs):
        for name, ref in zip(names, refs, strict=True):
            setattr(self, name, ref)


def call(name, z, fn, number, ins, outs, scratch, flops):
    names = [*ins, *outs, *scratch]

    def kernel(*refs):
        me, k = Here(), Refs(names, refs)
        me.meet()
        fn(z, me, k)

    hbm = pl.BlockSpec(memory_space=pl.ANY)
    made = pl.pallas_call(
        kernel,
        out_shape=[jax.ShapeDtypeStruct(*spec) for spec in outs.values()],
        in_specs=[hbm] * len(ins),
        out_specs=[hbm] * len(outs),
        scratch_shapes=list(scratch.values()),
        compiler_params=pltpu.CompilerParams(collective_id=number, has_side_effects=True, vmem_limit_bytes=67043328),
        cost_estimate=pl.CostEstimate(flops=flops, bytes_accessed=1 << 28, transcendentals=0),
        name=name,
    )(*ins.values())
    return dict(zip(outs, made, strict=True))


def solution(mesh):
    def step(x, dy, wg, wu, wd):
        _, T, D = x.shape
        F = wg.shape[TWO]
        z = Sizes(T, D, F)
        RB, FB, FC, L = z.RB, z.FB, z.FC, TWO
        ins = {"x": x, "dy": dy, "wg": wg, "wu": wu, "wd": wd}
        kept = {
            **{name: ((L, D, F), BF) for name in ("GG", "GU")},
            "GD": ((L, F, D), BF),
            **{name: ((L, T, F), F32) for name in ("SS", "TT")},
            "ACT": ((L, T, F), BF),
            "H1": ((T, D), BF),
            "ATH": ((L, D, T), BF),
        }
        results = {
            "dx": ((1, T, D), BF),
            **{name: ((L, RB, F), BF) for name in ("dwg", "dwu")},
            "dwdt": ((L, D, FB), BF),
        }
        gather = {name: dmas(z.UNITS) for name in ("gsx", "gsy", "gsz", "gsp", "grx", "gry", "grz", "grp")}
        item, pair = (TWO, THREE, RB, FC), (TWO, THREE, z.PR, FC)
        sums = {
            "DH": vmem(T, D),
            "DHT": vmem(D, T),
            "SP": vmem(TWO * z.HB, FC),
            "LP": vmem(TWO, THREE * z.HB, FC),
            **{name: vmem(*pair) for name in ("S1", "L1")},
            "K1": vmem(*pair, dtype=F32),
            **{name: vmem(*item) for name in ("S2", "L2", "S3", "L3")},
            "K2": vmem(*item, dtype=F32),
            "d2ds": dmas(TWO),
            "d2dr": dmas(TWO, TWO),
            "b2ds": dmas(TWO),
            "b2dr": dmas(TWO, FOUR),
            **{name: dmas(TWO, THREE) for name in ("s1s", "s1r", "s2s", "s2r", "s3s", "s3r", "osem")},
            "credit": pltpu.SemaphoreType.REGULAR,
            "lsem": dmas(1),
        }
        flops = TWO * T * D * F

        def whole(z, me, k):
            late, all_there, gather_end = forward(z, me, k)
            backward(z, me, k, late, all_there)
            gather_end()

        made = call("whole", z, whole, 0, ins, {**results, **kept}, {**gather, **sums}, flops * (STEPS + FOUR + TWO))
        return made["dx"], made["dwg"], made["dwu"], jnp.swapaxes(made["dwdt"], 1, TWO)

    states, cut = P(("rep", "r", "s"), None, None), P(None, "s", None)
    return jax.shard_map(
        step,
        mesh=mesh,
        in_specs=(states, states, cut, cut, cut),
        out_specs=(states, *[P("rep", "s", None)] * THREE),
        check_vma=False,
    )
```

```python
import functools

import jax
import jax.numpy as jnp
from jax import lax
from jax.experimental import pallas as pl
from jax.experimental.pallas import tpu as pltpu
from jax.sharding import PartitionSpec as P

MESH = pl.DeviceIdType.MESH
BF, F32 = jnp.bfloat16, jnp.float32
NB = 8
LEAD = 8
LAG = 2
TWO, THREE, FOUR = 2, 3, 4
STEPS = 11
LAST = TWO * STEPS


def nn(a, b):
    return lax.dot_general(a, b, (((1,), (0,)), ((), ())), preferred_element_type=F32)


def nt(a, b):
    return lax.dot_general(a, b, (((1,), (1,)), ((), ())), preferred_element_type=F32)


def rows_of(start, size):
    return pl.ds(start if isinstance(start, int) else pl.multiple_of(start, 16), size)


def cols_of(start, size):
    return pl.ds(start if isinstance(start, int) else pl.multiple_of(start, 128), size)


def odd(i):
    return lax.rem(i, TWO)


def copy(src, dst, sem):
    return pltpu.make_async_copy(src, dst, sem)


def done(ref, sem):
    pltpu.make_async_copy(ref, ref, sem).wait()


def both(a, b):
    return jnp.logical_and(a, b)


def either(a, b):
    return jnp.logical_or(a, b)


def vmem(*shape, dtype=BF):
    return pltpu.VMEM(shape, dtype)


def dmas(*shape):
    return pltpu.SemaphoreType.DMA(shape)


class Sizes:
    def __init__(self, T, D, F):
        self.T, self.D, self.F = T, D, F
        self.RB, self.FB, self.HB = D // NB, F // NB, D // TWO
        self.FC = self.FB
        self.UC, self.UD = self.FC // TWO, self.FB // FOUR
        self.NG, self.ND = F // self.UC, FOUR
        self.TM, self.TS = T // FOUR, T // NB
        self.PR = TWO * self.RB
        self.UNITS = TWO * (self.NG + self.ND)


class Here:
    def __init__(self):
        self.r, self.s = lax.axis_index("r"), lax.axis_index("s")
        rep, r, s = lax.axis_index("rep"), self.r, self.s
        self.c = c = odd(s)
        y, x = odd(lax.div(s, TWO)), lax.div(s, FOUR)
        self.xn, self.yn, partner = s + FOUR - NB * x, s + TWO - FOUR * y, s + 1 - TWO * c
        self.far = self.xn + self.yn - s
        self.over = self.yn + c * (self.xn - self.yn)
        self.u, self.v = x + c * (y - x), y + c * (x - y)
        n1 = self.xn + c * (self.yn - self.xn)
        n2 = self.xn + self.yn - n1
        self.to_p, self.to_x, self.to_y, self.to_z = (rep, r, partner), (rep, r, self.xn), (rep, r, self.yn), (rep, 1 - r, s)
        self.to_1, self.to_2 = (rep, r, n1), (rep, r, n2)
        self.z0, self.z1, self.c0, self.c1 = r == 0, r == 1, c == 0, c == 1

    def meet(self):
        barrier = pltpu.get_barrier_semaphore()
        for dev in (self.to_p, self.to_x, self.to_y, self.to_z):
            pl.semaphore_signal(barrier, inc=1, device_id=dev, device_id_type=MESH)
        pl.semaphore_wait(barrier, FOUR)


def remote(src, dst, ss, rs, dev):
    return pltpu.make_async_remote_copy(src, dst, ss, rs, device_id=dev, device_id_type=MESH)


def normed(h):
    wide = h.astype(F32)
    scale = lax.rsqrt(jnp.mean(wide * wide, -1, keepdims=True) + 1e-6)
    return (wide * scale).astype(BF)


def gather_of(z, me, k):
    segments = (
        (0, z.NG, "gu", 0),
        (z.NG, z.ND, "d", 0),
        (z.NG + z.ND, z.NG, "gu", 1),
        (z.UNITS - z.ND, z.ND, "d", 1),
    )

    def held(kind, l, n, d):
        if kind == "gu":
            return [G.at[l, rows_of(d * z.RB, z.RB), cols_of(n * z.UC, z.UC)] for G in (k.GG, k.GU)]
        return [k.GD.at[l, rows_of(d * z.FB + n * z.UD, z.UD), :]]

    def mine(kind, l, n):
        if kind == "gu":
            return [w.at[l, :, cols_of(n * z.UC, z.UC)] for w in (k.wg, k.wu)]
        return [k.wd.at[l, rows_of(n * z.UD, z.UD), :]]

    def got(kind, l, n, sem):
        done(k.GG.at[l, pl.ds(0, n * z.PR), pl.ds(0, z.UC)] if kind == "gu" else k.GD.at[l, pl.ds(0, n * z.UD), :], sem)

    def push(srcs, dsts, ss, rs, i, dev):
        for a, b in zip(srcs, dsts, strict=True):
            remote(a, b, ss.at[i], rs.at[i], dev).start()

    def pass_on(ref, i):
        push(ref, ref, k.gsp, k.grp, i, me.to_p)

    def stage_own(kind, l, n, i):
        own, there = mine(kind, l, n), held(kind, l, n, me.s)

        @pl.when(either(me.z0, me.c0))
        def _():
            push(own, there, k.gsx, k.grx, i, me.to_x)

        @pl.when(either(me.z0, me.c1))
        def _():
            push(own, there, k.gsy, k.gry, i, me.to_y)

        push(own, there, k.gsp, k.grp, i, me.to_p)

    def stage_1(kind, l, n, i):
        hx, hy = held(kind, l, n, me.xn), held(kind, l, n, me.yn)

        @pl.when(either(me.z0, me.c0))
        def _():
            got(kind, l, 1, k.grx.at[i])

        @pl.when(either(me.z0, me.c1))
        def _():
            got(kind, l, 1, k.gry.at[i])

        @pl.when(me.z0)
        def _():
            on = held(kind, l, n, me.over)
            push(on, on, k.gsz, k.grz, i, me.to_z)
            pass_on(hx, i)
            pass_on(hy, i)

        @pl.when(both(me.z1, me.c0))
        def _():
            push(hx, hx, k.gsy, k.gry, i, me.to_y)
            pass_on(hx, i)

        @pl.when(both(me.z1, me.c1))
        def _():
            push(hy, hy, k.gsx, k.grx, i, me.to_x)
            pass_on(hy, i)

    def stage_2(kind, l, n, i):
        @pl.when(me.z1)
        def _():
            far, over = held(kind, l, n, me.far), held(kind, l, n, me.over)

            @pl.when(me.c0)
            def _():
                got(kind, l, 1, k.gry.at[i])

            @pl.when(me.c1)
            def _():
                got(kind, l, 1, k.grx.at[i])

            push(far, far, k.gsz, k.grz, i, me.to_z)
            pass_on(far, i)
            got(kind, l, 1, k.grz.at[i])
            pass_on(over, i)

    def stage_3(kind, l, n, i):
        @pl.when(me.z0)
        def _():
            got(kind, l, 1, k.grz.at[i])
            pass_on(held(kind, l, n, me.far), i)

    def stage(fn, i, low, high):
        for start, n, kind, l in segments:
            a, b = max(start, low), min(start + n, high)
            if a < b:

                @pl.when(both(i >= a, i < b))
                def _(kind=kind, l=l, start=start):
                    fn(kind, l, i - start, i)

    def tick(t, low, high, first=0, last=z.UNITS, stages=THREE):
        t = jnp.asarray(t, jnp.int32)
        stage(stage_own, t + LEAD, low + LEAD, high + LEAD)
        for n, fn in enumerate((stage_1, stage_2, stage_3)[:stages]):
            lag = LAG * n
            stage(fn, t - lag, max(first, low - lag), min(last, high - lag))

    def ready(l, kind, n):
        start = next(a for a, _, kd, ll in segments if kd == kind and ll == l)
        got(kind, l, FOUR, k.grp.at[start + n])

    def begin():
        @pl.loop(0, LEAD)
        def _(i):
            stage(stage_own, i, 0, LEAD)

    def end():
        for start, n, kind, l in segments:

            @pl.loop(0, n)
            def _(i, start=start, kind=kind, l=l):
                for sem in (k.gsx, k.gsy, k.gsz):
                    got(kind, l, 1, sem.at[start + i])
                got(kind, l, FOUR, k.gsp.at[start + i])

    return tick, ready, begin, end, stage, stage_3


def loads_of(z, me, k):
    def load_gu(l, j, WG, WU, sems):
        cols = cols_of(j * z.FC, z.FC)

        @pl.loop(0, NB)
        def _(d):
            rows = rows_of(d * z.RB, z.RB)
            for n, (W, own, G) in enumerate(((WG, k.wg, k.GG), (WU, k.wu, k.GU))):

                @pl.when(d == me.s)
                def _(n=n, W=W, own=own):
                    copy(own.at[l, :, cols], W.at[rows, :], sems.at[n]).start()

                @pl.when(d != me.s)
                def _(n=n, W=W, G=G):
                    copy(G.at[l, rows, cols], W.at[rows, :], sems.at[n]).start()

    def load_d(l, j, W, sem):
        @pl.when(j == me.s)
        def _():
            copy(k.wd.at[l], W, sem).start()

        @pl.when(j != me.s)
        def _():
            copy(k.GD.at[l, rows_of(j * z.FB, z.FB), :], W, sem).start()

    return load_gu, load_d


def forward(z, me, k):
    tick, ready, gather_begin, gather_end, stage, stage_3 = gather_of(z, me, k)
    load_gu, load_d = loads_of(z, me, k)
    NS, U1 = NB, z.NG + z.ND

    def put_turned(ref, a):
        turned = a.T
        for d in range(NB):
            core, px, py = d % TWO, d // FOUR, (d // TWO) % TWO
            i = TWO * px + py if core == 0 else TWO * py + px
            ref[core * z.HB + i * z.RB : core * z.HB + (i + 1) * z.RB, :] = turned[d * z.RB : (d + 1) * z.RB, :]

    def turn(A):
        def body(xb, yb, ab, si, sj, so):
            def fetch(m, e):
                rows = rows_of(m * z.TS, z.TS)
                copy(k.x.at[0, rows, :], xb.at[e], si.at[e]).start()
                copy(k.dy.at[0, rows, :], yb.at[e], sj.at[e]).start()

            fetch(0, 0)

            def sent(e):
                done(ab.at[e], so.at[e])

            @pl.loop(0, NS)
            def _(m):
                e = odd(m)
                cols = cols_of(m * z.TS, z.TS)

                @pl.when(m + 1 < NS)
                def _():
                    fetch(m + 1, 1 - e)

                done(xb.at[e], si.at[e])
                done(yb.at[e], sj.at[e])
                a = normed(xb[e])
                A[rows_of(m * z.TS, z.TS), :] = a

                @pl.when(m >= TWO)
                def _():
                    sent(e)

                put_turned(ab.at[e], a)
                copy(ab.at[e], k.ATH.at[0, :, cols], so.at[e]).start()
                k.DHT[:, cols] = yb[e].T

                @pl.when(e == 1)
                def _():
                    tick(lax.div(m, TWO), 0, FOUR)

            sent(0)
            sent(1)

        blocks = [vmem(TWO, z.TS, z.D)] * TWO + [vmem(TWO, z.D, z.TS)]
        pl.run_scoped(body, *blocks, *[dmas(TWO)] * THREE)

    def gate_up(l, A, hook):
        def body(WG, WU, sb, tb, ab, ws, *so):
            kept = ((sb, k.SS), (tb, k.TT), (ab, k.ACT))

            def sent(e):
                for (b, _), sem in zip(kept, so, strict=True):
                    done(b.at[e], sem.at[e])

            def fetch(j, e):
                ready(l, "gu", TWO * j)
                ready(l, "gu", TWO * j + 1)
                load_gu(l, j, WG.at[e], WU.at[e], ws.at[e])

            fetch(0, 0)
            hook(-1)

            @pl.loop(0, NB)
            def _(j):
                slot = odd(j)
                cols = cols_of(j * z.FC, z.FC)
                with jax.named_scope("gu_wait"):
                    done(WG.at[slot], ws.at[slot, 0])
                    done(WU.at[slot], ws.at[slot, 1])

                @pl.loop(0, TWO)
                def _(m):
                    with jax.named_scope("gu_sent"):

                        @pl.when(j > 0)
                        def _():
                            for e in range(TWO):
                                sent(TWO * m + e)

                    with jax.named_scope("gu_dot"):
                        for e in range(TWO):
                            at = TWO * m + e
                            a = A[rows_of(at * z.TM, z.TM), :]
                            gate = nn(a, WG[slot])
                            up = nn(a, WU[slot])
                            sig = lax.logistic(gate)
                            sl = gate * sig
                            sb[at] = sl
                            tb[at] = up * (sig + sl * (1.0 - sig))
                            ab[at] = (sl * up).astype(BF)
                    for e in range(TWO):
                        at = TWO * m + e
                        for (b, to), sem in zip(kept, so, strict=True):
                            copy(b.at[at], to.at[l, rows_of(at * z.TM, z.TM), cols], sem.at[at]).start()

                    @pl.when(m == 0)
                    def _():
                        with jax.named_scope("gu_tick"):
                            hook(j)

                    @pl.when(both(m == 0, j + 1 < NB))
                    def _():
                        with jax.named_scope("gu_fetch"):
                            fetch(j + 1, 1 - slot)

            for e in range(FOUR):
                sent(e)

        weights = [vmem(TWO, z.D, z.FC)] * TWO
        tiles = [vmem(FOUR, z.TM, z.FC, dtype=F32)] * TWO + [vmem(FOUR, z.TM, z.FC)]
        pl.run_scoped(body, *weights, *tiles, dmas(TWO, TWO), *[dmas(FOUR)] * THREE)

    def down(A, hook):
        def body(W, ab, xb, hb, tb, ws, si, sj, so, sp):
            def fetch(m, e):
                rows = rows_of(m * z.TS, z.TS)
                copy(k.ACT.at[0, rows, :], ab.at[e], si.at[e]).start()
                copy(k.x.at[0, rows, :], xb.at[e], sj.at[e]).start()

            fetch(0, 0)
            for n in range(z.ND):
                with jax.named_scope("dn_ready"):
                    ready(0, "d", n)

                @pl.loop(0, NB)
                def _(d, n=n):
                    rows = rows_of(d * z.FB + n * z.UD, z.UD)

                    @pl.when(d == me.s)
                    def _():
                        copy(k.wd.at[0, pl.ds(n * z.UD, z.UD), :], W.at[rows, :], ws.at[0]).start()

                    @pl.when(d != me.s)
                    def _():
                        copy(k.GD.at[0, rows, :], W.at[rows, :], ws.at[0]).start()

            with jax.named_scope("dn_load"):
                done(W, ws.at[0])

            def fetched(e):
                done(ab.at[e], si.at[e])
                done(xb.at[e], sj.at[e])

            def product(e):
                low = nn(ab[e], W[...]).astype(BF)
                return (xb[e].astype(F32) + low.astype(F32)).astype(BF)

            def finish(m, e):
                a = normed(hb[e])
                A[rows_of(m * z.TS, z.TS), :] = a
                put_turned(tb.at[e], a)

            def send(m, e):
                copy(hb.at[e], k.H1.at[rows_of(m * z.TS, z.TS), :], so.at[e]).start()
                copy(tb.at[e], k.ATH.at[1, :, cols_of(m * z.TS, z.TS)], sp.at[e]).start()

            def sent(e):
                done(hb.at[e], so.at[e])
                done(tb.at[e], sp.at[e])

            fetched(0)
            fetch(1, 1)
            hb[0] = product(0)

            @pl.loop(1, NS)
            def _(m):
                e = odd(m)

                @pl.when(m + 1 < NS)
                def _():
                    fetch(m + 1, 1 - e)

                with jax.named_scope("dn_wait"):
                    fetched(e)

                    @pl.when(m >= TWO)
                    def _():
                        sent(e)

                with jax.named_scope("dn_dot"):
                    finish(m - 1, 1 - e)
                    hb[e] = product(e)
                send(m - 1, 1 - e)
                with jax.named_scope("dn_tick"):
                    hook(m)

            last = (NS - 1) % TWO
            finish(NS - 1, last)
            send(NS - 1, last)
            sent(1 - last)
            sent(last)

        tiles = [vmem(TWO, z.TS, z.F)] + [vmem(TWO, z.TS, z.D)] * TWO + [vmem(TWO, z.D, z.TS)]
        pl.run_scoped(body, vmem(z.F, z.D), *tiles, dmas(1), *[dmas(TWO)] * FOUR)

    def run(A):
        gather_begin()
        copy(k.dy.at[0], k.DH, k.lsem.at[0]).start()
        with jax.named_scope("turn"):
            turn(A)
        t1, t2, t3 = TWO * LAG + TWO, U1 + TWO * LAG, U1 + TWO * LAG + FOUR
        with jax.named_scope("start"):
            for n in range(TWO):
                stage(stage_3, jnp.int32(n), n, n + 1)

        def in_first(j):
            if isinstance(j, int):
                for t in range(FOUR, t1):
                    tick(t, t, t + 1, 0, z.UNITS, TWO)
                return
            for n in range(TWO):
                tick(TWO * j + n + t1, t1 + n, t1 + z.NG)

        gate_up(0, A, in_first)
        for t in range(t1 + z.NG, t2):
            tick(t, t, t + 1)

        def in_down(m):
            @pl.when(odd(m) == 1)
            def _():
                tick(t2 + lax.div(m, TWO), t2, t3)

        down(A, in_down)

        def in_second(j):
            if not isinstance(j, int):
                for n in range(TWO):
                    tick(TWO * j + n + t3, t3 + n, t3 + z.NG)

        gate_up(1, A, in_second)

    def all_there():
        for n in range(z.ND):
            ready(1, "d", n)

    pl.run_scoped(run, vmem(z.T, z.D))
    return all_there, gather_end


def backward(z, me, k, all_there):
    load_gu, load_d = loads_of(z, me, k)
    c, u, v = me.c, me.u, me.v
    RB, FC, HB, PR, TM = z.RB, z.FC, z.HB, z.PR, z.TM
    DR = THREE * RB
    KINDS = range(THREE)

    def place(core, i):
        return i + core * (odd(i) * TWO + lax.div(i, TWO) - i)

    def block_of(g):
        q = lax.rem(g, STEPS)
        b = lax.div(q, THREE)
        return 1 - lax.div(g, STEPS), b, q - THREE * b + lax.div(b, THREE)

    def first_row(b):
        return jnp.minimum(THREE * b, NB - THREE)

    def has(g, n):
        _, b, t = block_of(g)
        inside = both(g >= 0, g < LAST)
        if n == 0:
            return both(inside, either(b < TWO, t > 0))
        return inside if n == 1 else both(inside, t == 0)

    def halves(slot, n):
        rows = pl.ds(n * HB, HB)
        return remote(k.SP.at[rows, :], k.LP.at[slot, rows, :], k.d2ds.at[n], k.d2dr.at[slot, n], me.to_p)

    def block(slot, e):
        return remote(
            k.SP.at[rows_of(odd(e) * DR, DR), :], k.LP.at[slot, rows_of(e * DR, DR), :], k.b2ds.at[odd(e)], k.b2dr.at[slot, e], me.to_p
        )

    def first(slot, n):
        return remote(k.S1.at[slot, n], k.L1.at[slot, n], k.s1s.at[slot, n], k.s1r.at[slot, n], me.to_1)

    def second(slot, n):
        return remote(k.S2.at[slot, n], k.L2.at[slot, n], k.s2s.at[slot, n], k.s2r.at[slot, n], me.to_2)

    def third(slot, n):
        return remote(k.S3.at[slot, n], k.L3.at[slot, n], k.s3s.at[slot, n], k.s3r.at[slot, n], me.to_z)

    def sum_1(g):
        slot = odd(g)
        for n in KINDS:

            @pl.when(has(g - TWO, n))
            def _(n=n):
                second(slot, n).wait_send()

            @pl.when(has(g, n))
            def _(n=n):
                with jax.named_scope("l1"):
                    first(slot, n).wait_recv()
                away, home = rows_of((1 - v) * RB, RB), rows_of(v * RB, RB)
                k.S2[slot, n] = (k.K1[slot, n, away, :] + k.L1[slot, n, away, :].astype(F32)).astype(BF)
                k.K2[slot, n] = k.K1[slot, n, home, :] + k.L1[slot, n, home, :].astype(F32)
                second(slot, n).start()

        pl.semaphore_signal(k.credit, inc=1, device_id=me.to_1, device_id_type=MESH)

    def sum_2(g):
        slot = odd(g)
        for n in KINDS:

            @pl.when(has(g - TWO, n))
            def _(n=n):
                done(k.S3.at[slot, n], k.osem.at[slot, n])

            @pl.when(has(g, n))
            def _(n=n):
                with jax.named_scope("l2"):
                    second(slot, n).wait_recv()
                k.S3[slot, n] = (k.K2[slot, n] + k.L2[slot, n].astype(F32)).astype(BF)
                third(slot, n).start()

    def sum_3(g):
        slot = odd(g)
        l, b, t = block_of(g)
        for n in KINDS:

            @pl.when(has(g, n))
            def _(n=n):
                with jax.named_scope("l3"):
                    third(slot, n).wait()
                k.S3[slot, n] = (k.S3[slot, n].astype(F32) + k.L3[slot, n].astype(F32)).astype(BF)

                @pl.when(t == 0)
                def _():
                    copy(k.S3.at[slot, n], k.dwdt.at[l, rows_of((first_row(b) + n) * RB, RB), :], k.osem.at[slot, n]).start()

                if n < TWO:

                    @pl.when(t > 0)
                    def _():
                        to = (k.dwg, k.dwu)[n].at[l, :, cols_of((TWO * b + t - 1) * FC, FC)]
                        copy(k.S3.at[slot, n], to, k.osem.at[slot, n]).start()

    def sums(g):
        for lag, fn in ((FOUR, sum_3), (THREE, sum_2), (TWO, sum_1)):

            @pl.when(both(g >= lag, g < LAST + lag))
            def _(lag=lag, fn=fn):
                fn(g - lag)

    def first_sent(g):
        for n in KINDS:

            @pl.when(has(g, n))
            def _(n=n):
                first(odd(g), n).wait_send()

    def slots_free(g):
        first_sent(g - TWO)

        @pl.when(g >= TWO)
        def _():
            pl.semaphore_wait(k.credit, 1)

    def layer(it, AT, DA):
        l = 1 - it
        copy(k.ATH.at[l], AT, k.lsem.at[0]).start()

        def body(WG, WU, WD, stb, DGU, ws, si, sj, sa):
            def fetch(i):
                rows, cols = rows_of(lax.rem(i, FOUR) * TM, TM), cols_of(lax.div(i, FOUR) * FC, FC)
                e = lax.rem(i, THREE)
                copy(k.SS.at[l, rows, cols], stb.at[0, e], si.at[e]).start()
                copy(k.TT.at[l, rows, cols], stb.at[1, e], sj.at[e]).start()

            def column(q):
                theirs, own = lax.rem(TWO * (1 - v) + q, FOUR), lax.rem(TWO * (1 - u) + q, FOUR)
                return jnp.where(q < FOUR, TWO * place(1 - c, theirs) + 1 - c, TWO * place(c, own) + c)

            def fetch_act(q):
                e = lax.rem(q + TWO, THREE)
                copy(k.ACT.at[l, :, cols_of(column(q) * FC, FC)], DGU.at[e], sa.at[e]).start()

            load_gu(l, jnp.int32(0), WG, WU, ws)
            fetch_act(jnp.int32(0))
            fetch(jnp.int32(0))
            fetch(jnp.int32(1))

            @pl.loop(0, FOUR)
            def _(m):
                DA[rows_of(m * TM, TM), :] = jnp.zeros((TM, z.D), F32)

            with jax.named_scope("at_wait"):
                done(AT, k.lsem.at[0])

            def product(b, q):
                e = lax.rem(q + TWO, THREE)

                @pl.when(both(q > 0, q + TWO < NB))
                def _():
                    fetch_act(q + TWO)

                with jax.named_scope("act_wait"):
                    done(DGU.at[e], sa.at[e])
                return nn(k.DHT[rows_of(first_row(b) * RB, DR), :], DGU[e])

            def down_step(b, g):
                slot = odd(g)
                fetch_act(jnp.int32(1))
                fetch_act(jnp.int32(TWO))

                with jax.named_scope("d_theirs"):
                    @pl.loop(0, FOUR)
                    def _(e):
                        val = product(b, e).astype(BF)

                        @pl.when(e >= TWO)
                        def _():
                            block(slot, e - TWO).wait_send()

                        k.SP[rows_of(odd(e) * DR, DR), :] = val
                        block(slot, e).start()

                with jax.named_scope("slots"):
                    slots_free(g)

                with jax.named_scope("d_ours"):
                    @pl.loop(0, TWO)
                    def _(e):
                        block(slot, e).wait_recv()
                        val = (product(b, e + FOUR) + k.LP[slot, rows_of(e * DR, DR), :].astype(F32)).astype(BF)
                        for n in KINDS:
                            k.S1[slot, n, rows_of(e * RB, RB), :] = val[n * RB : (n + 1) * RB]

                for n in KINDS:

                    @pl.when(has(g, n))
                    def _(n=n):
                        first(slot, n).start()

                with jax.named_scope("d_keep"):
                    @pl.loop(0, TWO)
                    def _(e):
                        block(slot, e + TWO).wait_recv()
                        val = product(b, e + FOUR + TWO) + k.LP[slot, rows_of((e + TWO) * DR, DR), :].astype(F32)
                        for n in KINDS:
                            k.K1[slot, n, rows_of(e * RB, RB), :] = val[n * RB : (n + 1) * RB]

                for e in range(TWO):
                    block(slot, e).wait_send()

                @pl.when(b == 0)
                def _():
                    @pl.when(it == 0)
                    def _():
                        all_there()

                    load_d(l, jnp.int32(0), WD, ws.at[TWO])

            def gate_up_step(j, g):
                slot = odd(g)
                with jax.named_scope("wd_wait"):
                    done(WD, ws.at[TWO])

                @pl.loop(0, FOUR)
                def _(m):
                    i = j * FOUR + m
                    e = lax.rem(i, THREE)
                    rows = rows_of(m * TM, TM)

                    @pl.when(i + TWO < FOUR * NB)
                    def _():
                        fetch(i + TWO)

                    with jax.named_scope("st_wait"):
                        done(stb.at[0, e], si.at[e])
                        done(stb.at[1, e], sj.at[e])
                    with jax.named_scope("a_dot"):
                        dact = nt(k.DH[rows, :], WD[...]).astype(BF).astype(F32)
                        DGU[0, rows, :] = (dact * stb[1, e]).astype(BF)
                        DGU[1, rows, :] = (dact * stb[0, e]).astype(BF)

                @pl.when(j + 1 < NB)
                def _():
                    load_d(l, j + 1, WD, ws.at[TWO])

                with jax.named_scope("b_dot"):
                    for n in range(TWO):
                        k.SP[n * HB : (n + 1) * HB, :] = nn(AT[rows_of((1 - c) * HB, HB), :], DGU[n]).astype(BF)
                        halves(slot, n).start()
                with jax.named_scope("slots"):
                    slots_free(g)
                out, keep = TWO * (1 - u) * RB, TWO * u * RB
                for n in range(TWO):
                    with jax.named_scope("half_wait"):
                        halves(slot, n).wait_recv()
                    k.S1[slot, n] = (
                        nn(AT[rows_of(c * HB + out, PR), :], DGU[n]) + k.LP[slot, rows_of(n * HB + out, PR), :].astype(F32)
                    ).astype(BF)
                    k.K1[slot, n] = nn(AT[rows_of(c * HB + keep, PR), :], DGU[n]) + k.LP[slot, rows_of(n * HB + keep, PR), :].astype(F32)
                    first(slot, n).start()
                with jax.named_scope("w_wait"):
                    done(WG, ws.at[0])
                    done(WU, ws.at[1])

                with jax.named_scope("da"):
                    @pl.loop(0, FOUR)
                    def _(m):
                        rows = rows_of(m * TM, TM)
                        DA[rows, :] += nt(DGU[0, rows, :], WG[...]) + nt(DGU[1, rows, :], WU[...])

                @pl.when(j + 1 < NB)
                def _():
                    load_gu(l, j + 1, WG, WU, ws)

                @pl.when(both(lax.rem(j, TWO) == 1, j + TWO + 1 < NB))
                def _():
                    fetch_act(jnp.int32(0))

                for n in range(TWO):
                    halves(slot, n).wait_send()

            @pl.loop(0, STEPS)
            def _(q):
                g = it * STEPS + q
                _, b, t = block_of(g)
                with jax.named_scope("sums"):
                    sums(g)

                @pl.when(t == 0)
                def _():
                    down_step(b, g)

                @pl.when(t > 0)
                def _():
                    gate_up_step(TWO * b + t - 1, g)

        weights = [vmem(z.D, FC)] * TWO + [vmem(z.FB, z.D)]
        tiles = [vmem(TWO, THREE, TM, FC, dtype=F32), vmem(THREE, z.T, FC)]
        pl.run_scoped(body, *weights, *tiles, *[dmas(THREE)] * FOUR)
        with jax.named_scope("norm"):
            norm_back(l, DA)

    def norm_back(l, DA):
        def body(hb, ob, si, so):
            def fetch(m, e):
                rows = rows_of(m * z.TS, z.TS)

                @pl.when(l == 1)
                def _():
                    copy(k.H1.at[rows, :], hb.at[e], si.at[e]).start()

                @pl.when(l == 0)
                def _():
                    copy(k.x.at[0, rows, :], hb.at[e], si.at[e]).start()

            fetch(jnp.int32(0), 0)

            @pl.loop(0, NB)
            def _(m):
                e = odd(m)
                rows = rows_of(m * z.TS, z.TS)

                @pl.when(m + 1 < NB)
                def _():
                    fetch(m + 1, 1 - e)

                done(hb.at[e], si.at[e])

                @pl.when(both(l == 0, lax.rem(m, FOUR) == 0))
                def _():
                    with jax.named_scope("norm_sums"):
                        sums(LAST + lax.div(m, FOUR))

                @pl.when(both(l == 0, m >= TWO))
                def _():
                    done(ob.at[e], so.at[e])

                wide = hb[e].astype(F32)
                da = DA[rows, :].astype(BF).astype(F32)
                scale = lax.rsqrt(jnp.mean(wide * wide, -1, keepdims=True) + 1e-6)
                along = jnp.mean(da * wide, -1, keepdims=True)
                dn = (da * scale - wide * (along * scale * scale * scale)).astype(BF)
                new = (k.DH[rows, :].astype(F32) + dn.astype(F32)).astype(BF)
                k.DH[rows, :] = new
                ob[e] = new

                @pl.when(l == 1)
                def _():
                    k.DHT[:, cols_of(m * z.TS, z.TS)] = ob[e].T

                @pl.when(l == 0)
                def _():
                    copy(ob.at[e], k.dx.at[0, rows, :], so.at[e]).start()

            @pl.when(l == 0)
            def _():
                for e in range(TWO):
                    done(ob.at[e], so.at[e])

        pl.run_scoped(body, *[vmem(TWO, z.TS, z.D)] * TWO, *[dmas(TWO)] * TWO)

    done(k.DH, k.lsem.at[0])

    @pl.loop(0, TWO)
    def _(it):
        pl.run_scoped(functools.partial(layer, it), vmem(z.D, z.T), vmem(z.T, z.D, dtype=F32))

    def turn_back(ib, ob, si, so):
        for l in range(TWO):
            copy(k.dwdt.at[l], ib.at[l], si.at[l]).start()
        with jax.named_scope("tail"):
            sums(jnp.int32(LAST + TWO))
        with jax.named_scope("turn_back"):
            for l in range(TWO):
                done(ib.at[l], si.at[l])
                ob[l] = ib[l].T
                copy(ob.at[l], k.dwd.at[l], so.at[l]).start()
        with jax.named_scope("tail"):
            sums(jnp.int32(LAST + THREE))
        for l in range(TWO):
            done(ob.at[l], so.at[l])

    pl.run_scoped(turn_back, vmem(TWO, z.D, z.FB), vmem(TWO, z.FB, z.D), dmas(TWO), dmas(TWO))

    for g in (LAST - TWO, LAST - 1):
        first_sent(jnp.int32(g))
        for n in range(TWO):
            second(g % TWO, n).wait_send()
            done(k.S3.at[g % TWO, n], k.osem.at[g % TWO, n])
    pl.semaphore_wait(k.credit, TWO)


class Refs:
    def __init__(self, names, refs):
        for name, ref in zip(names, refs, strict=True):
            setattr(self, name, ref)


def call(name, z, fn, number, ins, outs, scratch, flops):
    names = [*ins, *outs, *scratch]

    def kernel(*refs):
        me, k = Here(), Refs(names, refs)
        me.meet()
        fn(z, me, k)

    hbm = pl.BlockSpec(memory_space=pl.ANY)
    made = pl.pallas_call(
        kernel,
        out_shape=[jax.ShapeDtypeStruct(*spec) for spec in outs.values()],
        in_specs=[hbm] * len(ins),
        out_specs=[hbm] * len(outs),
        scratch_shapes=list(scratch.values()),
        compiler_params=pltpu.CompilerParams(collective_id=number, has_side_effects=True, vmem_limit_bytes=67043328),
        cost_estimate=pl.CostEstimate(flops=flops, bytes_accessed=1 << 28, transcendentals=0),
        name=name,
    )(*ins.values())
    return dict(zip(outs, made, strict=True))


def solution(mesh):
    def step(x, dy, wg, wu, wd):
        _, T, D = x.shape
        F = wg.shape[TWO]
        z = Sizes(T, D, F)
        RB, FB, FC, L = z.RB, z.FB, z.FC, TWO
        ins = {"x": x, "dy": dy, "wg": wg, "wu": wu, "wd": wd}
        kept = {
            **{name: ((L, D, F), BF) for name in ("GG", "GU")},
            "GD": ((L, F, D), BF),
            **{name: ((L, T, F), F32) for name in ("SS", "TT")},
            "ACT": ((L, T, F), BF),
            "H1": ((T, D), BF),
            "ATH": ((L, D, T), BF),
            "dwdt": ((L, D, FB), BF),
        }
        results = {
            "dx": ((1, T, D), BF),
            **{name: ((L, RB, F), BF) for name in ("dwg", "dwu")},
            "dwd": ((L, FB, D), BF),
        }
        gather = {name: dmas(z.UNITS) for name in ("gsx", "gsy", "gsz", "gsp", "grx", "gry", "grz", "grp")}
        item, pair = (TWO, THREE, RB, FC), (TWO, THREE, z.PR, FC)
        sums = {
            "DH": vmem(T, D),
            "DHT": vmem(D, T),
            "SP": vmem(TWO * z.HB, FC),
            "LP": vmem(TWO, THREE * z.HB, FC),
            **{name: vmem(*pair) for name in ("S1", "L1")},
            "K1": vmem(*pair, dtype=F32),
            **{name: vmem(*item) for name in ("S2", "L2", "S3", "L3")},
            "K2": vmem(*item, dtype=F32),
            "d2ds": dmas(TWO),
            "d2dr": dmas(TWO, TWO),
            "b2ds": dmas(TWO),
            "b2dr": dmas(TWO, FOUR),
            **{name: dmas(TWO, THREE) for name in ("s1s", "s1r", "s2s", "s2r", "s3s", "s3r", "osem")},
            "credit": pltpu.SemaphoreType.REGULAR,
            "lsem": dmas(1),
        }
        flops = TWO * T * D * F

        def whole(z, me, k):
            all_there, gather_end = forward(z, me, k)
            backward(z, me, k, all_there)
            gather_end()

        made = call("whole", z, whole, 0, ins, {**results, **kept}, {**gather, **sums}, flops * (STEPS + FOUR + TWO))
        return made["dx"], made["dwg"], made["dwu"], made["dwd"]

    states, cut = P(("rep", "r", "s"), None, None), P(None, "s", None)
    return jax.shard_map(
        step,
        mesh=mesh,
        in_specs=(states, states, cut, cut, cut),
        out_specs=(states, *[P("rep", "s", None)] * THREE),
        check_vma=False,
    )
```

```python
import functools

import jax
import jax.numpy as jnp
from jax import lax
from jax.experimental import pallas as pl
from jax.experimental.pallas import tpu as pltpu
from jax.sharding import PartitionSpec as P

MESH = pl.DeviceIdType.MESH
BF, F32 = jnp.bfloat16, jnp.float32
NB = 8
LEAD = 8
LAG = 2
TWO, THREE, FOUR = 2, 3, 4
STEPS = 11
LAST = TWO * STEPS


def nn(a, b):
    return lax.dot_general(a, b, (((1,), (0,)), ((), ())), preferred_element_type=F32)


def nt(a, b):
    return lax.dot_general(a, b, (((1,), (1,)), ((), ())), preferred_element_type=F32)


def rows_of(start, size):
    return pl.ds(start if isinstance(start, int) else pl.multiple_of(start, 16), size)


def cols_of(start, size):
    return pl.ds(start if isinstance(start, int) else pl.multiple_of(start, 128), size)


def odd(i):
    return lax.rem(i, TWO)


def copy(src, dst, sem):
    return pltpu.make_async_copy(src, dst, sem)


def done(ref, sem):
    pltpu.make_async_copy(ref, ref, sem).wait()


def both(a, b):
    return jnp.logical_and(a, b)


def either(a, b):
    return jnp.logical_or(a, b)


def vmem(*shape, dtype=BF):
    return pltpu.VMEM(shape, dtype)


def dmas(*shape):
    return pltpu.SemaphoreType.DMA(shape)


class Sizes:
    def __init__(self, T, D, F):
        self.T, self.D, self.F = T, D, F
        self.RB, self.FB, self.HB = D // NB, F // NB, D // TWO
        self.FC = self.FB
        self.UC, self.UD = self.FC // TWO, self.FB // NB
        self.NG, self.ND = F // self.UC, NB
        self.TM, self.TS = T // FOUR, T // NB
        self.PR = TWO * self.RB
        self.UNITS = TWO * (self.NG + self.ND)


class Here:
    def __init__(self):
        self.r, self.s = lax.axis_index("r"), lax.axis_index("s")
        rep, r, s = lax.axis_index("rep"), self.r, self.s
        self.c = c = odd(s)
        y, x = odd(lax.div(s, TWO)), lax.div(s, FOUR)
        self.xn, self.yn, partner = s + FOUR - NB * x, s + TWO - FOUR * y, s + 1 - TWO * c
        self.far = self.xn + self.yn - s
        self.over = self.yn + c * (self.xn - self.yn)
        self.u, self.v = x + c * (y - x), y + c * (x - y)
        n1 = self.xn + c * (self.yn - self.xn)
        n2 = self.xn + self.yn - n1
        self.to_p, self.to_x, self.to_y, self.to_z = (rep, r, partner), (rep, r, self.xn), (rep, r, self.yn), (rep, 1 - r, s)
        self.to_1, self.to_2 = (rep, r, n1), (rep, r, n2)
        self.z0, self.z1, self.c0, self.c1 = r == 0, r == 1, c == 0, c == 1

    def meet(self):
        barrier = pltpu.get_barrier_semaphore()
        for dev in (self.to_p, self.to_x, self.to_y, self.to_z):
            pl.semaphore_signal(barrier, inc=1, device_id=dev, device_id_type=MESH)
        pl.semaphore_wait(barrier, FOUR)


def remote(src, dst, ss, rs, dev):
    return pltpu.make_async_remote_copy(src, dst, ss, rs, device_id=dev, device_id_type=MESH)


def normed(h):
    wide = h.astype(F32)
    scale = lax.rsqrt(jnp.mean(wide * wide, -1, keepdims=True) + 1e-6)
    return (wide * scale).astype(BF)


def gather_of(z, me, k):
    segments = (
        (0, z.NG, "gu", 0),
        (z.NG, z.ND, "d", 0),
        (z.NG + z.ND, z.NG, "gu", 1),
        (z.UNITS - z.ND, z.ND, "d", 1),
    )

    def held(kind, l, n, d):
        if kind == "gu":
            return [G.at[l, rows_of(d * z.RB, z.RB), cols_of(n * z.UC, z.UC)] for G in (k.GG, k.GU)]
        return [k.GD.at[l, rows_of(d * z.FB + n * z.UD, z.UD), :]]

    def mine(kind, l, n):
        if kind == "gu":
            return [w.at[l, :, cols_of(n * z.UC, z.UC)] for w in (k.wg, k.wu)]
        return [k.wd.at[l, rows_of(n * z.UD, z.UD), :]]

    def got(kind, l, n, sem):
        done(k.GG.at[l, pl.ds(0, n * z.PR), pl.ds(0, z.UC)] if kind == "gu" else k.GD.at[l, pl.ds(0, n * z.UD), :], sem)

    def push(srcs, dsts, ss, rs, i, dev):
        for a, b in zip(srcs, dsts, strict=True):
            remote(a, b, ss.at[i], rs.at[i], dev).start()

    def pass_on(ref, i):
        push(ref, ref, k.gsp, k.grp, i, me.to_p)

    def stage_own(kind, l, n, i):
        own, there = mine(kind, l, n), held(kind, l, n, me.s)

        @pl.when(either(me.z0, me.c0))
        def _():
            push(own, there, k.gsx, k.grx, i, me.to_x)

        @pl.when(either(me.z0, me.c1))
        def _():
            push(own, there, k.gsy, k.gry, i, me.to_y)

        push(own, there, k.gsp, k.grp, i, me.to_p)

    def stage_1(kind, l, n, i):
        hx, hy = held(kind, l, n, me.xn), held(kind, l, n, me.yn)

        @pl.when(either(me.z0, me.c0))
        def _():
            got(kind, l, 1, k.grx.at[i])

        @pl.when(either(me.z0, me.c1))
        def _():
            got(kind, l, 1, k.gry.at[i])

        @pl.when(me.z0)
        def _():
            on = held(kind, l, n, me.over)
            push(on, on, k.gsz, k.grz, i, me.to_z)
            pass_on(hx, i)
            pass_on(hy, i)

        @pl.when(both(me.z1, me.c0))
        def _():
            push(hx, hx, k.gsy, k.gry, i, me.to_y)
            pass_on(hx, i)

        @pl.when(both(me.z1, me.c1))
        def _():
            push(hy, hy, k.gsx, k.grx, i, me.to_x)
            pass_on(hy, i)

    def stage_2(kind, l, n, i):
        @pl.when(me.z1)
        def _():
            far, over = held(kind, l, n, me.far), held(kind, l, n, me.over)

            @pl.when(me.c0)
            def _():
                got(kind, l, 1, k.gry.at[i])

            @pl.when(me.c1)
            def _():
                got(kind, l, 1, k.grx.at[i])

            push(far, far, k.gsz, k.grz, i, me.to_z)
            pass_on(far, i)
            got(kind, l, 1, k.grz.at[i])
            pass_on(over, i)

    def stage_3(kind, l, n, i):
        @pl.when(me.z0)
        def _():
            got(kind, l, 1, k.grz.at[i])
            pass_on(held(kind, l, n, me.far), i)

    def stage(fn, i, low, high):
        for start, n, kind, l in segments:
            a, b = max(start, low), min(start + n, high)
            if a < b:

                @pl.when(both(i >= a, i < b))
                def _(kind=kind, l=l, start=start):
                    fn(kind, l, i - start, i)

    def tick(t, low, high, most=NB):
        t = jnp.asarray(t, jnp.int32)
        stage(stage_own, t + LEAD, low + LEAD, high + LEAD)
        for lag, fn in ((TWO * LAG, stage_3), (LAG, stage_2), (0, stage_1)):
            if lag < most:
                stage(fn, t - lag, max(0, low - lag), min(z.UNITS, high - lag))

    def ready(l, kind, n):
        start = next(a for a, _, kd, ll in segments if kd == kind and ll == l)
        got(kind, l, FOUR, k.grp.at[start + n])

    def begin():
        @pl.loop(0, LEAD)
        def _(i):
            stage(stage_own, i, 0, LEAD)

    def end():
        for start, n, kind, l in segments:

            @pl.loop(0, n)
            def _(i, start=start, kind=kind, l=l):
                for sem in (k.gsx, k.gsy, k.gsz):
                    got(kind, l, 1, sem.at[start + i])
                got(kind, l, FOUR, k.gsp.at[start + i])

    return tick, ready, begin, end, stage, stage_3


def loads_of(z, me, k):
    def load_gu(l, j, WG, WU, sems):
        cols = cols_of(j * z.FC, z.FC)

        @pl.loop(0, NB)
        def _(d):
            rows = rows_of(d * z.RB, z.RB)
            for n, (W, own, G) in enumerate(((WG, k.wg, k.GG), (WU, k.wu, k.GU))):

                @pl.when(d == me.s)
                def _(n=n, W=W, own=own):
                    copy(own.at[l, :, cols], W.at[rows, :], sems.at[n]).start()

                @pl.when(d != me.s)
                def _(n=n, W=W, G=G):
                    copy(G.at[l, rows, cols], W.at[rows, :], sems.at[n]).start()

    def load_d(l, j, W, sem):
        @pl.when(j == me.s)
        def _():
            copy(k.wd.at[l], W, sem).start()

        @pl.when(j != me.s)
        def _():
            copy(k.GD.at[l, rows_of(j * z.FB, z.FB), :], W, sem).start()

    return load_gu, load_d


def forward(z, me, k):
    tick, ready, gather_begin, gather_end, stage, stage_3 = gather_of(z, me, k)
    load_gu, load_d = loads_of(z, me, k)
    NS, U1 = NB, z.NG + z.ND

    def put_turned(ref, a):
        turned = a.T
        for d in range(NB):
            core, px, py = d % TWO, d // FOUR, (d // TWO) % TWO
            i = TWO * px + py if core == 0 else TWO * py + px
            ref[core * z.HB + i * z.RB : core * z.HB + (i + 1) * z.RB, :] = turned[d * z.RB : (d + 1) * z.RB, :]

    def turn(A):
        def body(xb, yb, ab, si, sj, so):
            def fetch(m, e):
                rows = rows_of(m * z.TS, z.TS)
                copy(k.x.at[0, rows, :], xb.at[e], si.at[e]).start()
                copy(k.dy.at[0, rows, :], yb.at[e], sj.at[e]).start()

            fetch(0, 0)

            def sent(e):
                done(ab.at[e], so.at[e])

            @pl.loop(0, NS)
            def _(m):
                e = odd(m)
                cols = cols_of(m * z.TS, z.TS)

                @pl.when(m + 1 < NS)
                def _():
                    fetch(m + 1, 1 - e)

                done(xb.at[e], si.at[e])
                done(yb.at[e], sj.at[e])
                a = normed(xb[e])
                A[rows_of(m * z.TS, z.TS), :] = a

                @pl.when(m >= TWO)
                def _():
                    sent(e)

                put_turned(ab.at[e], a)
                copy(ab.at[e], k.ATH.at[0, :, cols], so.at[e]).start()
                k.DHT[:, cols] = yb[e].T

                @pl.when(e == 1)
                def _():
                    tick(lax.div(m, TWO), 0, FOUR)

            sent(0)
            sent(1)

        blocks = [vmem(TWO, z.TS, z.D)] * TWO + [vmem(TWO, z.D, z.TS)]
        pl.run_scoped(body, *blocks, *[dmas(TWO)] * THREE)

    def gate_up(l, A, hook):
        def body(WG, WU, sb, tb, ab, ws, *so):
            kept = ((sb, k.SS), (tb, k.TT), (ab, k.ACT))

            def sent(e):
                for (b, _), sem in zip(kept, so, strict=True):
                    done(b.at[e], sem.at[e])

            def fetch(j, e):
                ready(l, "gu", TWO * j)
                ready(l, "gu", TWO * j + 1)
                load_gu(l, j, WG.at[e], WU.at[e], ws.at[e])

            fetch(0, 0)
            hook(-1, 0)

            @pl.loop(0, NB)
            def _(j):
                slot = odd(j)
                cols = cols_of(j * z.FC, z.FC)
                with jax.named_scope("gu_wait"):
                    done(WG.at[slot], ws.at[slot, 0])
                    done(WU.at[slot], ws.at[slot, 1])

                @pl.loop(0, TWO)
                def _(m):
                    with jax.named_scope("gu_sent"):

                        @pl.when(j > 0)
                        def _():
                            for e in range(TWO):
                                sent(TWO * m + e)

                    with jax.named_scope("gu_dot"):
                        for e in range(TWO):
                            at = TWO * m + e
                            a = A[rows_of(at * z.TM, z.TM), :]
                            gate = nn(a, WG[slot])
                            up = nn(a, WU[slot])
                            sig = lax.logistic(gate)
                            sl = gate * sig
                            sb[at] = sl
                            tb[at] = up * (sig + sl * (1.0 - sig))
                            ab[at] = (sl * up).astype(BF)
                    for e in range(TWO):
                        at = TWO * m + e
                        for (b, to), sem in zip(kept, so, strict=True):
                            copy(b.at[at], to.at[l, rows_of(at * z.TM, z.TM), cols], sem.at[at]).start()

                    with jax.named_scope("gu_tick"):
                        hook(j, m)

                    @pl.when(both(m == 0, j + 1 < NB))
                    def _():
                        with jax.named_scope("gu_fetch"):
                            fetch(j + 1, 1 - slot)

            for e in range(FOUR):
                sent(e)

        weights = [vmem(TWO, z.D, z.FC)] * TWO
        tiles = [vmem(FOUR, z.TM, z.FC, dtype=F32)] * TWO + [vmem(FOUR, z.TM, z.FC)]
        pl.run_scoped(body, *weights, *tiles, dmas(TWO, TWO), *[dmas(FOUR)] * THREE)

    def unit_of_down(n, W, ws):
        ready(0, "d", n)

        @pl.loop(0, NB)
        def _(d):
            rows = rows_of(d * z.FB + n * z.UD, z.UD)

            @pl.when(d == me.s)
            def _():
                copy(k.wd.at[0, rows_of(n * z.UD, z.UD), :], W.at[rows, :], ws.at[0]).start()

            @pl.when(d != me.s)
            def _():
                copy(k.GD.at[0, rows, :], W.at[rows, :], ws.at[0]).start()

    def down(A, W, ws, hook):
        def body(ab, xb, hb, tb, si, sj, so, sp):
            def fetch(m, e):
                rows = rows_of(m * z.TS, z.TS)
                copy(k.ACT.at[0, rows, :], ab.at[e], si.at[e]).start()
                copy(k.x.at[0, rows, :], xb.at[e], sj.at[e]).start()

            fetch(0, 0)
            with jax.named_scope("dn_load"):
                done(W, ws.at[0])

            def fetched(e):
                done(ab.at[e], si.at[e])
                done(xb.at[e], sj.at[e])

            def product(e):
                low = nn(ab[e], W[...]).astype(BF)
                return (xb[e].astype(F32) + low.astype(F32)).astype(BF)

            def finish(m, e):
                a = normed(hb[e])
                A[rows_of(m * z.TS, z.TS), :] = a
                put_turned(tb.at[e], a)

            def send(m):
                e = m % THREE if isinstance(m, int) else lax.rem(m, THREE)
                copy(hb.at[e], k.H1.at[rows_of(m * z.TS, z.TS), :], so.at[e]).start()
                copy(tb.at[e], k.ATH.at[1, :, cols_of(m * z.TS, z.TS)], sp.at[e]).start()

            def sent(e):
                done(hb.at[e], so.at[e])
                done(tb.at[e], sp.at[e])

            fetched(0)
            fetch(1, 1)
            hb[0] = product(0)

            @pl.loop(1, NS)
            def _(m):
                e, now, before = odd(m), lax.rem(m, THREE), lax.rem(m + TWO, THREE)

                @pl.when(m + 1 < NS)
                def _():
                    fetch(m + 1, 1 - e)

                with jax.named_scope("dn_wait"):
                    fetched(e)

                    @pl.when(m >= THREE)
                    def _():
                        sent(now)

                with jax.named_scope("dn_dot"):
                    finish(m - 1, before)
                    hb[now] = product(e)
                send(m - 1)
                with jax.named_scope("dn_tick"):
                    hook(m)

            last = (NS - 1) % THREE
            finish(NS - 1, last)
            send(NS - 1)
            for e in range(THREE):
                sent(e)

        tiles = [vmem(TWO, z.TS, z.F), vmem(TWO, z.TS, z.D), vmem(THREE, z.TS, z.D), vmem(THREE, z.D, z.TS)]
        pl.run_scoped(body, *tiles, *[dmas(TWO)] * TWO, *[dmas(THREE)] * TWO)

    def run(A):
        gather_begin()
        copy(k.dy.at[0], k.DH, k.lsem.at[0]).start()
        with jax.named_scope("turn"):
            turn(A)
        with jax.named_scope("start"):
            for n in range(TWO):
                stage(stage_3, jnp.int32(n), n, n + 1)
        t1 = TWO * LAG + FOUR
        t2 = U1 + TWO * LAG + 1

        def first_layer(W, ws):
            def hook(j, m):
                if isinstance(j, int):
                    for t in range(FOUR, t1 - 1):
                        tick(t, t, t + 1, TWO * LAG if t < t1 - TWO else NB)
                    return

                @pl.when(both(j == 0, m == 0))
                def _():
                    tick(t1 - 1, t1 - 1, t1)

                t = TWO * j + m + t1
                tick(t, t1, t1 + z.NG)
                late = t - (z.NG + TWO * LAG + 1)

                @pl.when(late >= 0)
                def _():
                    unit_of_down(late, W, ws)

            gate_up(0, A, hook)
            with jax.named_scope("dn_ready"):
                for t in range(t1 + z.NG, t2):
                    tick(t, t, t + 1)
                    unit_of_down(t - (z.NG + TWO * LAG + 1), W, ws)
            down(A, W, ws, lambda m: tick(m + t2 - 1, t2, t3))

        t3 = t2 + NS - 1
        pl.run_scoped(first_layer, vmem(z.F, z.D), dmas(1))

        def hook(j, m):
            if not isinstance(j, int):
                tick(TWO * j + m + t3, t3, t3 + z.NG)

        gate_up(1, A, hook)

    def all_there():
        for n in range(z.ND):
            ready(1, "d", n)

    pl.run_scoped(run, vmem(z.T, z.D))
    return all_there, gather_end


def backward(z, me, k, all_there):
    load_gu, load_d = loads_of(z, me, k)
    c, u, v = me.c, me.u, me.v
    RB, FC, HB, PR, TM = z.RB, z.FC, z.HB, z.PR, z.TM
    DR = THREE * RB
    KINDS = range(THREE)

    def place(core, i):
        return i + core * (odd(i) * TWO + lax.div(i, TWO) - i)

    def block_of(g):
        q = lax.rem(g, STEPS)
        b = lax.div(q, THREE)
        return 1 - lax.div(g, STEPS), b, q - THREE * b + lax.div(b, THREE)

    def first_row(b):
        return jnp.minimum(THREE * b, NB - THREE)

    def has(g, n):
        _, b, t = block_of(g)
        inside = both(g >= 0, g < LAST)
        if n == 0:
            return both(inside, either(b < TWO, t > 0))
        return inside if n == 1 else both(inside, t == 0)

    def halves(slot, n):
        rows = pl.ds(n * HB, HB)
        return remote(k.SP.at[rows, :], k.LP.at[slot, rows, :], k.d2ds.at[n], k.d2dr.at[slot, n], me.to_p)

    def block(slot, e):
        return remote(
            k.SP.at[rows_of(odd(e) * DR, DR), :], k.LP.at[slot, rows_of(e * DR, DR), :], k.b2ds.at[odd(e)], k.b2dr.at[slot, e], me.to_p
        )

    def first(slot, n):
        return remote(k.S1.at[slot, n], k.L1.at[slot, n], k.s1s.at[slot, n], k.s1r.at[slot, n], me.to_1)

    def second(slot, n):
        return remote(k.S2.at[slot, n], k.L2.at[slot, n], k.s2s.at[slot, n], k.s2r.at[slot, n], me.to_2)

    def third(slot, n):
        return remote(k.S3.at[slot, n], k.L3.at[slot, n], k.s3s.at[slot, n], k.s3r.at[slot, n], me.to_z)

    def sum_1(g):
        slot = odd(g)
        for n in KINDS:

            @pl.when(has(g - TWO, n))
            def _(n=n):
                second(slot, n).wait_send()

            @pl.when(has(g, n))
            def _(n=n):
                with jax.named_scope("l1"):
                    first(slot, n).wait_recv()
                away, home = rows_of((1 - v) * RB, RB), rows_of(v * RB, RB)
                k.S2[slot, n] = (k.K1[slot, n, away, :] + k.L1[slot, n, away, :].astype(F32)).astype(BF)
                k.K2[slot, n] = k.K1[slot, n, home, :] + k.L1[slot, n, home, :].astype(F32)
                second(slot, n).start()

        pl.semaphore_signal(k.credit, inc=1, device_id=me.to_1, device_id_type=MESH)

    def sum_2(g):
        slot = odd(g)
        for n in KINDS:

            @pl.when(has(g - TWO, n))
            def _(n=n):
                done(k.S3.at[slot, n], k.osem.at[slot, n])

            @pl.when(has(g, n))
            def _(n=n):
                with jax.named_scope("l2"):
                    second(slot, n).wait_recv()
                k.S3[slot, n] = (k.K2[slot, n] + k.L2[slot, n].astype(F32)).astype(BF)
                third(slot, n).start()

    def sum_3(g):
        slot = odd(g)
        l, b, t = block_of(g)
        for n in KINDS:

            @pl.when(has(g, n))
            def _(n=n):
                with jax.named_scope("l3"):
                    third(slot, n).wait()
                k.S3[slot, n] = (k.S3[slot, n].astype(F32) + k.L3[slot, n].astype(F32)).astype(BF)

                @pl.when(t == 0)
                def _():
                    copy(k.S3.at[slot, n], k.dwdt.at[l, rows_of((first_row(b) + n) * RB, RB), :], k.osem.at[slot, n]).start()

                if n < TWO:

                    @pl.when(t > 0)
                    def _():
                        to = (k.dwg, k.dwu)[n].at[l, :, cols_of((TWO * b + t - 1) * FC, FC)]
                        copy(k.S3.at[slot, n], to, k.osem.at[slot, n]).start()

    def sums(g):
        for lag, fn in ((FOUR, sum_3), (THREE, sum_2), (TWO, sum_1)):

            @pl.when(both(g >= lag, g < LAST + lag))
            def _(lag=lag, fn=fn):
                fn(g - lag)

    def first_sent(g):
        for n in KINDS:

            @pl.when(has(g, n))
            def _(n=n):
                first(odd(g), n).wait_send()

    def slots_free(g):
        first_sent(g - TWO)

        @pl.when(g >= TWO)
        def _():
            pl.semaphore_wait(k.credit, 1)

    def layer(it, AT, DA):
        l = 1 - it
        copy(k.ATH.at[l], AT, k.lsem.at[0]).start()

        def body(WG, WU, WD, stb, DGU, ws, si, sj, sa):
            def fetch(i):
                rows, cols = rows_of(lax.rem(i, FOUR) * TM, TM), cols_of(lax.div(i, FOUR) * FC, FC)
                e = lax.rem(i, THREE)
                copy(k.SS.at[l, rows, cols], stb.at[0, e], si.at[e]).start()
                copy(k.TT.at[l, rows, cols], stb.at[1, e], sj.at[e]).start()

            def column(q):
                theirs, own = lax.rem(TWO * (1 - v) + q, FOUR), lax.rem(TWO * (1 - u) + q, FOUR)
                return jnp.where(q < FOUR, TWO * place(1 - c, theirs) + 1 - c, TWO * place(c, own) + c)

            def fetch_act(q):
                e = lax.rem(q + TWO, THREE)
                copy(k.ACT.at[l, :, cols_of(column(q) * FC, FC)], DGU.at[e], sa.at[e]).start()

            load_gu(l, jnp.int32(0), WG, WU, ws)
            fetch_act(jnp.int32(0))
            fetch(jnp.int32(0))
            fetch(jnp.int32(1))

            @pl.loop(0, FOUR)
            def _(m):
                DA[rows_of(m * TM, TM), :] = jnp.zeros((TM, z.D), F32)

            with jax.named_scope("at_wait"):
                done(AT, k.lsem.at[0])

            def product(b, q):
                e = lax.rem(q + TWO, THREE)

                @pl.when(both(q > 0, q + TWO < NB))
                def _():
                    fetch_act(q + TWO)

                with jax.named_scope("act_wait"):
                    done(DGU.at[e], sa.at[e])
                return nn(k.DHT[rows_of(first_row(b) * RB, DR), :], DGU[e])

            def down_step(b, g):
                slot = odd(g)
                fetch_act(jnp.int32(1))
                fetch_act(jnp.int32(TWO))

                with jax.named_scope("d_theirs"):
                    @pl.loop(0, FOUR)
                    def _(e):
                        val = product(b, e).astype(BF)

                        @pl.when(e >= TWO)
                        def _():
                            block(slot, e - TWO).wait_send()

                        k.SP[rows_of(odd(e) * DR, DR), :] = val
                        block(slot, e).start()

                with jax.named_scope("slots"):
                    slots_free(g)

                with jax.named_scope("d_ours"):
                    @pl.loop(0, TWO)
                    def _(e):
                        block(slot, e).wait_recv()
                        val = (product(b, e + FOUR) + k.LP[slot, rows_of(e * DR, DR), :].astype(F32)).astype(BF)
                        for n in KINDS:
                            k.S1[slot, n, rows_of(e * RB, RB), :] = val[n * RB : (n + 1) * RB]

                for n in KINDS:

                    @pl.when(has(g, n))
                    def _(n=n):
                        first(slot, n).start()

                with jax.named_scope("d_keep"):
                    @pl.loop(0, TWO)
                    def _(e):
                        block(slot, e + TWO).wait_recv()
                        val = product(b, e + FOUR + TWO) + k.LP[slot, rows_of((e + TWO) * DR, DR), :].astype(F32)
                        for n in KINDS:
                            k.K1[slot, n, rows_of(e * RB, RB), :] = val[n * RB : (n + 1) * RB]

                for e in range(TWO):
                    block(slot, e).wait_send()

                @pl.when(b == 0)
                def _():
                    @pl.when(it == 0)
                    def _():
                        all_there()

                    load_d(l, jnp.int32(0), WD, ws.at[TWO])

            def gate_up_step(j, g):
                slot = odd(g)
                with jax.named_scope("wd_wait"):
                    done(WD, ws.at[TWO])

                @pl.loop(0, FOUR)
                def _(m):
                    i = j * FOUR + m
                    e = lax.rem(i, THREE)
                    rows = rows_of(m * TM, TM)

                    @pl.when(i + TWO < FOUR * NB)
                    def _():
                        fetch(i + TWO)

                    with jax.named_scope("st_wait"):
                        done(stb.at[0, e], si.at[e])
                        done(stb.at[1, e], sj.at[e])
                    with jax.named_scope("a_dot"):
                        dact = nt(k.DH[rows, :], WD[...]).astype(BF).astype(F32)
                        DGU[0, rows, :] = (dact * stb[1, e]).astype(BF)
                        DGU[1, rows, :] = (dact * stb[0, e]).astype(BF)

                @pl.when(j + 1 < NB)
                def _():
                    load_d(l, j + 1, WD, ws.at[TWO])

                with jax.named_scope("b_dot"):
                    for n in range(TWO):
                        k.SP[n * HB : (n + 1) * HB, :] = nn(AT[rows_of((1 - c) * HB, HB), :], DGU[n]).astype(BF)
                        halves(slot, n).start()
                with jax.named_scope("slots"):
                    slots_free(g)
                out, keep = TWO * (1 - u) * RB, TWO * u * RB
                for n in range(TWO):
                    with jax.named_scope("half_wait"):
                        halves(slot, n).wait_recv()
                    k.S1[slot, n] = (
                        nn(AT[rows_of(c * HB + out, PR), :], DGU[n]) + k.LP[slot, rows_of(n * HB + out, PR), :].astype(F32)
                    ).astype(BF)
                    k.K1[slot, n] = nn(AT[rows_of(c * HB + keep, PR), :], DGU[n]) + k.LP[slot, rows_of(n * HB + keep, PR), :].astype(F32)
                    first(slot, n).start()
                with jax.named_scope("w_wait"):
                    done(WG, ws.at[0])
                    done(WU, ws.at[1])

                with jax.named_scope("da"):
                    @pl.loop(0, FOUR)
                    def _(m):
                        rows = rows_of(m * TM, TM)
                        DA[rows, :] += nt(DGU[0, rows, :], WG[...]) + nt(DGU[1, rows, :], WU[...])

                @pl.when(j + 1 < NB)
                def _():
                    load_gu(l, j + 1, WG, WU, ws)

                @pl.when(both(lax.rem(j, TWO) == 1, j + TWO + 1 < NB))
                def _():
                    fetch_act(jnp.int32(0))

                for n in range(TWO):
                    halves(slot, n).wait_send()

            @pl.loop(0, STEPS)
            def _(q):
                g = it * STEPS + q
                _, b, t = block_of(g)
                with jax.named_scope("sums"):
                    sums(g)

                @pl.when(t == 0)
                def _():
                    down_step(b, g)

                @pl.when(t > 0)
                def _():
                    gate_up_step(TWO * b + t - 1, g)

        weights = [vmem(z.D, FC)] * TWO + [vmem(z.FB, z.D)]
        tiles = [vmem(TWO, THREE, TM, FC, dtype=F32), vmem(THREE, z.T, FC)]
        pl.run_scoped(body, *weights, *tiles, *[dmas(THREE)] * FOUR)
        with jax.named_scope("norm"):
            norm_back(l, DA)

    def norm_back(l, DA):
        def body(hb, ob, si, so):
            def fetch(m, e):
                rows = rows_of(m * z.TS, z.TS)

                @pl.when(l == 1)
                def _():
                    copy(k.H1.at[rows, :], hb.at[e], si.at[e]).start()

                @pl.when(l == 0)
                def _():
                    copy(k.x.at[0, rows, :], hb.at[e], si.at[e]).start()

            fetch(jnp.int32(0), 0)

            @pl.loop(0, NB)
            def _(m):
                e = odd(m)
                rows = rows_of(m * z.TS, z.TS)

                @pl.when(m + 1 < NB)
                def _():
                    fetch(m + 1, 1 - e)

                done(hb.at[e], si.at[e])

                @pl.when(both(l == 0, lax.rem(m, FOUR) == 0))
                def _():
                    with jax.named_scope("norm_sums"):
                        sums(LAST + lax.div(m, FOUR))

                @pl.when(both(l == 0, m >= TWO))
                def _():
                    done(ob.at[e], so.at[e])

                wide = hb[e].astype(F32)
                da = DA[rows, :].astype(BF).astype(F32)
                scale = lax.rsqrt(jnp.mean(wide * wide, -1, keepdims=True) + 1e-6)
                along = jnp.mean(da * wide, -1, keepdims=True)
                dn = (da * scale - wide * (along * scale * scale * scale)).astype(BF)
                new = (k.DH[rows, :].astype(F32) + dn.astype(F32)).astype(BF)
                k.DH[rows, :] = new
                ob[e] = new

                @pl.when(l == 1)
                def _():
                    k.DHT[:, cols_of(m * z.TS, z.TS)] = ob[e].T

                @pl.when(l == 0)
                def _():
                    copy(ob.at[e], k.dx.at[0, rows, :], so.at[e]).start()

            @pl.when(l == 0)
            def _():
                for e in range(TWO):
                    done(ob.at[e], so.at[e])

        pl.run_scoped(body, *[vmem(TWO, z.TS, z.D)] * TWO, *[dmas(TWO)] * TWO)

    done(k.DH, k.lsem.at[0])

    @pl.loop(0, TWO)
    def _(it):
        pl.run_scoped(functools.partial(layer, it), vmem(z.D, z.T), vmem(z.T, z.D, dtype=F32))

    def turn_back(ib, ob, si, so):
        for l in range(TWO):
            copy(k.dwdt.at[l], ib.at[l], si.at[l]).start()
        with jax.named_scope("tail"):
            sums(jnp.int32(LAST + TWO))
        with jax.named_scope("turn_back"):
            for l in range(TWO):
                done(ib.at[l], si.at[l])
                ob[l] = ib[l].T
                copy(ob.at[l], k.dwd.at[l], so.at[l]).start()
        with jax.named_scope("tail"):
            sums(jnp.int32(LAST + THREE))
        for l in range(TWO):
            done(ob.at[l], so.at[l])

    pl.run_scoped(turn_back, vmem(TWO, z.D, z.FB), vmem(TWO, z.FB, z.D), dmas(TWO), dmas(TWO))

    for g in (LAST - TWO, LAST - 1):
        first_sent(jnp.int32(g))
        for n in range(TWO):
            second(g % TWO, n).wait_send()
            done(k.S3.at[g % TWO, n], k.osem.at[g % TWO, n])
    pl.semaphore_wait(k.credit, TWO)


class Refs:
    def __init__(self, names, refs):
        for name, ref in zip(names, refs, strict=True):
            setattr(self, name, ref)


def call(name, z, fn, number, ins, outs, scratch, flops):
    names = [*ins, *outs, *scratch]

    def kernel(*refs):
        me, k = Here(), Refs(names, refs)
        me.meet()
        fn(z, me, k)

    hbm = pl.BlockSpec(memory_space=pl.ANY)
    made = pl.pallas_call(
        kernel,
        out_shape=[jax.ShapeDtypeStruct(*spec) for spec in outs.values()],
        in_specs=[hbm] * len(ins),
        out_specs=[hbm] * len(outs),
        scratch_shapes=list(scratch.values()),
        compiler_params=pltpu.CompilerParams(collective_id=number, has_side_effects=True, vmem_limit_bytes=67043328),
        cost_estimate=pl.CostEstimate(flops=flops, bytes_accessed=1 << 28, transcendentals=0),
        name=name,
    )(*ins.values())
    return dict(zip(outs, made, strict=True))


def solution(mesh):
    def step(x, dy, wg, wu, wd):
        _, T, D = x.shape
        F = wg.shape[TWO]
        z = Sizes(T, D, F)
        RB, FB, FC, L = z.RB, z.FB, z.FC, TWO
        ins = {"x": x, "dy": dy, "wg": wg, "wu": wu, "wd": wd}
        kept = {
            **{name: ((L, D, F), BF) for name in ("GG", "GU")},
            "GD": ((L, F, D), BF),
            **{name: ((L, T, F), F32) for name in ("SS", "TT")},
            "ACT": ((L, T, F), BF),
            "H1": ((T, D), BF),
            "ATH": ((L, D, T), BF),
            "dwdt": ((L, D, FB), BF),
        }
        results = {
            "dx": ((1, T, D), BF),
            **{name: ((L, RB, F), BF) for name in ("dwg", "dwu")},
            "dwd": ((L, FB, D), BF),
        }
        gather = {name: dmas(z.UNITS) for name in ("gsx", "gsy", "gsz", "gsp", "grx", "gry", "grz", "grp")}
        item, pair = (TWO, THREE, RB, FC), (TWO, THREE, z.PR, FC)
        sums = {
            "DH": vmem(T, D),
            "DHT": vmem(D, T),
            "SP": vmem(TWO * z.HB, FC),
            "LP": vmem(TWO, THREE * z.HB, FC),
            **{name: vmem(*pair) for name in ("S1", "L1")},
            "K1": vmem(*pair, dtype=F32),
            **{name: vmem(*item) for name in ("S2", "L2", "S3", "L3")},
            "K2": vmem(*item, dtype=F32),
            "d2ds": dmas(TWO),
            "d2dr": dmas(TWO, TWO),
            "b2ds": dmas(TWO),
            "b2dr": dmas(TWO, FOUR),
            **{name: dmas(TWO, THREE) for name in ("s1s", "s1r", "s2s", "s2r", "s3s", "s3r", "osem")},
            "credit": pltpu.SemaphoreType.REGULAR,
            "lsem": dmas(1),
        }
        flops = TWO * T * D * F

        def whole(z, me, k):
            all_there, gather_end = forward(z, me, k)
            backward(z, me, k, all_there)
            gather_end()

        made = call("whole", z, whole, 0, ins, {**results, **kept}, {**gather, **sums}, flops * (STEPS + FOUR + TWO))
        return made["dx"], made["dwg"], made["dwu"], made["dwd"]

    states, cut = P(("rep", "r", "s"), None, None), P(None, "s", None)
    return jax.shard_map(
        step,
        mesh=mesh,
        in_specs=(states, states, cut, cut, cut),
        out_specs=(states, *[P("rep", "s", None)] * THREE),
        check_vma=False,
    )
```

```python
import functools

import jax
import jax.numpy as jnp
from jax import lax
from jax.experimental import pallas as pl
from jax.experimental.pallas import tpu as pltpu
from jax.sharding import PartitionSpec as P

MESH = pl.DeviceIdType.MESH
BF, F32 = jnp.bfloat16, jnp.float32
NB = 8
LEAD = 8
LAG = 2
TWO, THREE, FOUR = 2, 3, 4
STEPS = 11
LAST = TWO * STEPS


def nn(a, b):
    return lax.dot_general(a, b, (((1,), (0,)), ((), ())), preferred_element_type=F32)


def nt(a, b):
    return lax.dot_general(a, b, (((1,), (1,)), ((), ())), preferred_element_type=F32)


def rows_of(start, size):
    return pl.ds(start if isinstance(start, int) else pl.multiple_of(start, 16), size)


def cols_of(start, size):
    return pl.ds(start if isinstance(start, int) else pl.multiple_of(start, 128), size)


def odd(i):
    return lax.rem(i, TWO)


def copy(src, dst, sem):
    return pltpu.make_async_copy(src, dst, sem)


def done(ref, sem):
    pltpu.make_async_copy(ref, ref, sem).wait()


def both(a, b):
    return jnp.logical_and(a, b)


def either(a, b):
    return jnp.logical_or(a, b)


def vmem(*shape, dtype=BF):
    return pltpu.VMEM(shape, dtype)


def dmas(*shape):
    return pltpu.SemaphoreType.DMA(shape)


class Sizes:
    def __init__(self, T, D, F):
        self.T, self.D, self.F = T, D, F
        self.RB, self.FB, self.HB = D // NB, F // NB, D // TWO
        self.FC = self.FB
        self.UC, self.UD = self.FC // TWO, self.FB // NB
        self.NG, self.ND = F // self.UC, NB
        self.TM, self.TS = T // FOUR, T // NB
        self.PR = TWO * self.RB
        self.UNITS = TWO * (self.NG + self.ND)


class Here:
    def __init__(self):
        self.r, self.s = lax.axis_index("r"), lax.axis_index("s")
        rep, r, s = lax.axis_index("rep"), self.r, self.s
        self.c = c = odd(s)
        y, x = odd(lax.div(s, TWO)), lax.div(s, FOUR)
        self.x, self.y = x, y
        self.xn, self.yn, partner = s + FOUR - NB * x, s + TWO - FOUR * y, s + 1 - TWO * c
        self.partner = partner
        self.far = self.xn + self.yn - s
        self.over = self.yn + c * (self.xn - self.yn)
        self.u, self.v = x + c * (y - x), y + c * (x - y)
        n1 = self.xn + c * (self.yn - self.xn)
        n2 = self.xn + self.yn - n1
        self.to_p, self.to_x, self.to_y, self.to_z = (rep, r, partner), (rep, r, self.xn), (rep, r, self.yn), (rep, 1 - r, s)
        self.to_1, self.to_2 = (rep, r, n1), (rep, r, n2)
        self.z0, self.z1, self.c0, self.c1 = r == 0, r == 1, c == 0, c == 1

    def meet(self):
        barrier = pltpu.get_barrier_semaphore()
        for dev in (self.to_p, self.to_x, self.to_y, self.to_z):
            pl.semaphore_signal(barrier, inc=1, device_id=dev, device_id_type=MESH)
        pl.semaphore_wait(barrier, FOUR)


def remote(src, dst, ss, rs, dev):
    return pltpu.make_async_remote_copy(src, dst, ss, rs, device_id=dev, device_id_type=MESH)


def normed(h):
    wide = h.astype(F32)
    scale = lax.rsqrt(jnp.mean(wide * wide, -1, keepdims=True) + 1e-6)
    return (wide * scale).astype(BF)


def gather_of(z, me, k):
    segments = (
        (0, z.NG, "gu", 0),
        (z.NG, z.ND, "d", 0),
        (z.NG + z.ND, z.NG, "gu", 1),
        (z.UNITS - z.ND, z.ND, "d", 1),
    )

    def held(kind, l, n, d):
        if kind == "gu":
            return [G.at[l, rows_of(d * z.RB, z.RB), cols_of(n * z.UC, z.UC)] for G in (k.GG, k.GU)]
        return [k.GD.at[l, rows_of(d * z.FB + n * z.UD, z.UD), :]]

    def mine(kind, l, n):
        if kind == "gu":
            return [w.at[l, :, cols_of(n * z.UC, z.UC)] for w in (k.wg, k.wu)]
        return [k.wd.at[l, rows_of(n * z.UD, z.UD), :]]

    def got(kind, l, n, sem):
        done(k.GG.at[l, pl.ds(0, n * z.PR), pl.ds(0, z.UC)] if kind == "gu" else k.GD.at[l, pl.ds(0, n * z.UD), :], sem)

    def push(srcs, dsts, ss, rs, i, dev):
        for a, b in zip(srcs, dsts, strict=True):
            remote(a, b, ss.at[i], rs.at[i], dev).start()

    def pass_on(ref, i):
        push(ref, ref, k.gsp, k.grp, i, me.to_p)

    def stage_own(kind, l, n, i):
        own, there = mine(kind, l, n), held(kind, l, n, me.s)

        @pl.when(either(me.z0, me.c0))
        def _():
            push(own, there, k.gsx, k.grx, i, me.to_x)

        @pl.when(either(me.z0, me.c1))
        def _():
            push(own, there, k.gsy, k.gry, i, me.to_y)

        push(own, there, k.gsp, k.grp, i, me.to_p)

    def stage_1(kind, l, n, i):
        hx, hy = held(kind, l, n, me.xn), held(kind, l, n, me.yn)

        @pl.when(either(me.z0, me.c0))
        def _():
            got(kind, l, 1, k.grx.at[i])

        @pl.when(either(me.z0, me.c1))
        def _():
            got(kind, l, 1, k.gry.at[i])

        @pl.when(me.z0)
        def _():
            on = held(kind, l, n, me.over)
            push(on, on, k.gsz, k.grz, i, me.to_z)
            pass_on(hx, i)
            pass_on(hy, i)

        @pl.when(both(me.z1, me.c0))
        def _():
            push(hx, hx, k.gsy, k.gry, i, me.to_y)
            pass_on(hx, i)

        @pl.when(both(me.z1, me.c1))
        def _():
            push(hy, hy, k.gsx, k.grx, i, me.to_x)
            pass_on(hy, i)

    def stage_2(kind, l, n, i):
        @pl.when(me.z1)
        def _():
            far, over = held(kind, l, n, me.far), held(kind, l, n, me.over)

            @pl.when(me.c0)
            def _():
                got(kind, l, 1, k.gry.at[i])

            @pl.when(me.c1)
            def _():
                got(kind, l, 1, k.grx.at[i])

            push(far, far, k.gsz, k.grz, i, me.to_z)
            pass_on(far, i)
            got(kind, l, 1, k.grz.at[i])
            pass_on(over, i)

    def stage_3(kind, l, n, i):
        @pl.when(me.z0)
        def _():
            got(kind, l, 1, k.grz.at[i])
            pass_on(held(kind, l, n, me.far), i)

    def stage(fn, i, low, high):
        for start, n, kind, l in segments:
            a, b = max(start, low), min(start + n, high)
            if a < b:

                @pl.when(both(i >= a, i < b))
                def _(kind=kind, l=l, start=start):
                    fn(kind, l, i - start, i)

    def tick(t, low, high, most=NB):
        t = jnp.asarray(t, jnp.int32)
        stage(stage_own, t + LEAD, low + LEAD, high + LEAD)
        for lag, fn in ((TWO * LAG, stage_3), (LAG, stage_2), (0, stage_1)):
            if lag < most:
                stage(fn, t - lag, max(0, low - lag), min(z.UNITS, high - lag))

    def ready(l, kind, n):
        start = next(a for a, _, kd, ll in segments if kd == kind and ll == l)
        got(kind, l, FOUR, k.grp.at[start + n])

    def begin():
        @pl.loop(0, LEAD)
        def _(i):
            stage(stage_own, i, 0, LEAD)

    def end():
        for start, n, kind, l in segments:

            @pl.loop(0, n)
            def _(i, start=start, kind=kind, l=l):
                for sem in (k.gsx, k.gsy, k.gsz):
                    got(kind, l, 1, sem.at[start + i])
                got(kind, l, FOUR, k.gsp.at[start + i])

    return tick, ready, begin, end, stage, stage_3


def loads_of(z, me, k):
    def load_gu(l, j, WG, WU, sems):
        cols = cols_of(j * z.FC, z.FC)
        others = ((FOUR * (1 - me.x), FOUR), (FOUR * me.x + TWO * (1 - me.y), TWO), (me.partner, 1))
        for n, (W, own, G) in enumerate(((WG, k.wg, k.GG), (WU, k.wu, k.GU))):
            copy(own.at[l, :, cols], W.at[rows_of(me.s * z.RB, z.RB), :], sems.at[n]).start()
            for d, size in others:
                rows = rows_of(d * z.RB, size * z.RB)
                copy(G.at[l, rows, cols], W.at[rows, :], sems.at[n]).start()

    def load_d(l, j, W, sem):
        @pl.when(j == me.s)
        def _():
            copy(k.wd.at[l], W, sem).start()

        @pl.when(j != me.s)
        def _():
            copy(k.GD.at[l, rows_of(j * z.FB, z.FB), :], W, sem).start()

    return load_gu, load_d


def forward(z, me, k):
    tick, ready, gather_begin, gather_end, stage, stage_3 = gather_of(z, me, k)
    load_gu, load_d = loads_of(z, me, k)
    NS, U1 = NB, z.NG + z.ND

    def put_turned(ref, a):
        turned = a.T
        for d in range(NB):
            core, px, py = d % TWO, d // FOUR, (d // TWO) % TWO
            i = TWO * px + py if core == 0 else TWO * py + px
            ref[core * z.HB + i * z.RB : core * z.HB + (i + 1) * z.RB, :] = turned[d * z.RB : (d + 1) * z.RB, :]

    def turn(A):
        def body(xb, yb, ab, bb, si, sj, so, sp):
            def fetch(m, e):
                rows = rows_of(m * z.TS, z.TS)
                copy(k.x.at[0, rows, :], xb.at[e], si.at[e]).start()
                copy(k.dy.at[0, rows, :], yb.at[e], sj.at[e]).start()

            fetch(0, 0)

            def sent(e):
                done(ab.at[e], so.at[e])
                done(bb.at[e], sp.at[e])

            @pl.loop(0, NS)
            def _(m):
                e = odd(m)
                cols = cols_of(m * z.TS, z.TS)

                @pl.when(m + 1 < NS)
                def _():
                    fetch(m + 1, 1 - e)

                done(xb.at[e], si.at[e])
                done(yb.at[e], sj.at[e])
                a = normed(xb[e])
                A[rows_of(m * z.TS, z.TS), :] = a

                @pl.when(m >= TWO)
                def _():
                    sent(e)

                put_turned(ab.at[e], a)
                bb[e] = yb[e].T
                copy(ab.at[e], k.ATH.at[0, :, cols], so.at[e]).start()
                copy(bb.at[e], k.DHTH.at[1, :, cols], sp.at[e]).start()

                @pl.when(e == 1)
                def _():
                    tick(lax.div(m, TWO), 0, FOUR)

            sent(0)
            sent(1)

        blocks = [vmem(TWO, z.TS, z.D)] * TWO + [vmem(TWO, z.D, z.TS)] * TWO
        pl.run_scoped(body, *blocks, *[dmas(TWO)] * FOUR)

    def gate_up(l, A, hook):
        def body(WG, WU, sb, tb, ab, ws, *so):
            kept = ((sb, k.SS), (tb, k.TT), (ab, k.ACT))

            def sent(e):
                for (b, _), sem in zip(kept, so, strict=True):
                    done(b.at[e], sem.at[e])

            def fetch(j, e):
                ready(l, "gu", TWO * j)
                ready(l, "gu", TWO * j + 1)
                load_gu(l, j, WG.at[e], WU.at[e], ws.at[e])

            fetch(0, 0)
            hook(-1, 0)

            @pl.loop(0, NB)
            def _(j):
                slot = odd(j)
                cols = cols_of(j * z.FC, z.FC)
                with jax.named_scope("gu_wait"):
                    done(WG.at[slot], ws.at[slot, 0])
                    done(WU.at[slot], ws.at[slot, 1])

                @pl.loop(0, TWO)
                def _(m):
                    with jax.named_scope("gu_sent"):

                        @pl.when(j > 0)
                        def _():
                            for e in range(TWO):
                                sent(TWO * m + e)

                    with jax.named_scope("gu_dot"):
                        for e in range(TWO):
                            at = TWO * m + e
                            a = A[rows_of(at * z.TM, z.TM), :]
                            gate = nn(a, WG[slot])
                            up = nn(a, WU[slot])
                            sig = lax.logistic(gate)
                            sl = gate * sig
                            sb[at] = sl
                            tb[at] = up * (sig + sl * (1.0 - sig))
                            ab[at] = (sl * up).astype(BF)
                    for e in range(TWO):
                        at = TWO * m + e
                        for (b, to), sem in zip(kept, so, strict=True):
                            copy(b.at[at], to.at[l, rows_of(at * z.TM, z.TM), cols], sem.at[at]).start()

                    with jax.named_scope("gu_tick"):
                        hook(j, m)

                    @pl.when(both(m == 0, j + 1 < NB))
                    def _():
                        with jax.named_scope("gu_fetch"):
                            fetch(j + 1, 1 - slot)

            for e in range(FOUR):
                sent(e)

        weights = [vmem(TWO, z.D, z.FC)] * TWO
        tiles = [vmem(FOUR, z.TM, z.FC, dtype=F32)] * TWO + [vmem(FOUR, z.TM, z.FC)]
        pl.run_scoped(body, *weights, *tiles, dmas(TWO, TWO), *[dmas(FOUR)] * THREE)

    def unit_of_down(n, W, ws):
        ready(0, "d", n)

        @pl.loop(0, NB)
        def _(d):
            rows = rows_of(d * z.FB + n * z.UD, z.UD)

            @pl.when(d == me.s)
            def _():
                copy(k.wd.at[0, rows_of(n * z.UD, z.UD), :], W.at[rows, :], ws.at[0]).start()

            @pl.when(d != me.s)
            def _():
                copy(k.GD.at[0, rows, :], W.at[rows, :], ws.at[0]).start()

    def down(A, W, ws, hook):
        def body(ab, xb, hb, tb, si, sj, so, sp):
            def fetch(m, e):
                rows = rows_of(m * z.TS, z.TS)
                copy(k.ACT.at[0, rows, :], ab.at[e], si.at[e]).start()
                copy(k.x.at[0, rows, :], xb.at[e], sj.at[e]).start()

            fetch(0, 0)
            with jax.named_scope("dn_load"):
                done(W, ws.at[0])

            def fetched(e):
                done(ab.at[e], si.at[e])
                done(xb.at[e], sj.at[e])

            def product(e):
                low = nn(ab[e], W[...]).astype(BF)
                return (xb[e].astype(F32) + low.astype(F32)).astype(BF)

            def finish(m, e):
                a = normed(hb[e])
                A[rows_of(m * z.TS, z.TS), :] = a
                put_turned(tb.at[e], a)

            def send(m):
                e = m % THREE if isinstance(m, int) else lax.rem(m, THREE)
                copy(hb.at[e], k.H1.at[rows_of(m * z.TS, z.TS), :], so.at[e]).start()
                copy(tb.at[e], k.ATH.at[1, :, cols_of(m * z.TS, z.TS)], sp.at[e]).start()

            def sent(e):
                done(hb.at[e], so.at[e])
                done(tb.at[e], sp.at[e])

            fetched(0)
            fetch(1, 1)
            hb[0] = product(0)

            @pl.loop(1, NS)
            def _(m):
                e, now, before = odd(m), lax.rem(m, THREE), lax.rem(m + TWO, THREE)

                @pl.when(m + 1 < NS)
                def _():
                    fetch(m + 1, 1 - e)

                with jax.named_scope("dn_wait"):
                    fetched(e)

                    @pl.when(m >= THREE)
                    def _():
                        sent(now)

                with jax.named_scope("dn_dot"):
                    finish(m - 1, before)
                    hb[now] = product(e)
                send(m - 1)
                with jax.named_scope("dn_tick"):
                    hook(m)

            last = (NS - 1) % THREE
            finish(NS - 1, last)
            send(NS - 1)
            for e in range(THREE):
                sent(e)

        tiles = [vmem(TWO, z.TS, z.F), vmem(TWO, z.TS, z.D), vmem(THREE, z.TS, z.D), vmem(THREE, z.D, z.TS)]
        pl.run_scoped(body, *tiles, *[dmas(TWO)] * TWO, *[dmas(THREE)] * TWO)

    def run(A):
        gather_begin()
        copy(k.dy.at[0], k.DH, k.lsem.at[0]).start()
        with jax.named_scope("turn"):
            turn(A)
        with jax.named_scope("start"):
            for n in range(TWO):
                stage(stage_3, jnp.int32(n), n, n + 1)
        t1 = TWO * LAG + FOUR
        t2 = U1 + TWO * LAG + 1

        def first_layer(W, ws):
            def hook(j, m):
                if isinstance(j, int):
                    for t in range(FOUR, t1 - 1):
                        tick(t, t, t + 1, TWO * LAG if t < t1 - TWO else NB)
                    return

                @pl.when(both(j == 0, m == 0))
                def _():
                    tick(t1 - 1, t1 - 1, t1)

                t = TWO * j + m + t1
                tick(t, t1, t1 + z.NG)
                late = t - (z.NG + TWO * LAG + 1)

                @pl.when(late >= 0)
                def _():
                    unit_of_down(late, W, ws)

            gate_up(0, A, hook)
            with jax.named_scope("dn_ready"):
                for t in range(t1 + z.NG, t2):
                    tick(t, t, t + 1)
                    unit_of_down(t - (z.NG + TWO * LAG + 1), W, ws)
            down(A, W, ws, lambda m: tick(m + t2 - 1, t2, t3))

        t3 = t2 + NS - 1
        pl.run_scoped(first_layer, vmem(z.F, z.D), dmas(1))

        def hook(j, m):
            if not isinstance(j, int):
                tick(TWO * j + m + t3, t3, t3 + z.NG)

        gate_up(1, A, hook)

    def all_there():
        for n in range(z.ND):
            ready(1, "d", n)

    pl.run_scoped(run, vmem(z.T, z.D))
    return all_there, gather_end


def backward(z, me, k, all_there):
    load_gu, load_d = loads_of(z, me, k)
    c, u, v = me.c, me.u, me.v
    RB, FC, HB, PR, TM = z.RB, z.FC, z.HB, z.PR, z.TM
    DR = THREE * RB
    KINDS = range(THREE)

    def place(core, i):
        return i + core * (odd(i) * TWO + lax.div(i, TWO) - i)

    def block_of(g):
        q = lax.rem(g, STEPS)
        b = lax.div(q, THREE)
        return 1 - lax.div(g, STEPS), b, q - THREE * b + lax.div(b, THREE)

    def first_row(b):
        return jnp.minimum(THREE * b, NB - THREE)

    def has(g, n):
        _, b, t = block_of(g)
        inside = both(g >= 0, g < LAST)
        if n == 0:
            return both(inside, either(b < TWO, t > 0))
        return inside if n == 1 else both(inside, t == 0)

    def halves(slot, n):
        rows = pl.ds(n * HB, HB)
        return remote(k.SP.at[rows, :], k.LP.at[slot, rows, :], k.d2ds.at[n], k.d2dr.at[slot, n], me.to_p)

    def block(slot, e):
        return remote(
            k.SP.at[rows_of(odd(e) * DR, DR), :], k.LP.at[slot, rows_of(e * DR, DR), :], k.b2ds.at[odd(e)], k.b2dr.at[slot, e], me.to_p
        )

    def first(slot, n):
        return remote(k.S1.at[slot, n], k.L1.at[slot, n], k.s1s.at[slot, n], k.s1r.at[slot, n], me.to_1)

    def second(slot, n):
        return remote(k.S2.at[slot, n], k.L2.at[slot, n], k.s2s.at[slot, n], k.s2r.at[slot, n], me.to_2)

    def third(slot, n):
        return remote(k.S3.at[slot, n], k.L3.at[slot, n], k.s3s.at[slot, n], k.s3r.at[slot, n], me.to_z)

    def sum_1(g):
        slot = odd(g)
        for n in KINDS:

            @pl.when(has(g - TWO, n))
            def _(n=n):
                second(slot, n).wait_send()

            @pl.when(has(g, n))
            def _(n=n):
                with jax.named_scope("l1"):
                    first(slot, n).wait_recv()
                away, home = rows_of((1 - v) * RB, RB), rows_of(v * RB, RB)
                k.S2[slot, n] = (k.K1[slot, n, away, :] + k.L1[slot, n, away, :].astype(F32)).astype(BF)
                k.K2[slot, n] = k.K1[slot, n, home, :] + k.L1[slot, n, home, :].astype(F32)
                second(slot, n).start()

        pl.semaphore_signal(k.credit, inc=1, device_id=me.to_1, device_id_type=MESH)

    def sum_2(g):
        slot = odd(g)
        for n in KINDS:

            @pl.when(has(g - TWO, n))
            def _(n=n):
                done(k.S3.at[slot, n], k.osem.at[slot, n])

            @pl.when(has(g, n))
            def _(n=n):
                with jax.named_scope("l2"):
                    second(slot, n).wait_recv()
                k.S3[slot, n] = (k.K2[slot, n] + k.L2[slot, n].astype(F32)).astype(BF)
                third(slot, n).start()

    def sum_3(g):
        slot = odd(g)
        l, b, t = block_of(g)
        for n in KINDS:

            @pl.when(has(g, n))
            def _(n=n):
                with jax.named_scope("l3"):
                    third(slot, n).wait()
                k.S3[slot, n] = (k.S3[slot, n].astype(F32) + k.L3[slot, n].astype(F32)).astype(BF)

                @pl.when(t == 0)
                def _():
                    copy(k.S3.at[slot, n], k.dwdt.at[l, rows_of((first_row(b) + n) * RB, RB), :], k.osem.at[slot, n]).start()

                if n < TWO:

                    @pl.when(t > 0)
                    def _():
                        to = (k.dwg, k.dwu)[n].at[l, :, cols_of((TWO * b + t - 1) * FC, FC)]
                        copy(k.S3.at[slot, n], to, k.osem.at[slot, n]).start()

    def sums(g):
        for lag, fn in ((FOUR, sum_3), (THREE, sum_2), (TWO, sum_1)):

            @pl.when(both(g >= lag, g < LAST + lag))
            def _(lag=lag, fn=fn):
                fn(g - lag)

    def first_sent(g):
        for n in KINDS:

            @pl.when(has(g, n))
            def _(n=n):
                first(odd(g), n).wait_send()

    def slots_free(g):
        first_sent(g - TWO)

        @pl.when(g >= TWO)
        def _():
            pl.semaphore_wait(k.credit, 1)

    def layers(AT, DA, WG, WU, WD, stb, DGU, AB, DHB, ws, si, sj, sa, hs, ns, ts):
        TS, TILES, QS = z.TS, FOUR * NB, THREE * NB

        def fetch(i):
            l, n, e = 1 - lax.div(i, TILES), lax.rem(i, TILES), odd(i)
            rows, cols = rows_of(lax.rem(n, FOUR) * TM, TM), cols_of(lax.div(n, FOUR) * FC, FC)
            copy(k.SS.at[l, rows, cols], stb.at[0, e], si.at[e]).start()
            copy(k.TT.at[l, rows, cols], stb.at[1, e], sj.at[e]).start()

        def fetch_act(i):
            l, q, e = 1 - lax.div(i, QS), lax.rem(i, NB), lax.rem(i, THREE)
            theirs, own = lax.rem(TWO * (1 - v) + q, FOUR), lax.rem(TWO * (1 - u) + q, FOUR)
            j = jnp.where(q < FOUR, TWO * place(1 - c, theirs) + 1 - c, TWO * place(c, own) + c)
            copy(k.ACT.at[l, :, cols_of(j * FC, FC)], AB.at[e], sa.at[e]).start()

        def fetch_rows(l, b):
            copy(k.DHTH.at[l, rows_of(first_row(b) * RB, DR), :], DHB, hs.at[0]).start()

        def fetch_turned(l):
            copy(k.ATH.at[l], AT, hs.at[1]).start()

        all_there()
        fetch(jnp.int32(0))
        for n in KINDS:
            fetch_act(jnp.int32(n))
        fetch_rows(1, jnp.int32(0))
        fetch_turned(1)
        done(k.DH, k.lsem.at[0])

        def layer(it):
            l = 1 - it
            load_d(l, jnp.int32(0), WD, ws.at[TWO])
            load_gu(l, jnp.int32(0), WG, WU, ws)

            @pl.loop(0, FOUR)
            def _(m):
                DA[rows_of(m * TM, TM), :] = jnp.zeros((TM, z.D), F32)

            def product(i, keep):
                e = lax.rem(i, THREE)
                with jax.named_scope("act_wait"):
                    done(AB.at[e], sa.at[e])
                keep(nn(DHB[...], AB[e]))

                @pl.when(i + THREE < TWO * QS)
                def _():
                    fetch_act(i + THREE)

            def down_step(b, g):
                slot, i = odd(g), (THREE * it + b) * NB
                with jax.named_scope("rows_wait"):
                    done(DHB, hs.at[0])
                with jax.named_scope("d_theirs"):

                    @pl.loop(0, FOUR)
                    def _(e):
                        @pl.when(e >= TWO)
                        def _():
                            block(slot, e - TWO).wait_send()

                        def keep(val):
                            k.SP[rows_of(odd(e) * DR, DR), :] = val.astype(BF)

                        product(i + e, keep)
                        block(slot, e).start()

                with jax.named_scope("sums"):
                    sums(g)
                with jax.named_scope("slots"):
                    slots_free(g)
                with jax.named_scope("d_ours"):

                    @pl.loop(0, TWO)
                    def _(e):
                        block(slot, e).wait_recv()

                        def keep(val):
                            val = (val + k.LP[slot, rows_of(e * DR, DR), :].astype(F32)).astype(BF)
                            for n in KINDS:
                                k.S1[slot, n, rows_of(e * RB, RB), :] = val[n * RB : (n + 1) * RB]

                        product(i + e + FOUR, keep)

                for n in KINDS:

                    @pl.when(has(g, n))
                    def _(n=n):
                        first(slot, n).start()

                with jax.named_scope("d_keep"):

                    @pl.loop(0, TWO)
                    def _(e):
                        block(slot, e + TWO).wait_recv()

                        def keep(val):
                            val = val + k.LP[slot, rows_of((e + TWO) * DR, DR), :].astype(F32)
                            for n in KINDS:
                                k.K1[slot, n, rows_of(e * RB, RB), :] = val[n * RB : (n + 1) * RB]

                        product(i + e + FOUR + TWO, keep)

                for e in range(TWO):
                    block(slot, e).wait_send()

                @pl.when(b + 1 < THREE)
                def _():
                    fetch_rows(l, b + 1)

            def add_da(rows):
                DA[rows, :] += nt(DGU[0, rows, :], WG[...]) + nt(DGU[1, rows, :], WU[...])

            def weights_there():
                done(WG, ws.at[0])
                done(WU, ws.at[1])

            def gate_up_step(j, g):
                slot = odd(g)
                with jax.named_scope("wd_wait"):
                    done(WD, ws.at[TWO])

                def tiles(before):
                    @pl.loop(0, FOUR)
                    def _(m):
                        i = it * TILES + j * FOUR + m
                        e = odd(i)
                        rows = rows_of(m * TM, TM)

                        @pl.when(i + 1 < TWO * TILES)
                        def _():
                            fetch(i + 1)

                        with jax.named_scope("st_wait"):
                            done(stb.at[0, e], si.at[e])
                            done(stb.at[1, e], sj.at[e])
                        with jax.named_scope("a_dot"):
                            before(rows)
                            dact = nt(k.DH[rows, :], WD[...]).astype(BF).astype(F32)
                            DGU[0, rows, :] = (dact * stb[1, e]).astype(BF)
                            DGU[1, rows, :] = (dact * stb[0, e]).astype(BF)

                @pl.when(j == 0)
                def _():
                    tiles(lambda rows: None)

                @pl.when(j > 0)
                def _():
                    with jax.named_scope("w_wait"):
                        weights_there()
                    tiles(add_da)
                    load_gu(l, j, WG, WU, ws)

                @pl.when(j + 1 < NB)
                def _():
                    load_d(l, j + 1, WD, ws.at[TWO])

                @pl.when(j == 0)
                def _():
                    with jax.named_scope("at_wait"):
                        done(AT, hs.at[1])

                with jax.named_scope("sums"):
                    sums(g)
                with jax.named_scope("b_dot"):
                    for n in range(TWO):
                        k.SP[n * HB : (n + 1) * HB, :] = nn(AT[rows_of((1 - c) * HB, HB), :], DGU[n]).astype(BF)
                        halves(slot, n).start()
                with jax.named_scope("slots"):
                    slots_free(g)
                out, keep = TWO * (1 - u) * RB, TWO * u * RB
                for n in range(TWO):
                    with jax.named_scope("half_wait"):
                        halves(slot, n).wait_recv()
                    with jax.named_scope("c_dot"):
                        k.S1[slot, n] = (
                            nn(AT[rows_of(c * HB + out, PR), :], DGU[n]) + k.LP[slot, rows_of(n * HB + out, PR), :].astype(F32)
                        ).astype(BF)
                        k.K1[slot, n] = nn(AT[rows_of(c * HB + keep, PR), :], DGU[n]) + k.LP[
                            slot, rows_of(n * HB + keep, PR), :
                        ].astype(F32)
                    first(slot, n).start()
                for n in range(TWO):
                    halves(slot, n).wait_send()

            @pl.loop(0, STEPS)
            def _(q):
                g = it * STEPS + q
                _, b, t = block_of(g)

                @pl.when(t == 0)
                def _():
                    down_step(b, g)

                @pl.when(t > 0)
                def _():
                    gate_up_step(TWO * b + t - 1, g)

            def fetch_states(m):
                rows, to = rows_of(m * TS, TS), WD.at[rows_of(odd(m) * TS, TS), :]

                @pl.when(l == 1)
                def _():
                    copy(k.H1.at[rows, :], to, ns.at[odd(m)]).start()

                @pl.when(l == 0)
                def _():
                    copy(k.x.at[0, rows, :], to, ns.at[odd(m)]).start()

            def there(m):
                done(WD.at[rows_of(odd(m) * TS, TS), :], ns.at[odd(m)])

            def norm(m):
                rows = rows_of(m * TS, TS)
                wide = WD[rows_of(odd(m) * TS, TS), :].astype(F32)
                da = DA[rows, :].astype(BF).astype(F32)
                scale = lax.rsqrt(jnp.mean(wide * wide, -1, keepdims=True) + 1e-6)
                along = jnp.mean(da * wide, -1, keepdims=True)
                dn = (da * scale - wide * (along * scale * scale * scale)).astype(BF)
                k.DH[rows, :] = (k.DH[rows, :].astype(F32) + dn.astype(F32)).astype(BF)

            def turned(m):
                return k.SP.at[:, cols_of(odd(m) * TS, TS)]

            def hand_on(m):
                rows, cols = rows_of(m * TS, TS), cols_of(m * TS, TS)

                @pl.when(l == 1)
                def _():
                    @pl.when(m >= TWO)
                    def _():
                        done(turned(m), ts.at[odd(m)])

                    k.SP[:, cols_of(odd(m) * TS, TS)] = k.DH[rows, :].T
                    copy(turned(m), k.DHTH.at[0, :, cols], ts.at[odd(m)]).start()

                @pl.when(l == 0)
                def _():
                    copy(k.DH.at[rows, :], k.dx.at[0, rows, :], ts.at[TWO]).start()

            fetch_states(jnp.int32(0))

            @pl.when(it == 0)
            def _():
                fetch_turned(0)

            with jax.named_scope("norm"):
                weights_there()
                add_da(rows_of(0, TS))

                @pl.loop(1, NB)
                def _(m):
                    @pl.when(both(l == 0, lax.rem(m, THREE) == 1))
                    def _():
                        with jax.named_scope("norm_sums"):
                            sums(LAST + lax.div(m, THREE))

                    fetch_states(m)
                    there(m - 1)
                    with jax.named_scope("norm_dot"):
                        norm(m - 1)
                        add_da(rows_of(m * TS, TS))
                    hand_on(m - 1)

                there(jnp.int32(NB - 1))
                norm(jnp.int32(NB - 1))
                hand_on(jnp.int32(NB - 1))

            @pl.when(l == 1)
            def _():
                for m in range(TWO):
                    done(turned(m), ts.at[m])
                fetch_rows(0, jnp.int32(0))

            @pl.when(l == 0)
            def _():
                done(k.DH, ts.at[TWO])

        @pl.loop(0, TWO)
        def _(it):
            layer(it)

    weights = [vmem(z.D, FC)] * TWO + [vmem(z.FB, z.D)]
    tiles = [vmem(TWO, TWO, TM, FC, dtype=F32), vmem(TWO, z.T, FC), vmem(THREE, z.T, FC), vmem(DR, z.T)]
    pl.run_scoped(
        layers, vmem(z.D, z.T), vmem(z.T, z.D, dtype=F32), *weights, *tiles, *[dmas(THREE)] * FOUR, *[dmas(TWO)] * TWO, dmas(THREE)
    )

    def turn_back(ib, ob, si, so):
        for l in range(TWO):
            copy(k.dwdt.at[l], ib.at[l], si.at[l]).start()
        with jax.named_scope("turn_back"):
            for l in range(TWO):
                done(ib.at[l], si.at[l])
                ob[l] = ib[l].T
                copy(ob.at[l], k.dwd.at[l], so.at[l]).start()
        with jax.named_scope("tail"):
            sums(jnp.int32(LAST + THREE))
        for l in range(TWO):
            done(ob.at[l], so.at[l])

    pl.run_scoped(turn_back, vmem(TWO, z.D, z.FB), vmem(TWO, z.FB, z.D), dmas(TWO), dmas(TWO))

    for g in (LAST - TWO, LAST - 1):
        first_sent(jnp.int32(g))
        for n in range(TWO):
            second(g % TWO, n).wait_send()
            done(k.S3.at[g % TWO, n], k.osem.at[g % TWO, n])
    pl.semaphore_wait(k.credit, TWO)


class Refs:
    def __init__(self, names, refs):
        for name, ref in zip(names, refs, strict=True):
            setattr(self, name, ref)


def call(name, z, fn, number, ins, outs, scratch, flops):
    names = [*ins, *outs, *scratch]

    def kernel(*refs):
        me, k = Here(), Refs(names, refs)
        me.meet()
        fn(z, me, k)

    hbm = pl.BlockSpec(memory_space=pl.ANY)
    made = pl.pallas_call(
        kernel,
        out_shape=[jax.ShapeDtypeStruct(*spec) for spec in outs.values()],
        in_specs=[hbm] * len(ins),
        out_specs=[hbm] * len(outs),
        scratch_shapes=list(scratch.values()),
        compiler_params=pltpu.CompilerParams(collective_id=number, has_side_effects=True, vmem_limit_bytes=67043328),
        cost_estimate=pl.CostEstimate(flops=flops, bytes_accessed=1 << 28, transcendentals=0),
        name=name,
    )(*ins.values())
    return dict(zip(outs, made, strict=True))


def solution(mesh):
    def step(x, dy, wg, wu, wd):
        _, T, D = x.shape
        F = wg.shape[TWO]
        z = Sizes(T, D, F)
        RB, FB, FC, L = z.RB, z.FB, z.FC, TWO
        ins = {"x": x, "dy": dy, "wg": wg, "wu": wu, "wd": wd}
        kept = {
            **{name: ((L, D, F), BF) for name in ("GG", "GU")},
            "GD": ((L, F, D), BF),
            **{name: ((L, T, F), F32) for name in ("SS", "TT")},
            "ACT": ((L, T, F), BF),
            "H1": ((T, D), BF),
            "ATH": ((L, D, T), BF),
            "DHTH": ((L, D, T), BF),
            "dwdt": ((L, D, FB), BF),
        }
        results = {
            "dx": ((1, T, D), BF),
            **{name: ((L, RB, F), BF) for name in ("dwg", "dwu")},
            "dwd": ((L, FB, D), BF),
        }
        gather = {name: dmas(z.UNITS) for name in ("gsx", "gsy", "gsz", "gsp", "grx", "gry", "grz", "grp")}
        item, pair = (TWO, THREE, RB, FC), (TWO, THREE, z.PR, FC)
        sums = {
            "DH": vmem(T, D),
            "SP": vmem(TWO * z.HB, FC),
            "LP": vmem(TWO, THREE * z.HB, FC),
            **{name: vmem(*pair) for name in ("S1", "L1")},
            "K1": vmem(*pair, dtype=F32),
            **{name: vmem(*item) for name in ("S2", "L2", "S3", "L3")},
            "K2": vmem(*item, dtype=F32),
            "d2ds": dmas(TWO),
            "d2dr": dmas(TWO, TWO),
            "b2ds": dmas(TWO),
            "b2dr": dmas(TWO, FOUR),
            **{name: dmas(TWO, THREE) for name in ("s1s", "s1r", "s2s", "s2r", "s3s", "s3r", "osem")},
            "credit": pltpu.SemaphoreType.REGULAR,
            "lsem": dmas(1),
        }
        flops = TWO * T * D * F

        def whole(z, me, k):
            all_there, gather_end = forward(z, me, k)
            backward(z, me, k, all_there)
            gather_end()

        made = call("whole", z, whole, 0, ins, {**results, **kept}, {**gather, **sums}, flops * (STEPS + FOUR + TWO))
        return made["dx"], made["dwg"], made["dwu"], made["dwd"]

    states, cut = P(("rep", "r", "s"), None, None), P(None, "s", None)
    return jax.shard_map(
        step,
        mesh=mesh,
        in_specs=(states, states, cut, cut, cut),
        out_specs=(states, *[P("rep", "s", None)] * THREE),
        check_vma=False,
    )
```

```python
import functools

import jax
import jax.numpy as jnp
from jax import lax
from jax.experimental import pallas as pl
from jax.experimental.pallas import tpu as pltpu
from jax.sharding import PartitionSpec as P

MESH = pl.DeviceIdType.MESH
BF, F32 = jnp.bfloat16, jnp.float32
NB = 8
LEAD = 8
LAG = 2
TWO, THREE, FOUR = 2, 3, 4
STEPS = 11
LAST = TWO * STEPS


def nn(a, b):
    return lax.dot_general(a, b, (((1,), (0,)), ((), ())), preferred_element_type=F32)


def nt(a, b):
    return lax.dot_general(a, b, (((1,), (1,)), ((), ())), preferred_element_type=F32)


def rows_of(start, size):
    return pl.ds(start if isinstance(start, int) else pl.multiple_of(start, 16), size)


def cols_of(start, size):
    return pl.ds(start if isinstance(start, int) else pl.multiple_of(start, 128), size)


def odd(i):
    return lax.rem(i, TWO)


def copy(src, dst, sem):
    return pltpu.make_async_copy(src, dst, sem)


def done(ref, sem):
    pltpu.make_async_copy(ref, ref, sem).wait()


def both(a, b):
    return jnp.logical_and(a, b)


def either(a, b):
    return jnp.logical_or(a, b)


def vmem(*shape, dtype=BF):
    return pltpu.VMEM(shape, dtype)


def dmas(*shape):
    return pltpu.SemaphoreType.DMA(shape)


class Sizes:
    def __init__(self, T, D, F):
        self.T, self.D, self.F = T, D, F
        self.RB, self.FB, self.HB = D // NB, F // NB, D // TWO
        self.FC = self.FB
        self.UC, self.UD = self.FC // TWO, self.FB // NB
        self.NG, self.ND = F // self.UC, NB
        self.TM, self.TS = T // FOUR, T // NB
        self.PR = TWO * self.RB
        self.UNITS = TWO * (self.NG + self.ND)


class Here:
    def __init__(self):
        self.r, self.s = lax.axis_index("r"), lax.axis_index("s")
        rep, r, s = lax.axis_index("rep"), self.r, self.s
        self.c = c = odd(s)
        y, x = odd(lax.div(s, TWO)), lax.div(s, FOUR)
        self.x, self.y = x, y
        self.xn, self.yn, partner = s + FOUR - NB * x, s + TWO - FOUR * y, s + 1 - TWO * c
        self.partner = partner
        self.far = self.xn + self.yn - s
        self.over = self.yn + c * (self.xn - self.yn)
        self.u, self.v = x + c * (y - x), y + c * (x - y)
        n1 = self.xn + c * (self.yn - self.xn)
        n2 = self.xn + self.yn - n1
        self.to_p, self.to_x, self.to_y, self.to_z = (rep, r, partner), (rep, r, self.xn), (rep, r, self.yn), (rep, 1 - r, s)
        self.to_1, self.to_2 = (rep, r, n1), (rep, r, n2)
        self.z0, self.z1, self.c0, self.c1 = r == 0, r == 1, c == 0, c == 1

    def meet(self):
        barrier = pltpu.get_barrier_semaphore()
        for dev in (self.to_p, self.to_x, self.to_y, self.to_z):
            pl.semaphore_signal(barrier, inc=1, device_id=dev, device_id_type=MESH)
        pl.semaphore_wait(barrier, FOUR)


def remote(src, dst, ss, rs, dev):
    return pltpu.make_async_remote_copy(src, dst, ss, rs, device_id=dev, device_id_type=MESH)


def normed(h):
    wide = h.astype(F32)
    scale = lax.rsqrt(jnp.mean(wide * wide, -1, keepdims=True) + 1e-6)
    return (wide * scale).astype(BF)


def gather_of(z, me, k):
    segments = (
        (0, z.NG, "gu", 0),
        (z.NG, z.ND, "d", 0),
        (z.NG + z.ND, z.NG, "gu", 1),
        (z.UNITS - z.ND, z.ND, "d", 1),
    )

    def held(kind, l, n, d):
        if kind == "gu":
            return [G.at[l, rows_of(d * z.RB, z.RB), cols_of(n * z.UC, z.UC)] for G in (k.GG, k.GU)]
        return [k.GD.at[l, rows_of(d * z.FB + n * z.UD, z.UD), :]]

    def mine(kind, l, n):
        if kind == "gu":
            return [w.at[l, :, cols_of(n * z.UC, z.UC)] for w in (k.wg, k.wu)]
        return [k.wd.at[l, rows_of(n * z.UD, z.UD), :]]

    def got(kind, l, n, sem):
        done(k.GG.at[l, pl.ds(0, n * z.PR), pl.ds(0, z.UC)] if kind == "gu" else k.GD.at[l, pl.ds(0, n * z.UD), :], sem)

    def push(srcs, dsts, ss, rs, i, dev):
        for a, b in zip(srcs, dsts, strict=True):
            remote(a, b, ss.at[i], rs.at[i], dev).start()

    def pass_on(ref, i):
        push(ref, ref, k.gsp, k.grp, i, me.to_p)

    def stage_own(kind, l, n, i):
        own, there = mine(kind, l, n), held(kind, l, n, me.s)

        @pl.when(either(me.z0, me.c0))
        def _():
            push(own, there, k.gsx, k.grx, i, me.to_x)

        @pl.when(either(me.z0, me.c1))
        def _():
            push(own, there, k.gsy, k.gry, i, me.to_y)

        push(own, there, k.gsp, k.grp, i, me.to_p)

    def stage_1(kind, l, n, i):
        hx, hy = held(kind, l, n, me.xn), held(kind, l, n, me.yn)

        @pl.when(either(me.z0, me.c0))
        def _():
            got(kind, l, 1, k.grx.at[i])

        @pl.when(either(me.z0, me.c1))
        def _():
            got(kind, l, 1, k.gry.at[i])

        @pl.when(me.z0)
        def _():
            on = held(kind, l, n, me.over)
            push(on, on, k.gsz, k.grz, i, me.to_z)
            pass_on(hx, i)
            pass_on(hy, i)

        @pl.when(both(me.z1, me.c0))
        def _():
            push(hx, hx, k.gsy, k.gry, i, me.to_y)
            pass_on(hx, i)

        @pl.when(both(me.z1, me.c1))
        def _():
            push(hy, hy, k.gsx, k.grx, i, me.to_x)
            pass_on(hy, i)

    def stage_2(kind, l, n, i):
        @pl.when(me.z1)
        def _():
            far, over = held(kind, l, n, me.far), held(kind, l, n, me.over)

            @pl.when(me.c0)
            def _():
                got(kind, l, 1, k.gry.at[i])

            @pl.when(me.c1)
            def _():
                got(kind, l, 1, k.grx.at[i])

            push(far, far, k.gsz, k.grz, i, me.to_z)
            pass_on(far, i)
            got(kind, l, 1, k.grz.at[i])
            pass_on(over, i)

    def stage_3(kind, l, n, i):
        @pl.when(me.z0)
        def _():
            got(kind, l, 1, k.grz.at[i])
            pass_on(held(kind, l, n, me.far), i)

    def stage(fn, i, low, high):
        for start, n, kind, l in segments:
            a, b = max(start, low), min(start + n, high)
            if a < b:

                @pl.when(both(i >= a, i < b))
                def _(kind=kind, l=l, start=start):
                    fn(kind, l, i - start, i)

    def tick(t, low, high, most=NB):
        t = jnp.asarray(t, jnp.int32)
        stage(stage_own, t + LEAD, low + LEAD, high + LEAD)
        for lag, fn in ((TWO * LAG, stage_3), (LAG, stage_2), (0, stage_1)):
            if lag < most:
                stage(fn, t - lag, max(0, low - lag), min(z.UNITS, high - lag))

    def ready(l, kind, n):
        start = next(a for a, _, kd, ll in segments if kd == kind and ll == l)
        got(kind, l, FOUR, k.grp.at[start + n])

    def begin():
        @pl.loop(0, LEAD)
        def _(i):
            stage(stage_own, i, 0, LEAD)

    def end():
        for start, n, kind, l in segments:

            @pl.loop(0, n)
            def _(i, start=start, kind=kind, l=l):
                for sem in (k.gsx, k.gsy, k.gsz):
                    got(kind, l, 1, sem.at[start + i])
                got(kind, l, FOUR, k.gsp.at[start + i])

    return tick, ready, begin, end, stage, stage_3


def loads_of(z, me, k):
    def load_gu(l, j, WG, WU, sems):
        cols = cols_of(j * z.FC, z.FC)
        others = ((FOUR * (1 - me.x), FOUR), (FOUR * me.x + TWO * (1 - me.y), TWO), (me.partner, 1))
        for n, (W, own, G) in enumerate(((WG, k.wg, k.GG), (WU, k.wu, k.GU))):
            copy(own.at[l, :, cols], W.at[rows_of(me.s * z.RB, z.RB), :], sems.at[n]).start()
            for d, size in others:
                rows = rows_of(d * z.RB, size * z.RB)
                copy(G.at[l, rows, cols], W.at[rows, :], sems.at[n]).start()

    def load_d(l, j, W, sem):
        @pl.when(j == me.s)
        def _():
            copy(k.wd.at[l], W, sem).start()

        @pl.when(j != me.s)
        def _():
            copy(k.GD.at[l, rows_of(j * z.FB, z.FB), :], W, sem).start()

    return load_gu, load_d


def forward(z, me, k):
    tick, ready, gather_begin, gather_end, stage, stage_3 = gather_of(z, me, k)
    load_gu, load_d = loads_of(z, me, k)
    NS, U1 = NB, z.NG + z.ND

    def put_turned(ref, a):
        turned = a.T
        for d in range(NB):
            core, px, py = d % TWO, d // FOUR, (d // TWO) % TWO
            i = TWO * px + py if core == 0 else TWO * py + px
            ref[core * z.HB + i * z.RB : core * z.HB + (i + 1) * z.RB, :] = turned[d * z.RB : (d + 1) * z.RB, :]

    def turn(A):
        def body(xb, yb, ab, bb, si, sj, so, sp):
            def fetch(m, e):
                rows = rows_of(m * z.TS, z.TS)
                copy(k.x.at[0, rows, :], xb.at[e], si.at[e]).start()
                copy(k.dy.at[0, rows, :], yb.at[e], sj.at[e]).start()

            fetch(0, 0)

            def sent(e):
                done(ab.at[e], so.at[e])
                done(bb.at[e], sp.at[e])

            @pl.loop(0, NS)
            def _(m):
                e = odd(m)
                cols = cols_of(m * z.TS, z.TS)

                @pl.when(m + 1 < NS)
                def _():
                    fetch(m + 1, 1 - e)

                done(xb.at[e], si.at[e])
                done(yb.at[e], sj.at[e])
                a = normed(xb[e])
                A[rows_of(m * z.TS, z.TS), :] = a

                @pl.when(m >= TWO)
                def _():
                    sent(e)

                put_turned(ab.at[e], a)
                bb[e] = yb[e].T
                copy(ab.at[e], k.ATH.at[0, :, cols], so.at[e]).start()
                copy(bb.at[e], k.DHTH.at[1, :, cols], sp.at[e]).start()

                @pl.when(e == 1)
                def _():
                    tick(lax.div(m, TWO), 0, FOUR)

            sent(0)
            sent(1)

        blocks = [vmem(TWO, z.TS, z.D)] * TWO + [vmem(TWO, z.D, z.TS)] * TWO
        pl.run_scoped(body, *blocks, *[dmas(TWO)] * FOUR)

    def gate_up(l, A, hook):
        def body(WG, WU, sb, tb, ab, ws, *so):
            kept = ((sb, k.SS), (tb, k.TT), (ab, k.ACT))

            def sent(e):
                for (b, _), sem in zip(kept, so, strict=True):
                    done(b.at[e], sem.at[e])

            def fetch(j, e):
                ready(l, "gu", TWO * j)
                ready(l, "gu", TWO * j + 1)
                load_gu(l, j, WG.at[e], WU.at[e], ws.at[e])

            fetch(0, 0)
            hook(-1, 0)

            @pl.loop(0, NB)
            def _(j):
                slot = odd(j)
                cols = cols_of(j * z.FC, z.FC)
                with jax.named_scope("gu_wait"):
                    done(WG.at[slot], ws.at[slot, 0])
                    done(WU.at[slot], ws.at[slot, 1])

                @pl.loop(0, TWO)
                def _(m):
                    with jax.named_scope("gu_sent"):

                        @pl.when(j > 0)
                        def _():
                            for e in range(TWO):
                                sent(TWO * m + e)

                    with jax.named_scope("gu_dot"):
                        for e in range(TWO):
                            at = TWO * m + e
                            a = A[rows_of(at * z.TM, z.TM), :]
                            gate = nn(a, WG[slot])
                            up = nn(a, WU[slot])
                            sig = lax.logistic(gate)
                            sl = gate * sig
                            sb[at] = sl
                            tb[at] = up * (sig + sl * (1.0 - sig))
                            ab[at] = (sl * up).astype(BF)
                    for e in range(TWO):
                        at = TWO * m + e
                        for (b, to), sem in zip(kept, so, strict=True):
                            copy(b.at[at], to.at[l, rows_of(at * z.TM, z.TM), cols], sem.at[at]).start()

                    with jax.named_scope("gu_tick"):
                        hook(j, m)

                    @pl.when(both(m == 0, j + 1 < NB))
                    def _():
                        with jax.named_scope("gu_fetch"):
                            fetch(j + 1, 1 - slot)

            for e in range(FOUR):
                sent(e)

        weights = [vmem(TWO, z.D, z.FC)] * TWO
        tiles = [vmem(FOUR, z.TM, z.FC, dtype=F32)] * TWO + [vmem(FOUR, z.TM, z.FC)]
        pl.run_scoped(body, *weights, *tiles, dmas(TWO, TWO), *[dmas(FOUR)] * THREE)

    QC, KP = z.FC // FOUR, TWO * z.FC

    def unit_of_down(n, W, ws):
        ready(0, "d", n)
        p = lax.div(n, TWO)

        @pl.loop(0, NB)
        def _(d):
            to = W.at[rows_of(p * KP + d * QC + odd(n) * z.UD, z.UD), :]

            @pl.when(d == me.s)
            def _():
                copy(k.wd.at[0, rows_of(n * z.UD, z.UD), :], to, ws.at[p]).start()

            @pl.when(d != me.s)
            def _():
                copy(k.GD.at[0, rows_of(d * z.FB + n * z.UD, z.UD), :], to, ws.at[p]).start()

    def down(A, W, ws, hook):
        def body(AC, acc, xb, hb, tb, si, sj, so, sp):
            def fetch_act(i):
                p, rows, e = lax.div(i, FOUR), rows_of(lax.rem(i, FOUR) * z.TM, z.TM), lax.rem(i, THREE)
                for d in range(NB):
                    to = AC.at[e, :, pl.ds(d * QC, QC)]
                    copy(k.ACT.at[0, rows, cols_of(d * z.FC + p * QC, QC)], to, si.at[e]).start()

            def act_there(i):
                with jax.named_scope("dn_act"):
                    done(AC.at[lax.rem(i, THREE)], si.at[lax.rem(i, THREE)])

                @pl.when(i + TWO < FOUR * FOUR)
                def _():
                    fetch_act(i + TWO)

            def fetch(m, e):
                copy(k.x.at[0, rows_of(m * z.TS, z.TS), :], xb.at[e], sj.at[e]).start()

            def there(p):
                with jax.named_scope("dn_load"):
                    done(W.at[rows_of(p * KP, KP), :], ws.at[p])

            def product(p, i, rows, at):
                return acc[rows, :] + nn(AC[lax.rem(i, THREE), at, :], W[rows_of(p * KP, KP), :])

            fetch_act(jnp.int32(0))
            fetch_act(jnp.int32(1))
            fetch(0, 0)

            @pl.loop(0, NS)
            def _(m):
                acc[rows_of(m * z.TS, z.TS), :] = jnp.zeros((z.TS, z.D), F32)

            @pl.loop(0, THREE)
            def _(p):
                there(p)

                @pl.loop(0, FOUR)
                def _(m):
                    rows = rows_of(m * z.TM, z.TM)
                    act_there(FOUR * p + m)
                    with jax.named_scope("dn_dot"):
                        acc[rows, :] = product(p, FOUR * p + m, rows, slice(None))

                    @pl.when(odd(m) == 1)
                    def _():
                        with jax.named_scope("dn_tick"):
                            hook(TWO * p + lax.div(m, TWO))

            there(jnp.int32(THREE))

            def tile_of(m):
                return lax.div(jnp.asarray(m, jnp.int32), TWO) + THREE * FOUR

            def states(m, e):
                rows, at = rows_of(m * z.TS, z.TS), rows_of(m % TWO * z.TS if isinstance(m, int) else odd(m) * z.TS, z.TS)
                low = product(jnp.int32(THREE), tile_of(m), rows, at).astype(BF)
                return (xb[e].astype(F32) + low.astype(F32)).astype(BF)

            def finish(m, e):
                a = normed(hb[e])
                A[rows_of(m * z.TS, z.TS), :] = a
                put_turned(tb.at[e], a)

            def send(m):
                e = m % THREE if isinstance(m, int) else lax.rem(m, THREE)
                copy(hb.at[e], k.H1.at[rows_of(m * z.TS, z.TS), :], so.at[e]).start()
                copy(tb.at[e], k.ATH.at[1, :, cols_of(m * z.TS, z.TS)], sp.at[e]).start()

            def sent(e):
                done(hb.at[e], so.at[e])
                done(tb.at[e], sp.at[e])

            done(xb.at[0], sj.at[0])
            fetch(1, 1)
            act_there(tile_of(0))
            hb[0] = states(0, 0)

            @pl.loop(1, NS)
            def _(m):
                e, now, before = odd(m), lax.rem(m, THREE), lax.rem(m + TWO, THREE)

                @pl.when(m + 1 < NS)
                def _():
                    fetch(m + 1, 1 - e)

                done(xb.at[e], sj.at[e])

                @pl.when(e == 0)
                def _():
                    act_there(tile_of(m))

                @pl.when(m >= THREE)
                def _():
                    sent(now)

                with jax.named_scope("dn_last"):
                    finish(m - 1, before)
                    hb[now] = states(m, e)
                send(m - 1)

                @pl.when(lax.rem(m, THREE) == TWO)
                def _():
                    with jax.named_scope("dn_tick"):
                        hook(TWO * THREE + lax.div(m, THREE))

            last = (NS - 1) % THREE
            finish(NS - 1, last)
            send(NS - 1)
            for e in range(THREE):
                sent(e)

        tiles = [vmem(THREE, z.TM, KP), vmem(z.T, z.D, dtype=F32), vmem(TWO, z.TS, z.D), vmem(THREE, z.TS, z.D), vmem(THREE, z.D, z.TS)]
        pl.run_scoped(body, *tiles, dmas(THREE), dmas(TWO), *[dmas(THREE)] * TWO)

    def run(A):
        gather_begin()
        copy(k.dy.at[0], k.DH, k.lsem.at[0]).start()
        with jax.named_scope("turn"):
            turn(A)
        with jax.named_scope("start"):
            for n in range(TWO):
                stage(stage_3, jnp.int32(n), n, n + 1)
        t1 = TWO * LAG + FOUR
        t2 = t1 + z.NG
        t3 = t2 + NB

        def first_layer(W, ws):
            def unit(t):
                n = t - (z.NG + TWO * LAG + 1)

                @pl.when(both(n >= 0, n < z.ND))
                def _():
                    unit_of_down(n, W, ws)

            def hook(j, m):
                if isinstance(j, int):
                    for t in range(FOUR, t1 - 1):
                        tick(t, t, t + 1, TWO * LAG if t < t1 - TWO else NB)
                    return

                @pl.when(both(j == 0, m == 0))
                def _():
                    tick(t1 - 1, t1 - 1, t1)

                t = TWO * j + m + t1
                tick(t, t1, t2)
                unit(t)

            gate_up(0, A, hook)

            def in_down(n):
                tick(n + t2, t2, t3)
                unit(n + t2)

            down(A, W, ws, in_down)

        pl.run_scoped(first_layer, vmem(z.F, z.D), dmas(FOUR))

        def hook(j, m):
            if not isinstance(j, int):
                t = TWO * j + m + t3 + jnp.maximum(j - FOUR, 0)
                tick(t, t3, z.UNITS + TWO * LAG)

                @pl.when(both(j >= FOUR, m == 1))
                def _():
                    tick(t + 1, t3 + NB, z.UNITS + TWO * LAG)

        gate_up(1, A, hook)

    def all_there():
        for n in range(z.ND):
            ready(1, "d", n)

    pl.run_scoped(run, vmem(z.T, z.D))
    return all_there, gather_end


def backward(z, me, k, all_there, gather_end):
    load_gu, load_d = loads_of(z, me, k)
    c, u, v = me.c, me.u, me.v
    RB, FC, HB, PR, TM = z.RB, z.FC, z.HB, z.PR, z.TM
    DR = THREE * RB
    KINDS = range(THREE)

    def place(core, i):
        return i + core * (odd(i) * TWO + lax.div(i, TWO) - i)

    def block_of(g):
        q = lax.rem(g, STEPS)
        b = lax.div(q, THREE)
        return 1 - lax.div(g, STEPS), b, q - THREE * b + lax.div(b, THREE)

    def first_row(b):
        return jnp.minimum(THREE * b, NB - THREE)

    def has(g, n):
        _, b, t = block_of(g)
        inside = both(g >= 0, g < LAST)
        if n == 0:
            return both(inside, either(b < TWO, t > 0))
        return inside if n == 1 else both(inside, t == 0)

    def halves(slot, n):
        rows = pl.ds(n * HB, HB)
        return remote(k.SP.at[rows, :], k.LP.at[slot, rows, :], k.d2ds.at[n], k.d2dr.at[slot, n], me.to_p)

    def block(slot, e, size):
        there = k.LP.at[slot, rows_of(e * DR, size), :]
        return remote(k.SP.at[rows_of(odd(e) * DR, size), :], there, k.b2ds.at[odd(e)], k.b2dr.at[slot, e], me.to_p)

    def first(slot, n):
        return remote(k.S1.at[slot, n], k.L1.at[slot, n], k.s1s.at[slot, n], k.s1r.at[slot, n], me.to_1)

    def second(slot, n):
        return remote(k.S2.at[slot, n], k.L2.at[slot, n], k.s2s.at[slot, n], k.s2r.at[slot, n], me.to_2)

    def third(slot, n):
        return remote(k.S3.at[slot, n], k.L3.at[slot, n], k.s3s.at[slot, n], k.s3r.at[slot, n], me.to_z)

    def sum_1(g):
        slot = odd(g)
        for n in KINDS:

            @pl.when(has(g - TWO, n))
            def _(n=n):
                second(slot, n).wait_send()

            @pl.when(has(g, n))
            def _(n=n):
                with jax.named_scope("l1"):
                    first(slot, n).wait_recv()
                away, home = rows_of((1 - v) * RB, RB), rows_of(v * RB, RB)
                k.S2[slot, n] = (k.K1[slot, n, away, :] + k.L1[slot, n, away, :].astype(F32)).astype(BF)
                k.K2[slot, n] = k.K1[slot, n, home, :] + k.L1[slot, n, home, :].astype(F32)
                second(slot, n).start()

        pl.semaphore_signal(k.credit, inc=1, device_id=me.to_1, device_id_type=MESH)

    def sum_2(g):
        slot = odd(g)
        for n in KINDS:

            @pl.when(has(g - TWO, n))
            def _(n=n):
                done(k.S3.at[slot, n], k.osem.at[slot, n])

            @pl.when(has(g, n))
            def _(n=n):
                with jax.named_scope("l2"):
                    second(slot, n).wait_recv()
                k.S3[slot, n] = (k.K2[slot, n] + k.L2[slot, n].astype(F32)).astype(BF)
                third(slot, n).start()

    def sum_3(g):
        slot = odd(g)
        l, b, t = block_of(g)
        for n in KINDS:

            @pl.when(has(g, n))
            def _(n=n):
                with jax.named_scope("l3"):
                    third(slot, n).wait()
                k.S3[slot, n] = (k.S3[slot, n].astype(F32) + k.L3[slot, n].astype(F32)).astype(BF)

                @pl.when(t == 0)
                def _():
                    copy(k.S3.at[slot, n], k.dwdt.at[l, rows_of((first_row(b) + n) * RB, RB), :], k.osem.at[slot, n]).start()

                if n < TWO:

                    @pl.when(t > 0)
                    def _():
                        to = (k.dwg, k.dwu)[n].at[l, :, cols_of((TWO * b + t - 1) * FC, FC)]
                        copy(k.S3.at[slot, n], to, k.osem.at[slot, n]).start()

    def sums(g):
        for lag, fn in ((FOUR, sum_3), (THREE, sum_2), (TWO, sum_1)):

            @pl.when(both(g >= lag, g < LAST + lag))
            def _(lag=lag, fn=fn):
                fn(g - lag)

    def first_sent(g):
        for n in KINDS:

            @pl.when(has(g, n))
            def _(n=n):
                first(odd(g), n).wait_send()

    def slots_free(g):
        first_sent(g - TWO)

        @pl.when(g >= TWO)
        def _():
            pl.semaphore_wait(k.credit, 1)

    def layers(AT, DA, WG, WU, WD, stb, DGU, AB, DHB, ws, si, sj, sa, hs, ns, ts):
        TS, TILES, QS = z.TS, FOUR * NB, THREE * NB

        def fetch(i):
            l, n, e = 1 - lax.div(i, TILES), lax.rem(i, TILES), odd(i)
            rows, cols = rows_of(lax.rem(n, FOUR) * TM, TM), cols_of(lax.div(n, FOUR) * FC, FC)
            copy(k.SS.at[l, rows, cols], stb.at[0, e], si.at[e]).start()
            copy(k.TT.at[l, rows, cols], stb.at[1, e], sj.at[e]).start()

        def fetch_act(i):
            l, q, e = 1 - lax.div(i, QS), lax.rem(i, NB), lax.rem(i, THREE)
            theirs, own = lax.rem(TWO * (1 - v) + q, FOUR), lax.rem(TWO * (1 - u) + q, FOUR)
            j = jnp.where(q < FOUR, TWO * place(1 - c, theirs) + 1 - c, TWO * place(c, own) + c)
            copy(k.ACT.at[l, :, cols_of(j * FC, FC)], AB.at[e], sa.at[e]).start()

        def fetch_rows(l, b, size):
            copy(k.DHTH.at[l, rows_of(b * DR, size), :], DHB.at[pl.ds(0, size), :], hs.at[0]).start()

        def fetch_turned(l):
            copy(k.ATH.at[l], AT, hs.at[1]).start()

        fetch_rows(1, 0, DR)
        all_there()
        fetch(jnp.int32(0))
        for n in KINDS:
            fetch_act(jnp.int32(n))
        fetch_turned(1)
        done(k.DH, k.lsem.at[0])

        def layer(it):
            l = 1 - it
            load_d(l, jnp.int32(0), WD, ws.at[TWO])
            load_gu(l, jnp.int32(0), WG, WU, ws)

            @pl.loop(0, FOUR)
            def _(m):
                DA[rows_of(m * TM, TM), :] = jnp.zeros((TM, z.D), F32)

            def product(i, size, keep):
                e = lax.rem(i, THREE)
                with jax.named_scope("act_wait"):
                    done(AB.at[e], sa.at[e])
                keep(nn(DHB[0:size, :], AB[e]))

                @pl.when(i + THREE < TWO * QS)
                def _():
                    fetch_act(i + THREE)

            def down_step(b, g, kinds):
                slot, i, size = odd(g), (THREE * it + b) * NB, len(kinds) * RB
                with jax.named_scope("rows_wait"):
                    done(DHB.at[pl.ds(0, size), :], hs.at[0])
                with jax.named_scope("d_theirs"):

                    @pl.loop(0, FOUR)
                    def _(e):
                        @pl.when(e >= TWO)
                        def _():
                            block(slot, e - TWO, size).wait_send()

                        def keep(val):
                            k.SP[rows_of(odd(e) * DR, size), :] = val.astype(BF)

                        product(i + e, size, keep)
                        block(slot, e, size).start()

                with jax.named_scope("sums"):
                    sums(g)
                with jax.named_scope("slots"):
                    slots_free(g)
                with jax.named_scope("d_ours"):

                    @pl.loop(0, TWO)
                    def _(e):
                        block(slot, e, size).wait_recv()

                        def keep(val):
                            val = (val + k.LP[slot, rows_of(e * DR, size), :].astype(F32)).astype(BF)
                            for at, n in enumerate(kinds):
                                k.S1[slot, n, rows_of(e * RB, RB), :] = val[at * RB : (at + 1) * RB]

                        product(i + e + FOUR, size, keep)

                for n in kinds:

                    first(slot, n).start()

                with jax.named_scope("d_keep"):

                    @pl.loop(0, TWO)
                    def _(e):
                        block(slot, e + TWO, size).wait_recv()

                        def keep(val):
                            val = val + k.LP[slot, rows_of((e + TWO) * DR, size), :].astype(F32)
                            for at, n in enumerate(kinds):
                                k.K1[slot, n, rows_of(e * RB, RB), :] = val[at * RB : (at + 1) * RB]

                        product(i + e + FOUR + TWO, size, keep)

                for e in range(TWO):
                    block(slot, e, size).wait_send()

                @pl.when(b == 0)
                def _():
                    fetch_rows(l, 1, DR)

                @pl.when(b == 1)
                def _():
                    fetch_rows(l, TWO, TWO * RB)

            def add_da(rows):
                DA[rows, :] += nt(DGU[0, rows, :], WG[...]) + nt(DGU[1, rows, :], WU[...])

            def weights_there():
                done(WG, ws.at[0])
                done(WU, ws.at[1])

            def gate_up_step(j, g):
                slot = odd(g)
                with jax.named_scope("wd_wait"):
                    done(WD, ws.at[TWO])

                def tiles(before):
                    @pl.loop(0, FOUR)
                    def _(m):
                        i = it * TILES + j * FOUR + m
                        e = odd(i)
                        rows = rows_of(m * TM, TM)

                        @pl.when(i + 1 < TWO * TILES)
                        def _():
                            fetch(i + 1)

                        with jax.named_scope("st_wait"):
                            done(stb.at[0, e], si.at[e])
                            done(stb.at[1, e], sj.at[e])
                        with jax.named_scope("a_dot"):
                            before(rows)
                            dact = nt(k.DH[rows, :], WD[...]).astype(BF).astype(F32)
                            DGU[0, rows, :] = (dact * stb[1, e]).astype(BF)
                            DGU[1, rows, :] = (dact * stb[0, e]).astype(BF)

                @pl.when(j == 0)
                def _():
                    tiles(lambda rows: None)

                @pl.when(j > 0)
                def _():
                    with jax.named_scope("w_wait"):
                        weights_there()
                    tiles(add_da)
                    load_gu(l, j, WG, WU, ws)

                @pl.when(j + 1 < NB)
                def _():
                    load_d(l, j + 1, WD, ws.at[TWO])

                @pl.when(j == 0)
                def _():
                    with jax.named_scope("at_wait"):
                        done(AT, hs.at[1])

                with jax.named_scope("sums"):
                    sums(g)
                with jax.named_scope("b_dot"):
                    for n in range(TWO):
                        k.SP[n * HB : (n + 1) * HB, :] = nn(AT[rows_of((1 - c) * HB, HB), :], DGU[n]).astype(BF)
                        halves(slot, n).start()
                with jax.named_scope("slots"):
                    slots_free(g)
                out, keep = TWO * (1 - u) * RB, TWO * u * RB
                for n in range(TWO):
                    with jax.named_scope("half_wait"):
                        halves(slot, n).wait_recv()
                    with jax.named_scope("c_dot"):
                        k.S1[slot, n] = (
                            nn(AT[rows_of(c * HB + out, PR), :], DGU[n]) + k.LP[slot, rows_of(n * HB + out, PR), :].astype(F32)
                        ).astype(BF)
                        k.K1[slot, n] = nn(AT[rows_of(c * HB + keep, PR), :], DGU[n]) + k.LP[
                            slot, rows_of(n * HB + keep, PR), :
                        ].astype(F32)
                    first(slot, n).start()
                for n in range(TWO):
                    halves(slot, n).wait_send()

            @pl.loop(0, STEPS)
            def _(q):
                g = it * STEPS + q
                _, b, t = block_of(g)

                @pl.when(both(t == 0, b < TWO))
                def _():
                    down_step(b, g, (0, 1, TWO))

                @pl.when(both(t == 0, b == TWO))
                def _():
                    down_step(b, g, (1, TWO))

                @pl.when(t > 0)
                def _():
                    gate_up_step(TWO * b + t - 1, g)

            def fetch_states(m):
                rows, to = rows_of(m * TS, TS), WD.at[rows_of(odd(m) * TS, TS), :]

                @pl.when(l == 1)
                def _():
                    copy(k.H1.at[rows, :], to, ns.at[odd(m)]).start()

                @pl.when(l == 0)
                def _():
                    copy(k.x.at[0, rows, :], to, ns.at[odd(m)]).start()

            def there(m):
                done(WD.at[rows_of(odd(m) * TS, TS), :], ns.at[odd(m)])

            def norm(m):
                rows = rows_of(m * TS, TS)
                wide = WD[rows_of(odd(m) * TS, TS), :].astype(F32)
                da = DA[rows, :].astype(BF).astype(F32)
                scale = lax.rsqrt(jnp.mean(wide * wide, -1, keepdims=True) + 1e-6)
                along = jnp.mean(da * wide, -1, keepdims=True)
                dn = (da * scale - wide * (along * scale * scale * scale)).astype(BF)
                k.DH[rows, :] = (k.DH[rows, :].astype(F32) + dn.astype(F32)).astype(BF)

            def turned(m):
                return k.SP.at[:, cols_of(odd(m) * TS, TS)]

            def hand_on(m):
                rows, cols = rows_of(m * TS, TS), cols_of(m * TS, TS)

                @pl.when(l == 1)
                def _():
                    @pl.when(m >= TWO)
                    def _():
                        done(turned(m), ts.at[odd(m)])

                    k.SP[:, cols_of(odd(m) * TS, TS)] = k.DH[rows, :].T
                    copy(turned(m), k.DHTH.at[0, :, cols], ts.at[odd(m)]).start()

                @pl.when(l == 0)
                def _():
                    copy(k.DH.at[rows, :], k.dx.at[0, rows, :], ts.at[TWO]).start()

            def back(n):
                return AT.at[pl.ds(n * z.FB, z.FB), pl.ds(0, z.D)]

            def turn_back():
                for n in range(TWO):
                    done(AB.at[n, pl.ds(0, z.D), :], sa.at[n])
                    AT[n * z.FB : (n + 1) * z.FB, 0 : z.D] = AB[n, 0 : z.D, :].T
                    copy(back(n), k.dwd.at[n], hs.at[n]).start()

            fetch_states(jnp.int32(0))

            @pl.when(it == 0)
            def _():
                fetch_turned(0)

            with jax.named_scope("norm"):
                weights_there()
                add_da(rows_of(0, TS))

                @pl.loop(1, NB)
                def _(m):
                    @pl.when(both(l == 0, m == 1))
                    def _():
                        gather_end()

                    @pl.when(both(l == 0, m == FOUR))
                    def _():
                        with jax.named_scope("turn_back"):
                            turn_back()

                    @pl.when(both(l == 0, lax.rem(m, THREE) == 1))
                    def _():
                        with jax.named_scope("norm_sums"):
                            sums(LAST + lax.div(m, THREE))

                    @pl.when(both(l == 0, m == 1))
                    def _():
                        for n in range(TWO):
                            copy(k.dwdt.at[n], AB.at[n, pl.ds(0, z.D), :], sa.at[n]).start()

                    fetch_states(m)
                    there(m - 1)
                    with jax.named_scope("norm_dot"):
                        norm(m - 1)
                        add_da(rows_of(m * TS, TS))
                    hand_on(m - 1)

                there(jnp.int32(NB - 1))
                norm(jnp.int32(NB - 1))
                hand_on(jnp.int32(NB - 1))

            @pl.when(l == 1)
            def _():
                for m in range(TWO):
                    done(turned(m), ts.at[m])
                fetch_rows(0, 0, DR)

            @pl.when(l == 0)
            def _():
                done(k.DH, ts.at[TWO])
                for n in range(TWO):
                    done(back(n), hs.at[n])

        @pl.loop(0, TWO)
        def _(it):
            layer(it)

    weights = [vmem(z.D, FC)] * TWO + [vmem(z.FB, z.D)]
    tiles = [vmem(TWO, TWO, TM, FC, dtype=F32), vmem(TWO, z.T, FC), vmem(THREE, z.T, FC), vmem(DR, z.T)]
    pl.run_scoped(
        layers, vmem(z.D, z.T), vmem(z.T, z.D, dtype=F32), *weights, *tiles, *[dmas(THREE)] * FOUR, *[dmas(TWO)] * TWO, dmas(THREE)
    )

    with jax.named_scope("tail"):
        sums(jnp.int32(LAST + THREE))
    for g in (LAST - TWO, LAST - 1):
        first_sent(jnp.int32(g))
        for n in range(TWO):
            second(g % TWO, n).wait_send()
            done(k.S3.at[g % TWO, n], k.osem.at[g % TWO, n])
    pl.semaphore_wait(k.credit, TWO)


class Refs:
    def __init__(self, names, refs):
        for name, ref in zip(names, refs, strict=True):
            setattr(self, name, ref)


def call(name, z, fn, number, ins, outs, scratch, flops):
    names = [*ins, *outs, *scratch]

    def kernel(*refs):
        me, k = Here(), Refs(names, refs)
        me.meet()
        fn(z, me, k)

    hbm = pl.BlockSpec(memory_space=pl.ANY)
    made = pl.pallas_call(
        kernel,
        out_shape=[jax.ShapeDtypeStruct(*spec) for spec in outs.values()],
        in_specs=[hbm] * len(ins),
        out_specs=[hbm] * len(outs),
        scratch_shapes=list(scratch.values()),
        compiler_params=pltpu.CompilerParams(collective_id=number, has_side_effects=True, vmem_limit_bytes=67043328),
        cost_estimate=pl.CostEstimate(flops=flops, bytes_accessed=1 << 28, transcendentals=0),
        name=name,
    )(*ins.values())
    return dict(zip(outs, made, strict=True))


def solution(mesh):
    def step(x, dy, wg, wu, wd):
        _, T, D = x.shape
        F = wg.shape[TWO]
        z = Sizes(T, D, F)
        RB, FB, FC, L = z.RB, z.FB, z.FC, TWO
        ins = {"x": x, "dy": dy, "wg": wg, "wu": wu, "wd": wd}
        kept = {
            **{name: ((L, D, F), BF) for name in ("GG", "GU")},
            "GD": ((L, F, D), BF),
            **{name: ((L, T, F), F32) for name in ("SS", "TT")},
            "ACT": ((L, T, F), BF),
            "H1": ((T, D), BF),
            "ATH": ((L, D, T), BF),
            "DHTH": ((L, D, T), BF),
            "dwdt": ((L, D, FB), BF),
        }
        results = {
            "dx": ((1, T, D), BF),
            **{name: ((L, RB, F), BF) for name in ("dwg", "dwu")},
            "dwd": ((L, FB, D), BF),
        }
        gather = {name: dmas(z.UNITS) for name in ("gsx", "gsy", "gsz", "gsp", "grx", "gry", "grz", "grp")}
        item, pair = (TWO, THREE, RB, FC), (TWO, THREE, z.PR, FC)
        sums = {
            "DH": vmem(T, D),
            "SP": vmem(TWO * z.HB, FC),
            "LP": vmem(TWO, THREE * z.HB, FC),
            **{name: vmem(*pair) for name in ("S1", "L1")},
            "K1": vmem(*pair, dtype=F32),
            **{name: vmem(*item) for name in ("S2", "L2", "S3", "L3")},
            "K2": vmem(*item, dtype=F32),
            "d2ds": dmas(TWO),
            "d2dr": dmas(TWO, TWO),
            "b2ds": dmas(TWO),
            "b2dr": dmas(TWO, FOUR),
            **{name: dmas(TWO, THREE) for name in ("s1s", "s1r", "s2s", "s2r", "s3s", "s3r", "osem")},
            "credit": pltpu.SemaphoreType.REGULAR,
            "lsem": dmas(1),
        }
        flops = TWO * T * D * F

        def whole(z, me, k):
            all_there, gather_end = forward(z, me, k)
            backward(z, me, k, all_there, gather_end)

        made = call("whole", z, whole, 0, ins, {**results, **kept}, {**gather, **sums}, flops * (STEPS + FOUR + TWO))
        return made["dx"], made["dwg"], made["dwu"], made["dwd"]

    states, cut = P(("rep", "r", "s"), None, None), P(None, "s", None)
    return jax.shard_map(
        step,
        mesh=mesh,
        in_specs=(states, states, cut, cut, cut),
        out_specs=(states, *[P("rep", "s", None)] * THREE),
        check_vma=False,
    )
```

```python
import functools

import jax
import jax.numpy as jnp
from jax import lax
from jax.experimental import pallas as pl
from jax.experimental.pallas import tpu as pltpu
from jax.sharding import PartitionSpec as P

MESH = pl.DeviceIdType.MESH
BF, F32 = jnp.bfloat16, jnp.float32
NB = 8
LEAD = 8
LAG = 2
TWO, THREE, FOUR = 2, 3, 4
STEPS = 11
LAST = TWO * STEPS


def nn(a, b):
    return lax.dot_general(a, b, (((1,), (0,)), ((), ())), preferred_element_type=F32)


def nt(a, b):
    return lax.dot_general(a, b, (((1,), (1,)), ((), ())), preferred_element_type=F32)


def rows_of(start, size):
    return pl.ds(start if isinstance(start, int) else pl.multiple_of(start, 16), size)


def cols_of(start, size):
    return pl.ds(start if isinstance(start, int) else pl.multiple_of(start, 128), size)


def odd(i):
    return lax.rem(i, TWO)


def copy(src, dst, sem):
    return pltpu.make_async_copy(src, dst, sem)


def done(ref, sem):
    pltpu.make_async_copy(ref, ref, sem).wait()


def both(a, b):
    return jnp.logical_and(a, b)


def either(a, b):
    return jnp.logical_or(a, b)


def vmem(*shape, dtype=BF):
    return pltpu.VMEM(shape, dtype)


def dmas(*shape):
    return pltpu.SemaphoreType.DMA(shape)


class Sizes:
    def __init__(self, T, D, F):
        self.T, self.D, self.F = T, D, F
        self.RB, self.FB, self.HB = D // NB, F // NB, D // TWO
        self.FC = self.FB
        self.UC, self.UD = self.FC // TWO, self.FB // NB
        self.NG, self.ND = F // self.UC, NB
        self.TM, self.TS = T // FOUR, T // NB
        self.PR = TWO * self.RB
        self.UNITS = TWO * (self.NG + self.ND)


class Here:
    def __init__(self):
        self.r, self.s = lax.axis_index("r"), lax.axis_index("s")
        rep, r, s = lax.axis_index("rep"), self.r, self.s
        self.c = c = odd(s)
        y, x = odd(lax.div(s, TWO)), lax.div(s, FOUR)
        self.x, self.y = x, y
        self.xn, self.yn, partner = s + FOUR - NB * x, s + TWO - FOUR * y, s + 1 - TWO * c
        self.partner = partner
        self.far = self.xn + self.yn - s
        self.over = self.yn + c * (self.xn - self.yn)
        self.u, self.v = x + c * (y - x), y + c * (x - y)
        n1 = self.xn + c * (self.yn - self.xn)
        n2 = self.xn + self.yn - n1
        self.to_p, self.to_x, self.to_y, self.to_z = (rep, r, partner), (rep, r, self.xn), (rep, r, self.yn), (rep, 1 - r, s)
        self.to_1, self.to_2 = (rep, r, n1), (rep, r, n2)
        self.z0, self.z1, self.c0, self.c1 = r == 0, r == 1, c == 0, c == 1

    def meet(self):
        barrier = pltpu.get_barrier_semaphore()
        for dev in (self.to_p, self.to_x, self.to_y, self.to_z):
            pl.semaphore_signal(barrier, inc=1, device_id=dev, device_id_type=MESH)
        pl.semaphore_wait(barrier, FOUR)


def remote(src, dst, ss, rs, dev):
    return pltpu.make_async_remote_copy(src, dst, ss, rs, device_id=dev, device_id_type=MESH)


def normed(h):
    wide = h.astype(F32)
    scale = lax.rsqrt(jnp.mean(wide * wide, -1, keepdims=True) + 1e-6)
    return (wide * scale).astype(BF)


def gather_of(z, me, k):
    segments = (
        (0, z.NG, "gu", 0),
        (z.NG, z.ND, "d", 0),
        (z.NG + z.ND, z.NG, "gu", 1),
        (z.UNITS - z.ND, z.ND, "d", 1),
    )

    def held(kind, l, n, d):
        if kind == "gu":
            return [G.at[l, rows_of(d * z.RB, z.RB), cols_of(n * z.UC, z.UC)] for G in (k.GG, k.GU)]
        return [k.GD.at[l, rows_of(d * z.FB + n * z.UD, z.UD), :]]

    def mine(kind, l, n):
        if kind == "gu":
            return [w.at[l, :, cols_of(n * z.UC, z.UC)] for w in (k.wg, k.wu)]
        return [k.wd.at[l, rows_of(n * z.UD, z.UD), :]]

    def got(kind, l, n, sem):
        done(k.GG.at[l, pl.ds(0, n * z.PR), pl.ds(0, z.UC)] if kind == "gu" else k.GD.at[l, pl.ds(0, n * z.UD), :], sem)

    def push(srcs, dsts, ss, rs, i, dev):
        for a, b in zip(srcs, dsts, strict=True):
            remote(a, b, ss.at[i], rs.at[i], dev).start()

    def pass_on(ref, i):
        push(ref, ref, k.gsp, k.grp, i, me.to_p)

    def stage_own(kind, l, n, i):
        own, there = mine(kind, l, n), held(kind, l, n, me.s)

        @pl.when(either(me.z0, me.c0))
        def _():
            push(own, there, k.gsx, k.grx, i, me.to_x)

        @pl.when(either(me.z0, me.c1))
        def _():
            push(own, there, k.gsy, k.gry, i, me.to_y)

        push(own, there, k.gsp, k.grp, i, me.to_p)

    def stage_1(kind, l, n, i):
        hx, hy = held(kind, l, n, me.xn), held(kind, l, n, me.yn)

        @pl.when(either(me.z0, me.c0))
        def _():
            got(kind, l, 1, k.grx.at[i])

        @pl.when(either(me.z0, me.c1))
        def _():
            got(kind, l, 1, k.gry.at[i])

        @pl.when(me.z0)
        def _():
            on = held(kind, l, n, me.over)
            push(on, on, k.gsz, k.grz, i, me.to_z)
            pass_on(hx, i)
            pass_on(hy, i)

        @pl.when(both(me.z1, me.c0))
        def _():
            push(hx, hx, k.gsy, k.gry, i, me.to_y)
            pass_on(hx, i)

        @pl.when(both(me.z1, me.c1))
        def _():
            push(hy, hy, k.gsx, k.grx, i, me.to_x)
            pass_on(hy, i)

    def stage_2(kind, l, n, i):
        @pl.when(me.z1)
        def _():
            far, over = held(kind, l, n, me.far), held(kind, l, n, me.over)

            @pl.when(me.c0)
            def _():
                got(kind, l, 1, k.gry.at[i])

            @pl.when(me.c1)
            def _():
                got(kind, l, 1, k.grx.at[i])

            push(far, far, k.gsz, k.grz, i, me.to_z)
            pass_on(far, i)
            got(kind, l, 1, k.grz.at[i])
            pass_on(over, i)

    def stage_3(kind, l, n, i):
        @pl.when(me.z0)
        def _():
            got(kind, l, 1, k.grz.at[i])
            pass_on(held(kind, l, n, me.far), i)

    def stage(fn, i, low, high):
        for start, n, kind, l in segments:
            a, b = max(start, low), min(start + n, high)
            if a < b:

                @pl.when(both(i >= a, i < b))
                def _(kind=kind, l=l, start=start):
                    fn(kind, l, i - start, i)

    def tick(t, low, high, most=NB):
        t = jnp.asarray(t, jnp.int32)
        stage(stage_own, t + LEAD, low + LEAD, high + LEAD)
        for lag, fn in ((TWO * LAG, stage_3), (LAG, stage_2), (0, stage_1)):
            if lag < most:
                stage(fn, t - lag, max(0, low - lag), min(z.UNITS, high - lag))

    def ready(l, kind, n):
        start = next(a for a, _, kd, ll in segments if kd == kind and ll == l)
        got(kind, l, FOUR, k.grp.at[start + n])

    def begin():
        @pl.loop(0, LEAD)
        def _(i):
            stage(stage_own, i, 0, LEAD)

    def end():
        for start, n, kind, l in segments:

            @pl.loop(0, n)
            def _(i, start=start, kind=kind, l=l):
                for sem in (k.gsx, k.gsy, k.gsz):
                    got(kind, l, 1, sem.at[start + i])
                got(kind, l, FOUR, k.gsp.at[start + i])

    return tick, ready, begin, end, stage, stage_3


def loads_of(z, me, k):
    def load_gu(l, j, WG, WU, sems):
        cols = cols_of(j * z.FC, z.FC)
        others = ((FOUR * (1 - me.x), FOUR), (FOUR * me.x + TWO * (1 - me.y), TWO), (me.partner, 1))
        for n, (W, own, G) in enumerate(((WG, k.wg, k.GG), (WU, k.wu, k.GU))):
            copy(own.at[l, :, cols], W.at[rows_of(me.s * z.RB, z.RB), :], sems.at[n]).start()
            for d, size in others:
                rows = rows_of(d * z.RB, size * z.RB)
                copy(G.at[l, rows, cols], W.at[rows, :], sems.at[n]).start()

    def load_d(l, j, W, sem):
        @pl.when(j == me.s)
        def _():
            copy(k.wd.at[l], W, sem).start()

        @pl.when(j != me.s)
        def _():
            copy(k.GD.at[l, rows_of(j * z.FB, z.FB), :], W, sem).start()

    return load_gu, load_d


def forward(z, me, k):
    tick, ready, gather_begin, gather_end, stage, stage_3 = gather_of(z, me, k)
    load_gu, load_d = loads_of(z, me, k)
    NS, U1 = NB, z.NG + z.ND

    def put_turned(ref, a):
        turned = a.T
        for d in range(NB):
            core, px, py = d % TWO, d // FOUR, (d // TWO) % TWO
            i = TWO * px + py if core == 0 else TWO * py + px
            ref[core * z.HB + i * z.RB : core * z.HB + (i + 1) * z.RB, :] = turned[d * z.RB : (d + 1) * z.RB, :]

    def turn(A):
        def body(xb, yb, ab, bb, si, sj, so, sp):
            def fetch(m, e):
                rows = rows_of(m * z.TS, z.TS)
                copy(k.x.at[0, rows, :], xb.at[e], si.at[e]).start()
                copy(k.dy.at[0, rows, :], yb.at[e], sj.at[e]).start()

            fetch(0, 0)

            def sent(e):
                done(ab.at[e], so.at[e])
                done(bb.at[e], sp.at[e])

            @pl.loop(0, NS)
            def _(m):
                e = odd(m)
                cols = cols_of(m * z.TS, z.TS)

                @pl.when(m + 1 < NS)
                def _():
                    fetch(m + 1, 1 - e)

                done(xb.at[e], si.at[e])
                done(yb.at[e], sj.at[e])
                a = normed(xb[e])
                A[rows_of(m * z.TS, z.TS), :] = a

                @pl.when(m >= TWO)
                def _():
                    sent(e)

                put_turned(ab.at[e], a)
                bb[e] = yb[e].T
                copy(ab.at[e], k.ATH.at[0, :, cols], so.at[e]).start()
                copy(bb.at[e], k.DHTH.at[1, :, cols], sp.at[e]).start()

                @pl.when(e == 1)
                def _():
                    tick(lax.div(m, TWO), 0, FOUR)

            sent(0)
            sent(1)

        blocks = [vmem(TWO, z.TS, z.D)] * TWO + [vmem(TWO, z.D, z.TS)] * TWO
        pl.run_scoped(body, *blocks, *[dmas(TWO)] * FOUR)

    def gate_up(l, A, hook):
        def body(WG, WU, sb, tb, ab, ws, *so):
            kept = ((sb, k.SS), (tb, k.TT), (ab, k.ACT))

            def sent(e):
                for (b, _), sem in zip(kept, so, strict=True):
                    done(b.at[e], sem.at[e])

            def fetch(j, e):
                ready(l, "gu", TWO * j)
                ready(l, "gu", TWO * j + 1)
                load_gu(l, j, WG.at[e], WU.at[e], ws.at[e])

            fetch(0, 0)
            hook(-1, 0)

            @pl.loop(0, NB)
            def _(j):
                slot = odd(j)
                cols = cols_of(j * z.FC, z.FC)
                with jax.named_scope("gu_wait"):
                    done(WG.at[slot], ws.at[slot, 0])
                    done(WU.at[slot], ws.at[slot, 1])

                @pl.loop(0, TWO)
                def _(m):
                    with jax.named_scope("gu_sent"):

                        @pl.when(j > 0)
                        def _():
                            for e in range(TWO):
                                sent(TWO * m + e)

                    with jax.named_scope("gu_dot"):
                        for e in range(TWO):
                            at = TWO * m + e
                            a = A[rows_of(at * z.TM, z.TM), :]
                            gate = nn(a, WG[slot])
                            up = nn(a, WU[slot])
                            sig = lax.logistic(gate)
                            sl = gate * sig
                            sb[at] = sl
                            tb[at] = up * (sig + sl * (1.0 - sig))
                            ab[at] = (sl * up).astype(BF)
                    for e in range(TWO):
                        at = TWO * m + e
                        for (b, to), sem in zip(kept, so, strict=True):
                            copy(b.at[at], to.at[l, rows_of(at * z.TM, z.TM), cols], sem.at[at]).start()

                    with jax.named_scope("gu_tick"):
                        hook(j, m)

                    @pl.when(both(m == 0, j + 1 < NB))
                    def _():
                        with jax.named_scope("gu_fetch"):
                            fetch(j + 1, 1 - slot)

            for e in range(FOUR):
                sent(e)

        weights = [vmem(TWO, z.D, z.FC)] * TWO
        tiles = [vmem(FOUR, z.TM, z.FC, dtype=F32)] * TWO + [vmem(FOUR, z.TM, z.FC)]
        pl.run_scoped(body, *weights, *tiles, dmas(TWO, TWO), *[dmas(FOUR)] * THREE)

    QC, KP = z.FC // FOUR, TWO * z.FC

    def unit_of_down(n, W, ws):
        ready(0, "d", n)
        p = lax.div(n, TWO)

        @pl.loop(0, NB)
        def _(d):
            to = W.at[rows_of(p * KP + d * QC + odd(n) * z.UD, z.UD), :]

            @pl.when(d == me.s)
            def _():
                copy(k.wd.at[0, rows_of(n * z.UD, z.UD), :], to, ws.at[p]).start()

            @pl.when(d != me.s)
            def _():
                copy(k.GD.at[0, rows_of(d * z.FB + n * z.UD, z.UD), :], to, ws.at[p]).start()

    def down(A, W, ws, hook):
        def body(AC, acc, xb, hb, tb, si, sj, so, sp):
            def fetch_act(i):
                p, rows, e = lax.div(i, FOUR), rows_of(lax.rem(i, FOUR) * z.TM, z.TM), lax.rem(i, THREE)
                for d in range(NB):
                    to = AC.at[e, :, pl.ds(d * QC, QC)]
                    copy(k.ACT.at[0, rows, cols_of(d * z.FC + p * QC, QC)], to, si.at[e]).start()

            def act_there(i):
                with jax.named_scope("dn_act"):
                    done(AC.at[lax.rem(i, THREE)], si.at[lax.rem(i, THREE)])

                @pl.when(i + TWO < FOUR * FOUR)
                def _():
                    fetch_act(i + TWO)

            def fetch(m, e):
                copy(k.x.at[0, rows_of(m * z.TS, z.TS), :], xb.at[e], sj.at[e]).start()

            def there(p):
                with jax.named_scope("dn_load"):
                    done(W.at[rows_of(p * KP, KP), :], ws.at[p])

            def product(p, i, rows, at):
                return acc[rows, :] + nn(AC[lax.rem(i, THREE), at, :], W[rows_of(p * KP, KP), :])

            fetch_act(jnp.int32(0))
            fetch_act(jnp.int32(1))
            fetch(0, 0)

            @pl.loop(0, NS)
            def _(m):
                acc[rows_of(m * z.TS, z.TS), :] = jnp.zeros((z.TS, z.D), F32)

            @pl.loop(0, THREE)
            def _(p):
                there(p)

                @pl.loop(0, FOUR)
                def _(m):
                    rows = rows_of(m * z.TM, z.TM)
                    act_there(FOUR * p + m)
                    with jax.named_scope("dn_dot"):
                        acc[rows, :] = product(p, FOUR * p + m, rows, slice(None))

                    @pl.when(odd(m) == 1)
                    def _():
                        with jax.named_scope("dn_tick"):
                            hook(TWO * p + lax.div(m, TWO))

            there(jnp.int32(THREE))

            def tile_of(m):
                return lax.div(jnp.asarray(m, jnp.int32), TWO) + THREE * FOUR

            def states(m, e):
                rows, at = rows_of(m * z.TS, z.TS), rows_of(m % TWO * z.TS if isinstance(m, int) else odd(m) * z.TS, z.TS)
                low = product(jnp.int32(THREE), tile_of(m), rows, at).astype(BF)
                return (xb[e].astype(F32) + low.astype(F32)).astype(BF)

            def finish(m, e):
                a = normed(hb[e])
                A[rows_of(m * z.TS, z.TS), :] = a
                put_turned(tb.at[e], a)

            def send(m):
                e = m % THREE if isinstance(m, int) else lax.rem(m, THREE)
                copy(hb.at[e], k.H1.at[rows_of(m * z.TS, z.TS), :], so.at[e]).start()
                copy(tb.at[e], k.ATH.at[1, :, cols_of(m * z.TS, z.TS)], sp.at[e]).start()

            def sent(e):
                done(hb.at[e], so.at[e])
                done(tb.at[e], sp.at[e])

            done(xb.at[0], sj.at[0])
            fetch(1, 1)
            act_there(tile_of(0))
            hb[0] = states(0, 0)

            @pl.loop(1, NS)
            def _(m):
                e, now, before = odd(m), lax.rem(m, THREE), lax.rem(m + TWO, THREE)

                @pl.when(m + 1 < NS)
                def _():
                    fetch(m + 1, 1 - e)

                done(xb.at[e], sj.at[e])

                @pl.when(e == 0)
                def _():
                    act_there(tile_of(m))

                @pl.when(m >= THREE)
                def _():
                    sent(now)

                with jax.named_scope("dn_last"):
                    finish(m - 1, before)
                    hb[now] = states(m, e)
                send(m - 1)

                @pl.when(e == 1)
                def _():
                    with jax.named_scope("dn_tick"):
                        hook(TWO * THREE + lax.div(m, TWO))

            last = (NS - 1) % THREE
            finish(NS - 1, last)
            send(NS - 1)
            for e in range(THREE):
                sent(e)

        tiles = [vmem(THREE, z.TM, KP), vmem(z.T, z.D, dtype=F32), vmem(TWO, z.TS, z.D), vmem(THREE, z.TS, z.D), vmem(THREE, z.D, z.TS)]
        pl.run_scoped(body, *tiles, dmas(THREE), dmas(TWO), *[dmas(THREE)] * TWO)

    def run(A):
        gather_begin()
        copy(k.dy.at[0], k.DH, k.lsem.at[0]).start()
        with jax.named_scope("turn"):
            turn(A)
        with jax.named_scope("start"):
            for n in range(TWO):
                stage(stage_3, jnp.int32(n), n, n + 1)
        t1 = TWO * LAG + FOUR
        t2 = t1 + z.NG
        t3 = t2 + NB + TWO

        def first_layer(W, ws):
            def unit(t):
                n = t - (z.NG + TWO * LAG + 1)

                @pl.when(both(n >= 0, n < z.ND))
                def _():
                    unit_of_down(n, W, ws)

            def hook(j, m):
                if isinstance(j, int):
                    for t in range(FOUR, t1 - 1):
                        tick(t, t, t + 1, TWO * LAG if t < t1 - TWO else NB)
                    return

                @pl.when(both(j == 0, m == 0))
                def _():
                    tick(t1 - 1, t1 - 1, t1)

                t = TWO * j + m + t1
                tick(t, t1, t2)
                unit(t)

            gate_up(0, A, hook)

            def in_down(n):
                tick(n + t2, t2, t3)
                unit(n + t2)

            down(A, W, ws, in_down)

        pl.run_scoped(first_layer, vmem(z.F, z.D), dmas(FOUR))

        def hook(j, m):
            if not isinstance(j, int):
                tick(TWO * j + m + t3, t3, t3 + z.NG)

        gate_up(1, A, hook)

    t4 = z.UNITS + TWO * LAG - TWO

    def late(n):
        tick(n + t4, t4, t4 + TWO)

    def all_there():
        for n in range(z.ND):
            ready(1, "d", n)

    pl.run_scoped(run, vmem(z.T, z.D))
    return late, all_there, gather_end


def backward(z, me, k, late, all_there, gather_end):
    load_gu, load_d = loads_of(z, me, k)
    c, u, v = me.c, me.u, me.v
    RB, FC, HB, PR, TM = z.RB, z.FC, z.HB, z.PR, z.TM
    DR = THREE * RB
    KINDS = range(THREE)

    def place(core, i):
        return i + core * (odd(i) * TWO + lax.div(i, TWO) - i)

    def block_of(g):
        q = lax.rem(g, STEPS)
        b = lax.div(q, THREE)
        return 1 - lax.div(g, STEPS), b, q - THREE * b + lax.div(b, THREE)

    def first_row(b):
        return jnp.minimum(THREE * b, NB - THREE)

    def has(g, n):
        _, b, t = block_of(g)
        inside = both(g >= 0, g < LAST)
        if n == 0:
            return both(inside, either(b < TWO, t > 0))
        return inside if n == 1 else both(inside, t == 0)

    def halves(slot, n):
        rows = pl.ds(n * HB, HB)
        return remote(k.SP.at[rows, :], k.LP.at[slot, rows, :], k.d2ds.at[n], k.d2dr.at[slot, n], me.to_p)

    def block(slot, e, size):
        there = k.LP.at[slot, rows_of(e * DR, size), :]
        return remote(k.SP.at[rows_of(odd(e) * DR, size), :], there, k.b2ds.at[odd(e)], k.b2dr.at[slot, e], me.to_p)

    def first(slot, n):
        return remote(k.S1.at[slot, n], k.L1.at[slot, n], k.s1s.at[slot, n], k.s1r.at[slot, n], me.to_1)

    def second(slot, n):
        return remote(k.S2.at[slot, n], k.L2.at[slot, n], k.s2s.at[slot, n], k.s2r.at[slot, n], me.to_2)

    def third(slot, n):
        return remote(k.S3.at[slot, n], k.L3.at[slot, n], k.s3s.at[slot, n], k.s3r.at[slot, n], me.to_z)

    def sum_1(g):
        slot = odd(g)
        for n in KINDS:

            @pl.when(has(g - TWO, n))
            def _(n=n):
                second(slot, n).wait_send()

            @pl.when(has(g, n))
            def _(n=n):
                with jax.named_scope("l1"):
                    first(slot, n).wait_recv()
                away, home = rows_of((1 - v) * RB, RB), rows_of(v * RB, RB)
                k.S2[slot, n] = (k.K1[slot, n, away, :] + k.L1[slot, n, away, :].astype(F32)).astype(BF)
                k.K2[slot, n] = k.K1[slot, n, home, :] + k.L1[slot, n, home, :].astype(F32)
                second(slot, n).start()

        pl.semaphore_signal(k.credit, inc=1, device_id=me.to_1, device_id_type=MESH)

    def sum_2(g):
        slot = odd(g)
        for n in KINDS:

            @pl.when(has(g - TWO, n))
            def _(n=n):
                done(k.S3.at[slot, n], k.osem.at[slot, n])

            @pl.when(has(g, n))
            def _(n=n):
                with jax.named_scope("l2"):
                    second(slot, n).wait_recv()
                k.S3[slot, n] = (k.K2[slot, n] + k.L2[slot, n].astype(F32)).astype(BF)
                third(slot, n).start()

    def sum_3(g):
        slot = odd(g)
        l, b, t = block_of(g)
        for n in KINDS:

            @pl.when(has(g, n))
            def _(n=n):
                with jax.named_scope("l3"):
                    third(slot, n).wait()
                k.S3[slot, n] = (k.S3[slot, n].astype(F32) + k.L3[slot, n].astype(F32)).astype(BF)

                @pl.when(t == 0)
                def _():
                    copy(k.S3.at[slot, n], k.dwdt.at[l, rows_of((first_row(b) + n) * RB, RB), :], k.osem.at[slot, n]).start()

                if n < TWO:

                    @pl.when(t > 0)
                    def _():
                        to = (k.dwg, k.dwu)[n].at[l, :, cols_of((TWO * b + t - 1) * FC, FC)]
                        copy(k.S3.at[slot, n], to, k.osem.at[slot, n]).start()

    def sums(g):
        for lag, fn in ((FOUR, sum_3), (THREE, sum_2), (TWO, sum_1)):

            @pl.when(both(g >= lag, g < LAST + lag))
            def _(lag=lag, fn=fn):
                fn(g - lag)

    def first_sent(g):
        for n in KINDS:

            @pl.when(has(g, n))
            def _(n=n):
                first(odd(g), n).wait_send()

    def slots_free(g):
        @pl.when(g >= TWO)
        def _():
            pl.semaphore_wait(k.credit, 1)

    def layers(AT, DA, WG, WU, WD, stb, DGU, AB, DHB, ws, si, sj, sa, hs, ns, ts):
        TS, TILES, QS = z.TS, FOUR * NB, THREE * NB

        def fetch(i):
            l, n, e = 1 - lax.div(i, TILES), lax.rem(i, TILES), odd(i)
            rows, cols = rows_of(lax.rem(n, FOUR) * TM, TM), cols_of(lax.div(n, FOUR) * FC, FC)
            copy(k.SS.at[l, rows, cols], stb.at[0, e], si.at[e]).start()
            copy(k.TT.at[l, rows, cols], stb.at[1, e], sj.at[e]).start()

        def fetch_act(i):
            l, q, e = 1 - lax.div(i, QS), lax.rem(i, NB), lax.rem(i, THREE)
            theirs, own = lax.rem(TWO * (1 - v) + q, FOUR), lax.rem(TWO * (1 - u) + q, FOUR)
            j = jnp.where(q < FOUR, TWO * place(1 - c, theirs) + 1 - c, TWO * place(c, own) + c)
            copy(k.ACT.at[l, :, cols_of(j * FC, FC)], AB.at[e], sa.at[e]).start()

        def fetch_rows(l, b, size):
            copy(k.DHTH.at[l, rows_of(b * DR, size), :], DHB.at[pl.ds(0, size), :], hs.at[0]).start()

        def fetch_turned(l):
            copy(k.ATH.at[l], AT, hs.at[1]).start()

        fetch_rows(1, 0, DR)
        fetch(jnp.int32(0))
        for n in KINDS:
            fetch_act(jnp.int32(n))
        fetch_turned(1)
        done(k.DH, k.lsem.at[0])

        def layer(it):
            l = 1 - it

            @pl.when(it == 1)
            def _():
                load_d(l, jnp.int32(0), WD, ws.at[TWO])

            load_gu(l, jnp.int32(0), WG, WU, ws)

            @pl.loop(0, FOUR)
            def _(m):
                DA[rows_of(m * TM, TM), :] = jnp.zeros((TM, z.D), F32)

            def product(i, size, keep):
                e = lax.rem(i, THREE)
                with jax.named_scope("act_wait"):
                    done(AB.at[e], sa.at[e])
                keep(nn(DHB[0:size, :], AB[e]))

                @pl.when(i + THREE < TWO * QS)
                def _():
                    fetch_act(i + THREE)

            def down_step(b, g, kinds):
                slot, i, size = odd(g), (THREE * it + b) * NB, len(kinds) * RB
                with jax.named_scope("rows_wait"):
                    done(DHB.at[pl.ds(0, size), :], hs.at[0])
                with jax.named_scope("d_theirs"):

                    @pl.loop(0, FOUR)
                    def _(e):
                        @pl.when(e >= TWO)
                        def _():
                            block(slot, e - TWO, size).wait_send()

                        def keep(val):
                            k.SP[rows_of(odd(e) * DR, size), :] = val.astype(BF)

                        product(i + e, size, keep)
                        block(slot, e, size).start()

                        @pl.when(both(g == 0, odd(e) == 1))
                        def _():
                            with jax.named_scope("late"):
                                late(lax.div(e, TWO))

                with jax.named_scope("sums"):
                    sums(g)
                first_sent(g - TWO)
                with jax.named_scope("d_ours"):

                    @pl.loop(0, TWO)
                    def _(e):
                        block(slot, e, size).wait_recv()

                        def keep(val):
                            val = (val + k.LP[slot, rows_of(e * DR, size), :].astype(F32)).astype(BF)
                            for at, n in enumerate(kinds):
                                k.S1[slot, n, rows_of(e * RB, RB), :] = val[at * RB : (at + 1) * RB]

                        product(i + e + FOUR, size, keep)

                with jax.named_scope("slots"):
                    slots_free(g)
                for n in kinds:
                    first(slot, n).start()

                @pl.when(g == 0)
                def _():
                    all_there()
                    load_d(l, jnp.int32(0), WD, ws.at[TWO])

                with jax.named_scope("d_keep"):

                    @pl.loop(0, TWO)
                    def _(e):
                        block(slot, e + TWO, size).wait_recv()

                        def keep(val):
                            val = val + k.LP[slot, rows_of((e + TWO) * DR, size), :].astype(F32)
                            for at, n in enumerate(kinds):
                                k.K1[slot, n, rows_of(e * RB, RB), :] = val[at * RB : (at + 1) * RB]

                        product(i + e + FOUR + TWO, size, keep)

                for e in range(TWO):
                    block(slot, e, size).wait_send()

                @pl.when(b == 0)
                def _():
                    fetch_rows(l, 1, DR)

                @pl.when(b == 1)
                def _():
                    fetch_rows(l, TWO, TWO * RB)

            def add_da(rows):
                DA[rows, :] += nt(DGU[0, rows, :], WG[...]) + nt(DGU[1, rows, :], WU[...])

            def weights_there():
                done(WG, ws.at[0])
                done(WU, ws.at[1])

            def gate_up_step(j, g):
                slot = odd(g)
                with jax.named_scope("wd_wait"):
                    done(WD, ws.at[TWO])

                def tiles(before):
                    @pl.loop(0, FOUR)
                    def _(m):
                        i = it * TILES + j * FOUR + m
                        e = odd(i)
                        rows = rows_of(m * TM, TM)

                        @pl.when(i + 1 < TWO * TILES)
                        def _():
                            fetch(i + 1)

                        with jax.named_scope("st_wait"):
                            done(stb.at[0, e], si.at[e])
                            done(stb.at[1, e], sj.at[e])
                        with jax.named_scope("a_dot"):
                            before(rows)
                            dact = nt(k.DH[rows, :], WD[...]).astype(BF).astype(F32)
                            DGU[0, rows, :] = (dact * stb[1, e]).astype(BF)
                            DGU[1, rows, :] = (dact * stb[0, e]).astype(BF)

                @pl.when(j == 0)
                def _():
                    tiles(lambda rows: None)

                @pl.when(j > 0)
                def _():
                    with jax.named_scope("w_wait"):
                        weights_there()
                    tiles(add_da)
                    load_gu(l, j, WG, WU, ws)

                @pl.when(j + 1 < NB)
                def _():
                    load_d(l, j + 1, WD, ws.at[TWO])

                @pl.when(j == 0)
                def _():
                    with jax.named_scope("at_wait"):
                        done(AT, hs.at[1])

                with jax.named_scope("b_dot"):
                    for n in range(TWO):
                        k.SP[n * HB : (n + 1) * HB, :] = nn(AT[rows_of((1 - c) * HB, HB), :], DGU[n]).astype(BF)
                        halves(slot, n).start()
                with jax.named_scope("sums"):
                    sums(g)
                first_sent(g - TWO)
                out, keep = TWO * (1 - u) * RB, TWO * u * RB
                for n in range(TWO):
                    with jax.named_scope("half_wait"):
                        halves(slot, n).wait_recv()
                    with jax.named_scope("c_dot"):
                        k.S1[slot, n] = (
                            nn(AT[rows_of(c * HB + out, PR), :], DGU[n]) + k.LP[slot, rows_of(n * HB + out, PR), :].astype(F32)
                        ).astype(BF)
                        k.K1[slot, n] = nn(AT[rows_of(c * HB + keep, PR), :], DGU[n]) + k.LP[
                            slot, rows_of(n * HB + keep, PR), :
                        ].astype(F32)
                    if n == 0:
                        with jax.named_scope("slots"):
                            slots_free(g)
                    first(slot, n).start()
                for n in range(TWO):
                    halves(slot, n).wait_send()

            @pl.loop(0, STEPS)
            def _(q):
                g = it * STEPS + q
                _, b, t = block_of(g)

                @pl.when(both(t == 0, b < TWO))
                def _():
                    down_step(b, g, (0, 1, TWO))

                @pl.when(both(t == 0, b == TWO))
                def _():
                    down_step(b, g, (1, TWO))

                @pl.when(t > 0)
                def _():
                    gate_up_step(TWO * b + t - 1, g)

            def fetch_states(m):
                rows, to = rows_of(m * TS, TS), WD.at[rows_of(odd(m) * TS, TS), :]

                @pl.when(l == 1)
                def _():
                    copy(k.H1.at[rows, :], to, ns.at[odd(m)]).start()

                @pl.when(l == 0)
                def _():
                    copy(k.x.at[0, rows, :], to, ns.at[odd(m)]).start()

            def there(m):
                done(WD.at[rows_of(odd(m) * TS, TS), :], ns.at[odd(m)])

            def norm(m):
                size = TS // NB
                for n in range(NB):
                    rows = rows_of(m * TS + n * size, size)
                    wide = WD[rows_of(odd(m) * TS + n * size, size), :].astype(F32)
                    da = DA[rows, :].astype(BF).astype(F32)
                    scale = lax.rsqrt(jnp.mean(wide * wide, -1, keepdims=True) + 1e-6)
                    along = jnp.mean(da * wide, -1, keepdims=True)
                    dn = (da * scale - wide * (along * scale * scale * scale)).astype(BF)
                    k.DH[rows, :] = (k.DH[rows, :].astype(F32) + dn.astype(F32)).astype(BF)

            def turned(m):
                return k.SP.at[:, cols_of(odd(m) * TS, TS)]

            def hand_on(m):
                rows, cols = rows_of(m * TS, TS), cols_of(m * TS, TS)

                @pl.when(l == 1)
                def _():
                    @pl.when(m >= TWO)
                    def _():
                        done(turned(m), ts.at[odd(m)])

                    k.SP[:, cols_of(odd(m) * TS, TS)] = k.DH[rows, :].T
                    copy(turned(m), k.DHTH.at[0, :, cols], ts.at[odd(m)]).start()

                @pl.when(l == 0)
                def _():
                    copy(k.DH.at[rows, :], k.dx.at[0, rows, :], ts.at[TWO]).start()

            def back(n):
                return AT.at[pl.ds(n * z.FB, z.FB), pl.ds(0, z.D)]

            def turn_back():
                for n in range(TWO):
                    done(AB.at[n, pl.ds(0, z.D), :], sa.at[n])
                    AT[n * z.FB : (n + 1) * z.FB, 0 : z.D] = AB[n, 0 : z.D, :].T
                    copy(back(n), k.dwd.at[n], hs.at[n]).start()

            fetch_states(jnp.int32(0))

            @pl.when(it == 0)
            def _():
                fetch_turned(0)

            with jax.named_scope("norm"):
                weights_there()
                add_da(rows_of(0, TS))

                @pl.loop(1, NB)
                def _(m):
                    @pl.when(both(l == 0, m == 1))
                    def _():
                        gather_end()

                    @pl.when(both(l == 0, m == FOUR))
                    def _():
                        with jax.named_scope("turn_back"):
                            turn_back()

                    @pl.when(both(l == 0, lax.rem(m, THREE) == 1))
                    def _():
                        with jax.named_scope("norm_sums"):
                            sums(LAST + lax.div(m, THREE))

                    @pl.when(both(l == 0, m == 1))
                    def _():
                        for n in range(TWO):
                            copy(k.dwdt.at[n], AB.at[n, pl.ds(0, z.D), :], sa.at[n]).start()

                    fetch_states(m)
                    there(m - 1)
                    with jax.named_scope("norm_dot"):
                        norm(m - 1)
                        add_da(rows_of(m * TS, TS))
                    hand_on(m - 1)

                there(jnp.int32(NB - 1))
                norm(jnp.int32(NB - 1))
                hand_on(jnp.int32(NB - 1))

            @pl.when(l == 1)
            def _():
                for m in range(TWO):
                    done(turned(m), ts.at[m])
                fetch_rows(0, 0, DR)

            @pl.when(l == 0)
            def _():
                done(k.DH, ts.at[TWO])
                for n in range(TWO):
                    done(back(n), hs.at[n])

        @pl.loop(0, TWO)
        def _(it):
            layer(it)

    weights = [vmem(z.D, FC)] * TWO + [vmem(z.FB, z.D)]
    tiles = [vmem(TWO, TWO, TM, FC, dtype=F32), vmem(TWO, z.T, FC), vmem(THREE, z.T, FC), vmem(DR, z.T)]
    pl.run_scoped(
        layers, vmem(z.D, z.T), vmem(z.T, z.D, dtype=F32), *weights, *tiles, *[dmas(THREE)] * FOUR, *[dmas(TWO)] * TWO, dmas(THREE)
    )

    with jax.named_scope("tail"):
        sums(jnp.int32(LAST + THREE))
    for g in (LAST - TWO, LAST - 1):
        first_sent(jnp.int32(g))
        for n in range(TWO):
            second(g % TWO, n).wait_send()
            done(k.S3.at[g % TWO, n], k.osem.at[g % TWO, n])
    pl.semaphore_wait(k.credit, TWO)


class Refs:
    def __init__(self, names, refs):
        for name, ref in zip(names, refs, strict=True):
            setattr(self, name, ref)


def call(name, z, fn, number, ins, outs, scratch, flops):
    names = [*ins, *outs, *scratch]

    def kernel(*refs):
        me, k = Here(), Refs(names, refs)
        me.meet()
        fn(z, me, k)

    hbm = pl.BlockSpec(memory_space=pl.ANY)
    made = pl.pallas_call(
        kernel,
        out_shape=[jax.ShapeDtypeStruct(*spec) for spec in outs.values()],
        in_specs=[hbm] * len(ins),
        out_specs=[hbm] * len(outs),
        scratch_shapes=list(scratch.values()),
        compiler_params=pltpu.CompilerParams(collective_id=number, has_side_effects=True, vmem_limit_bytes=67043328),
        cost_estimate=pl.CostEstimate(flops=flops, bytes_accessed=1 << 28, transcendentals=0),
        name=name,
    )(*ins.values())
    return dict(zip(outs, made, strict=True))


def solution(mesh):
    def step(x, dy, wg, wu, wd):
        _, T, D = x.shape
        F = wg.shape[TWO]
        z = Sizes(T, D, F)
        RB, FB, FC, L = z.RB, z.FB, z.FC, TWO
        ins = {"x": x, "dy": dy, "wg": wg, "wu": wu, "wd": wd}
        kept = {
            **{name: ((L, D, F), BF) for name in ("GG", "GU")},
            "GD": ((L, F, D), BF),
            **{name: ((L, T, F), F32) for name in ("SS", "TT")},
            "ACT": ((L, T, F), BF),
            "H1": ((T, D), BF),
            "ATH": ((L, D, T), BF),
            "DHTH": ((L, D, T), BF),
            "dwdt": ((L, D, FB), BF),
        }
        results = {
            "dx": ((1, T, D), BF),
            **{name: ((L, RB, F), BF) for name in ("dwg", "dwu")},
            "dwd": ((L, FB, D), BF),
        }
        gather = {name: dmas(z.UNITS) for name in ("gsx", "gsy", "gsz", "gsp", "grx", "gry", "grz", "grp")}
        item, pair = (TWO, THREE, RB, FC), (TWO, THREE, z.PR, FC)
        sums = {
            "DH": vmem(T, D),
            "SP": vmem(TWO * z.HB, FC),
            "LP": vmem(TWO, THREE * z.HB, FC),
            **{name: vmem(*pair) for name in ("S1", "L1")},
            "K1": vmem(*pair, dtype=F32),
            **{name: vmem(*item) for name in ("S2", "L2", "S3", "L3")},
            "K2": vmem(*item, dtype=F32),
            "d2ds": dmas(TWO),
            "d2dr": dmas(TWO, TWO),
            "b2ds": dmas(TWO),
            "b2dr": dmas(TWO, FOUR),
            **{name: dmas(TWO, THREE) for name in ("s1s", "s1r", "s2s", "s2r", "s3s", "s3r", "osem")},
            "credit": pltpu.SemaphoreType.REGULAR,
            "lsem": dmas(1),
        }
        flops = TWO * T * D * F

        def whole(z, me, k):
            backward(z, me, k, *forward(z, me, k))

        made = call("whole", z, whole, 0, ins, {**results, **kept}, {**gather, **sums}, flops * (STEPS + FOUR + TWO))
        return made["dx"], made["dwg"], made["dwu"], made["dwd"]

    states, cut = P(("rep", "r", "s"), None, None), P(None, "s", None)
    return jax.shard_map(
        step,
        mesh=mesh,
        in_specs=(states, states, cut, cut, cut),
        out_specs=(states, *[P("rep", "s", None)] * THREE),
        check_vma=False,
    )
```

```python
import functools

import jax
import jax.numpy as jnp
from jax import lax
from jax.experimental import pallas as pl
from jax.experimental.pallas import tpu as pltpu
from jax.sharding import PartitionSpec as P

MESH = pl.DeviceIdType.MESH
BF, F32 = jnp.bfloat16, jnp.float32
NB = 8
LEAD = 8
LAG = 2
TWO, THREE, FOUR = 2, 3, 4
STEPS = 11
LAST = TWO * STEPS


def nn(a, b):
    return lax.dot_general(a, b, (((1,), (0,)), ((), ())), preferred_element_type=F32)


def nt(a, b):
    return lax.dot_general(a, b, (((1,), (1,)), ((), ())), preferred_element_type=F32)


def rows_of(start, size):
    return pl.ds(start if isinstance(start, int) else pl.multiple_of(start, 16), size)


def cols_of(start, size):
    return pl.ds(start if isinstance(start, int) else pl.multiple_of(start, 128), size)


def odd(i):
    return lax.rem(i, TWO)


def copy(src, dst, sem):
    return pltpu.make_async_copy(src, dst, sem)


def done(ref, sem):
    pltpu.make_async_copy(ref, ref, sem).wait()


def both(a, b):
    return jnp.logical_and(a, b)


def either(a, b):
    return jnp.logical_or(a, b)


def vmem(*shape, dtype=BF):
    return pltpu.VMEM(shape, dtype)


def dmas(*shape):
    return pltpu.SemaphoreType.DMA(shape)


class Sizes:
    def __init__(self, T, D, F):
        self.T, self.D, self.F = T, D, F
        self.RB, self.FB, self.HB = D // NB, F // NB, D // TWO
        self.FC = self.FB
        self.UC, self.UD = self.FC // TWO, self.FB // NB
        self.NG, self.ND = F // self.UC, NB
        self.TM, self.TS = T // FOUR, T // NB
        self.PR = TWO * self.RB
        self.UNITS = TWO * (self.NG + self.ND)


class Here:
    def __init__(self):
        self.r, self.s = lax.axis_index("r"), lax.axis_index("s")
        rep, r, s = lax.axis_index("rep"), self.r, self.s
        self.c = c = odd(s)
        y, x = odd(lax.div(s, TWO)), lax.div(s, FOUR)
        self.x, self.y = x, y
        self.xn, self.yn, partner = s + FOUR - NB * x, s + TWO - FOUR * y, s + 1 - TWO * c
        self.partner = partner
        self.far = self.xn + self.yn - s
        self.over = self.yn + c * (self.xn - self.yn)
        self.u, self.v = x + c * (y - x), y + c * (x - y)
        n1 = self.xn + c * (self.yn - self.xn)
        n2 = self.xn + self.yn - n1
        self.to_p, self.to_x, self.to_y, self.to_z = (rep, r, partner), (rep, r, self.xn), (rep, r, self.yn), (rep, 1 - r, s)
        self.to_1, self.to_2 = (rep, r, n1), (rep, r, n2)
        self.z0, self.z1, self.c0, self.c1 = r == 0, r == 1, c == 0, c == 1

    def meet(self):
        barrier = pltpu.get_barrier_semaphore()
        for dev in (self.to_p, self.to_x, self.to_y, self.to_z):
            pl.semaphore_signal(barrier, inc=1, device_id=dev, device_id_type=MESH)
        pl.semaphore_wait(barrier, FOUR)


def remote(src, dst, ss, rs, dev):
    return pltpu.make_async_remote_copy(src, dst, ss, rs, device_id=dev, device_id_type=MESH)


def normed(h):
    wide = h.astype(F32)
    scale = lax.rsqrt(jnp.mean(wide * wide, -1, keepdims=True) + 1e-6)
    return (wide * scale).astype(BF)


def gather_of(z, me, k):
    segments = (
        (0, z.NG, "gu", 0),
        (z.NG, z.ND, "d", 0),
        (z.NG + z.ND, z.NG, "gu", 1),
        (z.UNITS - z.ND, z.ND, "d", 1),
    )

    def held(kind, l, n, d):
        if kind == "gu":
            return [k.GU.at[:, l, rows_of(d * z.RB, z.RB), cols_of(n * z.UC, z.UC)]]
        return [k.GD.at[l, rows_of(d * z.FB + n * z.UD, z.UD), :]]

    def mine(kind, l, n):
        if kind == "gu":
            return [w.at[l, :, cols_of(n * z.UC, z.UC)] for w in (k.wg, k.wu)]
        return [k.wd.at[l, rows_of(n * z.UD, z.UD), :]]

    def got(kind, l, n, sem):
        done(k.GU.at[:, l, pl.ds(0, n * z.RB), pl.ds(0, z.UC)] if kind == "gu" else k.GD.at[l, pl.ds(0, n * z.UD), :], sem)

    def push(srcs, dsts, ss, rs, i, dev):
        for a, b in zip(srcs, dsts, strict=True):
            remote(a, b, ss.at[i], rs.at[i], dev).start()

    def pass_on(ref, i):
        push(ref, ref, k.gsp, k.grp, i, me.to_p)

    def stage_own(kind, l, n, i):
        own, there = mine(kind, l, n), held(kind, l, n, me.s)
        there = [there[0].at[w] for w in range(TWO)] if kind == "gu" else there

        @pl.when(either(me.z0, me.c0))
        def _():
            push(own, there, k.gsx, k.grx, i, me.to_x)

        @pl.when(either(me.z0, me.c1))
        def _():
            push(own, there, k.gsy, k.gry, i, me.to_y)

        push(own, there, k.gsp, k.grp, i, me.to_p)

    def stage_1(kind, l, n, i):
        hx, hy = held(kind, l, n, me.xn), held(kind, l, n, me.yn)

        @pl.when(either(me.z0, me.c0))
        def _():
            got(kind, l, 1, k.grx.at[i])

        @pl.when(either(me.z0, me.c1))
        def _():
            got(kind, l, 1, k.gry.at[i])

        @pl.when(me.z0)
        def _():
            on = held(kind, l, n, me.over)
            push(on, on, k.gsz, k.grz, i, me.to_z)
            pass_on(hx, i)
            pass_on(hy, i)

        @pl.when(both(me.z1, me.c0))
        def _():
            push(hx, hx, k.gsy, k.gry, i, me.to_y)
            pass_on(hx, i)

        @pl.when(both(me.z1, me.c1))
        def _():
            push(hy, hy, k.gsx, k.grx, i, me.to_x)
            pass_on(hy, i)

    def stage_2(kind, l, n, i):
        @pl.when(me.z1)
        def _():
            far, over = held(kind, l, n, me.far), held(kind, l, n, me.over)

            @pl.when(me.c0)
            def _():
                got(kind, l, 1, k.gry.at[i])

            @pl.when(me.c1)
            def _():
                got(kind, l, 1, k.grx.at[i])

            push(far, far, k.gsz, k.grz, i, me.to_z)
            pass_on(far, i)
            got(kind, l, 1, k.grz.at[i])
            pass_on(over, i)

    def stage_3(kind, l, n, i):
        @pl.when(me.z0)
        def _():
            got(kind, l, 1, k.grz.at[i])
            pass_on(held(kind, l, n, me.far), i)

    def stage(fn, i, low, high):
        for start, n, kind, l in segments:
            a, b = max(start, low), min(start + n, high)
            if a < b:

                @pl.when(both(i >= a, i < b))
                def _(kind=kind, l=l, start=start):
                    fn(kind, l, i - start, i)

    def tick(t, low, high, most=NB):
        t = jnp.asarray(t, jnp.int32)
        stage(stage_own, t + LEAD, low + LEAD, high + LEAD)
        for lag, fn in ((TWO * LAG, stage_3), (LAG, stage_2), (0, stage_1)):
            if lag < most:
                stage(fn, t - lag, max(0, low - lag), min(z.UNITS, high - lag))

    def ready(l, kind, n):
        start = next(a for a, _, kd, ll in segments if kd == kind and ll == l)
        got(kind, l, FOUR, k.grp.at[start + n])

    def begin():
        @pl.loop(0, LEAD)
        def _(i):
            stage(stage_own, i, 0, LEAD)

    def end():
        for start, n, kind, l in segments:

            @pl.loop(0, n)
            def _(i, start=start, kind=kind, l=l):
                for sem in (k.gsx, k.gsy, k.gsz):
                    got(kind, l, 1, sem.at[start + i])
                got(kind, l, FOUR, k.gsp.at[start + i])

    return tick, ready, begin, end, stage, stage_3


def loads_of(z, me, k):
    def load_gu(l, j, WG, WU, sems):
        cols = cols_of(j * z.FC, z.FC)
        others = ((FOUR * (1 - me.x), FOUR), (FOUR * me.x + TWO * (1 - me.y), TWO), (me.partner, 1))
        for n, (W, own, G) in enumerate(((WG, k.wg, k.GU.at[0]), (WU, k.wu, k.GU.at[1]))):
            copy(own.at[l, :, cols], W.at[rows_of(me.s * z.RB, z.RB), :], sems.at[n]).start()
            for d, size in others:
                rows = rows_of(d * z.RB, size * z.RB)
                copy(G.at[l, rows, cols], W.at[rows, :], sems.at[n]).start()

    def load_d(l, j, W, sem):
        @pl.when(j == me.s)
        def _():
            copy(k.wd.at[l], W, sem).start()

        @pl.when(j != me.s)
        def _():
            copy(k.GD.at[l, rows_of(j * z.FB, z.FB), :], W, sem).start()

    return load_gu, load_d


def forward(z, me, k):
    tick, ready, gather_begin, gather_end, stage, stage_3 = gather_of(z, me, k)
    load_gu, load_d = loads_of(z, me, k)
    NS, U1 = NB, z.NG + z.ND

    def put_turned(ref, a):
        turned = a.T
        for d in range(NB):
            core, px, py = d % TWO, d // FOUR, (d // TWO) % TWO
            i = TWO * px + py if core == 0 else TWO * py + px
            ref[core * z.HB + i * z.RB : core * z.HB + (i + 1) * z.RB, :] = turned[d * z.RB : (d + 1) * z.RB, :]

    def turn(A):
        def body(xb, yb, ab, bb, si, sj, so, sp):
            def fetch(m, e):
                rows = rows_of(m * z.TS, z.TS)
                copy(k.x.at[0, rows, :], xb.at[e], si.at[e]).start()
                copy(k.dy.at[0, rows, :], yb.at[e], sj.at[e]).start()

            fetch(0, 0)

            def sent(e):
                done(ab.at[e], so.at[e])
                done(bb.at[e], sp.at[e])

            @pl.loop(0, NS)
            def _(m):
                e = odd(m)
                cols = cols_of(m * z.TS, z.TS)

                @pl.when(m + 1 < NS)
                def _():
                    fetch(m + 1, 1 - e)

                done(xb.at[e], si.at[e])
                done(yb.at[e], sj.at[e])
                a = normed(xb[e])
                A[rows_of(m * z.TS, z.TS), :] = a

                @pl.when(m >= TWO)
                def _():
                    sent(e)

                put_turned(ab.at[e], a)
                bb[e] = yb[e].T
                copy(ab.at[e], k.ATH.at[0, :, cols], so.at[e]).start()
                copy(bb.at[e], k.DHTH.at[1, :, cols], sp.at[e]).start()

                @pl.when(e == 1)
                def _():
                    tick(lax.div(m, TWO), 0, FOUR)

            sent(0)
            sent(1)

        blocks = [vmem(TWO, z.TS, z.D)] * TWO + [vmem(TWO, z.D, z.TS)] * TWO
        pl.run_scoped(body, *blocks, *[dmas(TWO)] * FOUR)

    def gate_up(l, A, hook):
        def body(WG, WU, sb, tb, ab, ws, *so):
            kept = ((sb, k.SS), (tb, k.TT), (ab, k.ACT))

            def sent(e):
                for (b, _), sem in zip(kept, so, strict=True):
                    done(b.at[e], sem.at[e])

            def fetch(j, e):
                ready(l, "gu", TWO * j)
                ready(l, "gu", TWO * j + 1)
                load_gu(l, j, WG.at[e], WU.at[e], ws.at[e])

            fetch(0, 0)
            hook(-1, 0)

            @pl.loop(0, NB)
            def _(j):
                slot = odd(j)
                cols = cols_of(j * z.FC, z.FC)
                with jax.named_scope("gu_wait"):
                    done(WG.at[slot], ws.at[slot, 0])
                    done(WU.at[slot], ws.at[slot, 1])

                @pl.loop(0, TWO)
                def _(m):
                    with jax.named_scope("gu_sent"):

                        @pl.when(j > 0)
                        def _():
                            for e in range(TWO):
                                sent(TWO * m + e)

                    with jax.named_scope("gu_dot"):
                        for e in range(TWO):
                            at = TWO * m + e
                            a = A[rows_of(at * z.TM, z.TM), :]
                            gate = nn(a, WG[slot])
                            up = nn(a, WU[slot])
                            sig = lax.logistic(gate)
                            sl = gate * sig
                            sb[at] = sl
                            tb[at] = up * (sig + sl * (1.0 - sig))
                            ab[at] = (sl * up).astype(BF)
                    for e in range(TWO):
                        at = TWO * m + e
                        for (b, to), sem in zip(kept, so, strict=True):
                            copy(b.at[at], to.at[l, rows_of(at * z.TM, z.TM), cols], sem.at[at]).start()

                    with jax.named_scope("gu_tick"):
                        hook(j, m)

                    @pl.when(both(m == 0, j + 1 < NB))
                    def _():
                        with jax.named_scope("gu_fetch"):
                            fetch(j + 1, 1 - slot)

            for e in range(FOUR):
                sent(e)

        weights = [vmem(TWO, z.D, z.FC)] * TWO
        tiles = [vmem(FOUR, z.TM, z.FC, dtype=F32)] * TWO + [vmem(FOUR, z.TM, z.FC)]
        pl.run_scoped(body, *weights, *tiles, dmas(TWO, TWO), *[dmas(FOUR)] * THREE)

    QC, KP = z.FC // FOUR, TWO * z.FC

    def unit_of_down(n, W, ws):
        ready(0, "d", n)
        p = lax.div(n, TWO)

        @pl.loop(0, NB)
        def _(d):
            to = W.at[rows_of(p * KP + d * QC + odd(n) * z.UD, z.UD), :]

            @pl.when(d == me.s)
            def _():
                copy(k.wd.at[0, rows_of(n * z.UD, z.UD), :], to, ws.at[p]).start()

            @pl.when(d != me.s)
            def _():
                copy(k.GD.at[0, rows_of(d * z.FB + n * z.UD, z.UD), :], to, ws.at[p]).start()

    def down(A, W, ws, hook):
        def body(AC, acc, xb, hb, tb, si, sj, so, sp):
            def fetch_act(i):
                p, rows, e = lax.div(i, FOUR), rows_of(lax.rem(i, FOUR) * z.TM, z.TM), lax.rem(i, THREE)
                for d in range(NB):
                    to = AC.at[e, :, pl.ds(d * QC, QC)]
                    copy(k.ACT.at[0, rows, cols_of(d * z.FC + p * QC, QC)], to, si.at[e]).start()

            def act_there(i):
                with jax.named_scope("dn_act"):
                    done(AC.at[lax.rem(i, THREE)], si.at[lax.rem(i, THREE)])

                @pl.when(i + TWO < FOUR * FOUR)
                def _():
                    fetch_act(i + TWO)

            def fetch(m, e):
                copy(k.x.at[0, rows_of(m * z.TS, z.TS), :], xb.at[e], sj.at[e]).start()

            def there(p):
                with jax.named_scope("dn_load"):
                    done(W.at[rows_of(p * KP, KP), :], ws.at[p])

            def product(p, i, rows, at):
                return acc[rows, :] + nn(AC[lax.rem(i, THREE), at, :], W[rows_of(p * KP, KP), :])

            fetch_act(jnp.int32(0))
            fetch_act(jnp.int32(1))
            fetch(0, 0)

            @pl.loop(0, NS)
            def _(m):
                acc[rows_of(m * z.TS, z.TS), :] = jnp.zeros((z.TS, z.D), F32)

            @pl.loop(0, THREE)
            def _(p):
                there(p)

                @pl.loop(0, FOUR)
                def _(m):
                    rows = rows_of(m * z.TM, z.TM)
                    act_there(FOUR * p + m)
                    with jax.named_scope("dn_dot"):
                        acc[rows, :] = product(p, FOUR * p + m, rows, slice(None))

                    @pl.when(odd(m) == 1)
                    def _():
                        with jax.named_scope("dn_tick"):
                            hook(TWO * p + lax.div(m, TWO))

            there(jnp.int32(THREE))

            def tile_of(m):
                return lax.div(jnp.asarray(m, jnp.int32), TWO) + THREE * FOUR

            def states(m, e):
                rows, at = rows_of(m * z.TS, z.TS), rows_of(m % TWO * z.TS if isinstance(m, int) else odd(m) * z.TS, z.TS)
                low = product(jnp.int32(THREE), tile_of(m), rows, at).astype(BF)
                return (xb[e].astype(F32) + low.astype(F32)).astype(BF)

            def finish(m, e):
                a = normed(hb[e])
                A[rows_of(m * z.TS, z.TS), :] = a
                put_turned(tb.at[e], a)

            def send(m):
                e = m % THREE if isinstance(m, int) else lax.rem(m, THREE)
                copy(hb.at[e], k.H1.at[rows_of(m * z.TS, z.TS), :], so.at[e]).start()
                copy(tb.at[e], k.ATH.at[1, :, cols_of(m * z.TS, z.TS)], sp.at[e]).start()

            def sent(e):
                done(hb.at[e], so.at[e])
                done(tb.at[e], sp.at[e])

            done(xb.at[0], sj.at[0])
            fetch(1, 1)
            act_there(tile_of(0))
            hb[0] = states(0, 0)

            @pl.loop(1, NS)
            def _(m):
                e, now, before = odd(m), lax.rem(m, THREE), lax.rem(m + TWO, THREE)

                @pl.when(m + 1 < NS)
                def _():
                    fetch(m + 1, 1 - e)

                done(xb.at[e], sj.at[e])

                @pl.when(e == 0)
                def _():
                    act_there(tile_of(m))

                @pl.when(m >= THREE)
                def _():
                    sent(now)

                with jax.named_scope("dn_last"):
                    finish(m - 1, before)
                    hb[now] = states(m, e)
                send(m - 1)

                @pl.when(e == 1)
                def _():
                    with jax.named_scope("dn_tick"):
                        hook(TWO * THREE + lax.div(m, TWO))

            last = (NS - 1) % THREE
            finish(NS - 1, last)
            send(NS - 1)
            for e in range(THREE):
                sent(e)

        tiles = [vmem(THREE, z.TM, KP), vmem(z.T, z.D, dtype=F32), vmem(TWO, z.TS, z.D), vmem(THREE, z.TS, z.D), vmem(THREE, z.D, z.TS)]
        pl.run_scoped(body, *tiles, dmas(THREE), dmas(TWO), *[dmas(THREE)] * TWO)

    def run(A):
        gather_begin()
        copy(k.dy.at[0], k.DH, k.lsem.at[0]).start()
        with jax.named_scope("turn"):
            turn(A)
        with jax.named_scope("start"):
            for n in range(TWO):
                stage(stage_3, jnp.int32(n), n, n + 1)
        t1 = TWO * LAG + FOUR
        t2 = t1 + z.NG
        t3 = t2 + NB + TWO

        def first_layer(W, ws):
            def unit(t):
                n = t - (z.NG + TWO * LAG + 1)

                @pl.when(both(n >= 0, n < z.ND))
                def _():
                    unit_of_down(n, W, ws)

            def hook(j, m):
                if isinstance(j, int):
                    for t in range(FOUR, t1 - 1):
                        tick(t, t, t + 1, TWO * LAG if t < t1 - TWO else NB)
                    return

                @pl.when(both(j == 0, m == 0))
                def _():
                    tick(t1 - 1, t1 - 1, t1)

                t = TWO * j + m + t1
                tick(t, t1, t2)
                unit(t)

            gate_up(0, A, hook)

            def in_down(n):
                tick(n + t2, t2, t3)
                unit(n + t2)

            down(A, W, ws, in_down)

        pl.run_scoped(first_layer, vmem(z.F, z.D), dmas(FOUR))

        def hook(j, m):
            if not isinstance(j, int):
                tick(TWO * j + m + t3, t3, t3 + z.NG)

        gate_up(1, A, hook)

    t4 = z.UNITS + TWO * LAG - TWO

    def late(n):
        tick(n + t4, t4, t4 + TWO)

    def all_there():
        for n in range(z.ND):
            ready(1, "d", n)

    pl.run_scoped(run, vmem(z.T, z.D))
    return late, all_there, gather_end


def backward(z, me, k, late, all_there, gather_end):
    load_gu, load_d = loads_of(z, me, k)
    c, u, v = me.c, me.u, me.v
    RB, FC, HB, PR, TM = z.RB, z.FC, z.HB, z.PR, z.TM
    DR = THREE * RB
    KINDS = range(THREE)

    def place(core, i):
        return i + core * (odd(i) * TWO + lax.div(i, TWO) - i)

    def block_of(g):
        q = lax.rem(g, STEPS)
        b = lax.div(q, THREE)
        return 1 - lax.div(g, STEPS), b, q - THREE * b + lax.div(b, THREE)

    def first_row(b):
        return jnp.minimum(THREE * b, NB - THREE)

    def has(g, n):
        _, b, t = block_of(g)
        inside = both(g >= 0, g < LAST)
        if n == 0:
            return both(inside, either(b < TWO, t > 0))
        return inside if n == 1 else both(inside, t == 0)

    def halves(slot, n, part, first_at):
        at = 1 - first_at if part == 0 else first_at
        rows, i = rows_of(n * HB + TWO * at * RB, PR), TWO * n + part
        return remote(k.SP.at[rows, :], k.LP.at[slot, rows, :], k.d2ds.at[i], k.d2dr.at[slot, i], me.to_p)

    def block(slot, e, size):
        there = k.LP.at[slot, rows_of(e * DR, size), :]
        return remote(k.SP.at[rows_of(odd(e) * DR, size), :], there, k.b2ds.at[odd(e)], k.b2dr.at[slot, e], me.to_p)

    def first(slot, n):
        return remote(k.S1.at[slot, n], k.L1.at[slot, n], k.s1s.at[slot, n], k.s1r.at[slot, n], me.to_1)

    def second(slot, n):
        return remote(k.S2.at[slot, n], k.L2.at[slot, n], k.s2s.at[slot, n], k.s2r.at[slot, n], me.to_2)

    def third(slot, n):
        return remote(k.S3.at[slot, n], k.L3.at[slot, n], k.s3s.at[slot, n], k.s3r.at[slot, n], me.to_z)

    def sum_1(g):
        slot = odd(g)
        for n in KINDS:

            @pl.when(has(g - TWO, n))
            def _(n=n):
                second(slot, n).wait_send()

            @pl.when(has(g, n))
            def _(n=n):
                with jax.named_scope("l1"):
                    first(slot, n).wait_recv()
                away, home = rows_of((1 - v) * RB, RB), rows_of(v * RB, RB)
                k.S2[slot, n] = (k.K1[slot, n, away, :] + k.L1[slot, n, away, :].astype(F32)).astype(BF)
                k.K2[slot, n] = k.K1[slot, n, home, :] + k.L1[slot, n, home, :].astype(F32)
                second(slot, n).start()

        pl.semaphore_signal(k.credit, inc=1, device_id=me.to_1, device_id_type=MESH)

    def sum_2(g):
        slot = odd(g)
        for n in KINDS:

            @pl.when(has(g - TWO, n))
            def _(n=n):
                done(k.S3.at[slot, n], k.osem.at[slot, n])

            @pl.when(has(g, n))
            def _(n=n):
                with jax.named_scope("l2"):
                    second(slot, n).wait_recv()
                k.S3[slot, n] = (k.K2[slot, n] + k.L2[slot, n].astype(F32)).astype(BF)
                third(slot, n).start()

    def sum_3(g):
        slot = odd(g)
        l, b, t = block_of(g)
        for n in KINDS:

            @pl.when(has(g, n))
            def _(n=n):
                with jax.named_scope("l3"):
                    third(slot, n).wait()
                k.S3[slot, n] = (k.S3[slot, n].astype(F32) + k.L3[slot, n].astype(F32)).astype(BF)

                @pl.when(t == 0)
                def _():
                    copy(k.S3.at[slot, n], k.dwdt.at[l, rows_of((first_row(b) + n) * RB, RB), :], k.osem.at[slot, n]).start()

                if n < TWO:

                    @pl.when(t > 0)
                    def _():
                        to = (k.dwg, k.dwu)[n].at[l, :, cols_of((TWO * b + t - 1) * FC, FC)]
                        copy(k.S3.at[slot, n], to, k.osem.at[slot, n]).start()

    def sums(g):
        for lag, fn in ((FOUR, sum_3), (THREE, sum_2), (TWO, sum_1)):

            @pl.when(both(g >= lag, g < LAST + lag))
            def _(lag=lag, fn=fn):
                fn(g - lag)

    def first_sent(g):
        for n in KINDS:

            @pl.when(has(g, n))
            def _(n=n):
                first(odd(g), n).wait_send()

    def slots_free(g):
        @pl.when(g >= TWO)
        def _():
            pl.semaphore_wait(k.credit, 1)

    def layers(AT, DA, WG, WU, WD, stb, DGU, AB, DHB, ws, si, sj, sa, hs, ns, ts):
        TS, TILES, QS = z.TS, FOUR * NB, THREE * NB

        def fetch(i):
            l, n, e = 1 - lax.div(i, TILES), lax.rem(i, TILES), odd(i)
            rows, cols = rows_of(lax.rem(n, FOUR) * TM, TM), cols_of(lax.div(n, FOUR) * FC, FC)
            copy(k.SS.at[l, rows, cols], stb.at[0, e], si.at[e]).start()
            copy(k.TT.at[l, rows, cols], stb.at[1, e], sj.at[e]).start()

        def fetch_act(i):
            l, q, e = 1 - lax.div(i, QS), lax.rem(i, NB), lax.rem(i, THREE)
            theirs, own = lax.rem(TWO * (1 - v) + q, FOUR), lax.rem(TWO * (1 - u) + q, FOUR)
            j = jnp.where(q < FOUR, TWO * place(1 - c, theirs) + 1 - c, TWO * place(c, own) + c)
            copy(k.ACT.at[l, :, cols_of(j * FC, FC)], AB.at[e], sa.at[e]).start()

        def fetch_rows(l, b, size):
            copy(k.DHTH.at[l, rows_of(b * DR, size), :], DHB.at[pl.ds(0, size), :], hs.at[0]).start()

        def fetch_turned(l):
            copy(k.ATH.at[l], AT, hs.at[1]).start()

        fetch_rows(1, 0, DR)
        fetch(jnp.int32(0))
        for n in KINDS:
            fetch_act(jnp.int32(n))
        fetch_turned(1)
        done(k.DH, k.lsem.at[0])

        def layer(it):
            l = 1 - it

            @pl.when(it == 1)
            def _():
                load_d(l, jnp.int32(0), WD, ws.at[TWO])

            load_gu(l, jnp.int32(0), WG, WU, ws)

            @pl.loop(0, FOUR)
            def _(m):
                DA[rows_of(m * TM, TM), :] = jnp.zeros((TM, z.D), F32)

            def product(i, size, keep):
                e = lax.rem(i, THREE)
                with jax.named_scope("act_wait"):
                    done(AB.at[e], sa.at[e])
                keep(nn(DHB[0:size, :], AB[e]))

                @pl.when(i + THREE < TWO * QS)
                def _():
                    fetch_act(i + THREE)

            def down_step(b, g, kinds):
                slot, i, size = odd(g), (THREE * it + b) * NB, len(kinds) * RB
                with jax.named_scope("rows_wait"):
                    done(DHB.at[pl.ds(0, size), :], hs.at[0])
                with jax.named_scope("d_theirs"):

                    @pl.loop(0, FOUR)
                    def _(e):
                        @pl.when(e >= TWO)
                        def _():
                            block(slot, e - TWO, size).wait_send()

                        def keep(val):
                            k.SP[rows_of(odd(e) * DR, size), :] = val.astype(BF)

                        product(i + e, size, keep)
                        block(slot, e, size).start()

                        @pl.when(both(g == 0, odd(e) == 1))
                        def _():
                            with jax.named_scope("late"):
                                late(lax.div(e, TWO))

                with jax.named_scope("sums"):
                    sums(g)
                first_sent(g - TWO)
                with jax.named_scope("d_ours"):

                    @pl.loop(0, TWO)
                    def _(e):
                        block(slot, e, size).wait_recv()

                        def keep(val):
                            val = (val + k.LP[slot, rows_of(e * DR, size), :].astype(F32)).astype(BF)
                            for at, n in enumerate(kinds):
                                k.S1[slot, n, rows_of(e * RB, RB), :] = val[at * RB : (at + 1) * RB]

                        product(i + e + FOUR, size, keep)

                with jax.named_scope("slots"):
                    slots_free(g)
                for n in kinds:
                    first(slot, n).start()

                @pl.when(g == 0)
                def _():
                    all_there()
                    load_d(l, jnp.int32(0), WD, ws.at[TWO])

                with jax.named_scope("d_keep"):

                    @pl.loop(0, TWO)
                    def _(e):
                        block(slot, e + TWO, size).wait_recv()

                        def keep(val):
                            val = val + k.LP[slot, rows_of((e + TWO) * DR, size), :].astype(F32)
                            for at, n in enumerate(kinds):
                                k.K1[slot, n, rows_of(e * RB, RB), :] = val[at * RB : (at + 1) * RB]

                        product(i + e + FOUR + TWO, size, keep)

                for e in range(TWO):
                    block(slot, e, size).wait_send()

                @pl.when(b == 0)
                def _():
                    fetch_rows(l, 1, DR)

                @pl.when(b == 1)
                def _():
                    fetch_rows(l, TWO, TWO * RB)

            def add_da(rows):
                DA[rows, :] += nt(DGU[0, rows, :], WG[...]) + nt(DGU[1, rows, :], WU[...])

            def weights_there():
                done(WG, ws.at[0])
                done(WU, ws.at[1])

            def gate_up_step(j, g):
                slot = odd(g)
                with jax.named_scope("wd_wait"):
                    done(WD, ws.at[TWO])

                def tiles(before):
                    @pl.loop(0, FOUR)
                    def _(m):
                        i = it * TILES + j * FOUR + m
                        e = odd(i)
                        rows = rows_of(m * TM, TM)

                        @pl.when(i + 1 < TWO * TILES)
                        def _():
                            fetch(i + 1)

                        with jax.named_scope("st_wait"):
                            done(stb.at[0, e], si.at[e])
                            done(stb.at[1, e], sj.at[e])
                        with jax.named_scope("a_dot"):
                            before(rows)
                            dact = nt(k.DH[rows, :], WD[...]).astype(BF).astype(F32)
                            DGU[0, rows, :] = (dact * stb[1, e]).astype(BF)
                            DGU[1, rows, :] = (dact * stb[0, e]).astype(BF)

                @pl.when(j == 0)
                def _():
                    tiles(lambda rows: None)

                @pl.when(j > 0)
                def _():
                    with jax.named_scope("w_wait"):
                        weights_there()
                    tiles(add_da)
                    load_gu(l, j, WG, WU, ws)

                @pl.when(j + 1 < NB)
                def _():
                    load_d(l, j + 1, WD, ws.at[TWO])

                @pl.when(j == 0)
                def _():
                    with jax.named_scope("at_wait"):
                        done(AT, hs.at[1])

                with jax.named_scope("sums"):
                    sums(g)
                first_sent(g - TWO)
                with jax.named_scope("b_dot"):
                    for n in range(TWO):
                        k.SP[n * HB : (n + 1) * HB, :] = nn(AT[rows_of((1 - c) * HB, HB), :], DGU[n]).astype(BF)
                        for part in range(TWO):
                            halves(slot, n, part, v).start()
                out, keep = TWO * (1 - u) * RB, TWO * u * RB
                for n in range(TWO):
                    with jax.named_scope("half_wait"):
                        halves(slot, n, 0, u).wait_recv()
                    with jax.named_scope("c_dot"):
                        k.S1[slot, n] = (
                            nn(AT[rows_of(c * HB + out, PR), :], DGU[n]) + k.LP[slot, rows_of(n * HB + out, PR), :].astype(F32)
                        ).astype(BF)
                        halves(slot, n, 1, u).wait_recv()
                        k.K1[slot, n] = nn(AT[rows_of(c * HB + keep, PR), :], DGU[n]) + k.LP[
                            slot, rows_of(n * HB + keep, PR), :
                        ].astype(F32)
                    if n == 0:
                        with jax.named_scope("slots"):
                            slots_free(g)
                    first(slot, n).start()
                for n in range(TWO):
                    for part in range(TWO):
                        halves(slot, n, part, v).wait_send()

            @pl.loop(0, STEPS)
            def _(q):
                g = it * STEPS + q
                _, b, t = block_of(g)

                @pl.when(both(t == 0, b < TWO))
                def _():
                    down_step(b, g, (0, 1, TWO))

                @pl.when(both(t == 0, b == TWO))
                def _():
                    down_step(b, g, (1, TWO))

                @pl.when(t > 0)
                def _():
                    gate_up_step(TWO * b + t - 1, g)

            def fetch_states(m):
                rows, to = rows_of(m * TS, TS), WD.at[rows_of(odd(m) * TS, TS), :]

                @pl.when(l == 1)
                def _():
                    copy(k.H1.at[rows, :], to, ns.at[odd(m)]).start()

                @pl.when(l == 0)
                def _():
                    copy(k.x.at[0, rows, :], to, ns.at[odd(m)]).start()

            def there(m):
                done(WD.at[rows_of(odd(m) * TS, TS), :], ns.at[odd(m)])

            def norm(m):
                size = TS // NB
                for n in range(NB):
                    rows = rows_of(m * TS + n * size, size)
                    wide = WD[rows_of(odd(m) * TS + n * size, size), :].astype(F32)
                    da = DA[rows, :].astype(BF).astype(F32)
                    scale = lax.rsqrt(jnp.mean(wide * wide, -1, keepdims=True) + 1e-6)
                    along = jnp.mean(da * wide, -1, keepdims=True)
                    dn = (da * scale - wide * (along * scale * scale * scale)).astype(BF)
                    k.DH[rows, :] = (k.DH[rows, :].astype(F32) + dn.astype(F32)).astype(BF)

            def turned(m):
                return k.SP.at[:, cols_of(odd(m) * TS, TS)]

            def hand_on(m):
                rows, cols = rows_of(m * TS, TS), cols_of(m * TS, TS)

                @pl.when(l == 1)
                def _():
                    @pl.when(m >= TWO)
                    def _():
                        done(turned(m), ts.at[odd(m)])

                    k.SP[:, cols_of(odd(m) * TS, TS)] = k.DH[rows, :].T
                    copy(turned(m), k.DHTH.at[0, :, cols], ts.at[odd(m)]).start()

                @pl.when(l == 0)
                def _():
                    copy(k.DH.at[rows, :], k.dx.at[0, rows, :], ts.at[TWO]).start()

            def back(n):
                return AT.at[pl.ds(n * z.FB, z.FB), pl.ds(0, z.D)]

            def turn_back():
                for n in range(TWO):
                    done(AB.at[n, pl.ds(0, z.D), :], sa.at[n])
                    AT[n * z.FB : (n + 1) * z.FB, 0 : z.D] = AB[n, 0 : z.D, :].T
                    copy(back(n), k.dwd.at[n], hs.at[n]).start()

            fetch_states(jnp.int32(0))

            @pl.when(it == 0)
            def _():
                fetch_turned(0)

            with jax.named_scope("norm"):
                weights_there()
                add_da(rows_of(0, TS))

                @pl.loop(1, NB)
                def _(m):
                    @pl.when(both(l == 0, m == 1))
                    def _():
                        gather_end()

                    @pl.when(both(l == 0, m == FOUR))
                    def _():
                        with jax.named_scope("turn_back"):
                            turn_back()

                    @pl.when(both(l == 0, lax.rem(m, THREE) == 1))
                    def _():
                        with jax.named_scope("norm_sums"):
                            sums(LAST + lax.div(m, THREE))

                    @pl.when(both(l == 0, m == 1))
                    def _():
                        for n in range(TWO):
                            copy(k.dwdt.at[n], AB.at[n, pl.ds(0, z.D), :], sa.at[n]).start()

                    fetch_states(m)
                    there(m - 1)
                    with jax.named_scope("norm_dot"):
                        norm(m - 1)
                        add_da(rows_of(m * TS, TS))
                    hand_on(m - 1)

                there(jnp.int32(NB - 1))
                norm(jnp.int32(NB - 1))
                hand_on(jnp.int32(NB - 1))

            @pl.when(l == 1)
            def _():
                for m in range(TWO):
                    done(turned(m), ts.at[m])
                fetch_rows(0, 0, DR)

            @pl.when(l == 0)
            def _():
                done(k.DH, ts.at[TWO])
                for n in range(TWO):
                    done(back(n), hs.at[n])

        @pl.loop(0, TWO)
        def _(it):
            layer(it)

    weights = [vmem(z.D, FC)] * TWO + [vmem(z.FB, z.D)]
    tiles = [vmem(TWO, TWO, TM, FC, dtype=F32), vmem(TWO, z.T, FC), vmem(THREE, z.T, FC), vmem(DR, z.T)]
    pl.run_scoped(
        layers, vmem(z.D, z.T), vmem(z.T, z.D, dtype=F32), *weights, *tiles, *[dmas(THREE)] * FOUR, *[dmas(TWO)] * TWO, dmas(THREE)
    )

    with jax.named_scope("tail"):
        sums(jnp.int32(LAST + THREE))
    for g in (LAST - TWO, LAST - 1):
        first_sent(jnp.int32(g))
        for n in range(TWO):
            second(g % TWO, n).wait_send()
            done(k.S3.at[g % TWO, n], k.osem.at[g % TWO, n])
    pl.semaphore_wait(k.credit, TWO)


class Refs:
    def __init__(self, names, refs):
        for name, ref in zip(names, refs, strict=True):
            setattr(self, name, ref)


def call(name, z, fn, number, ins, outs, scratch, flops):
    names = [*ins, *outs, *scratch]

    def kernel(*refs):
        me, k = Here(), Refs(names, refs)
        me.meet()
        fn(z, me, k)

    hbm = pl.BlockSpec(memory_space=pl.ANY)
    made = pl.pallas_call(
        kernel,
        out_shape=[jax.ShapeDtypeStruct(*spec) for spec in outs.values()],
        in_specs=[hbm] * len(ins),
        out_specs=[hbm] * len(outs),
        scratch_shapes=list(scratch.values()),
        compiler_params=pltpu.CompilerParams(collective_id=number, has_side_effects=True, vmem_limit_bytes=67043328),
        cost_estimate=pl.CostEstimate(flops=flops, bytes_accessed=1 << 28, transcendentals=0),
        name=name,
    )(*ins.values())
    return dict(zip(outs, made, strict=True))


def solution(mesh):
    def step(x, dy, wg, wu, wd):
        _, T, D = x.shape
        F = wg.shape[TWO]
        z = Sizes(T, D, F)
        RB, FB, FC, L = z.RB, z.FB, z.FC, TWO
        ins = {"x": x, "dy": dy, "wg": wg, "wu": wu, "wd": wd}
        kept = {
            "GU": ((TWO, L, D, F), BF),
            "GD": ((L, F, D), BF),
            **{name: ((L, T, F), F32) for name in ("SS", "TT")},
            "ACT": ((L, T, F), BF),
            "H1": ((T, D), BF),
            "ATH": ((L, D, T), BF),
            "DHTH": ((L, D, T), BF),
            "dwdt": ((L, D, FB), BF),
        }
        results = {
            "dx": ((1, T, D), BF),
            **{name: ((L, RB, F), BF) for name in ("dwg", "dwu")},
            "dwd": ((L, FB, D), BF),
        }
        gather = {name: dmas(z.UNITS) for name in ("gsx", "gsy", "gsz", "gsp", "grx", "gry", "grz", "grp")}
        item, pair = (TWO, THREE, RB, FC), (TWO, THREE, z.PR, FC)
        sums = {
            "DH": vmem(T, D),
            "SP": vmem(TWO * z.HB, FC),
            "LP": vmem(TWO, THREE * z.HB, FC),
            **{name: vmem(*pair) for name in ("S1", "L1")},
            "K1": vmem(*pair, dtype=F32),
            **{name: vmem(*item) for name in ("S2", "L2", "S3", "L3")},
            "K2": vmem(*item, dtype=F32),
            "d2ds": dmas(FOUR),
            "d2dr": dmas(TWO, FOUR),
            "b2ds": dmas(TWO),
            "b2dr": dmas(TWO, FOUR),
            **{name: dmas(TWO, THREE) for name in ("s1s", "s1r", "s2s", "s2r", "s3s", "s3r", "osem")},
            "credit": pltpu.SemaphoreType.REGULAR,
            "lsem": dmas(1),
        }
        flops = TWO * T * D * F

        def whole(z, me, k):
            backward(z, me, k, *forward(z, me, k))

        made = call("whole", z, whole, 0, ins, {**results, **kept}, {**gather, **sums}, flops * (STEPS + FOUR + TWO))
        return made["dx"], made["dwg"], made["dwu"], made["dwd"]

    states, cut = P(("rep", "r", "s"), None, None), P(None, "s", None)
    return jax.shard_map(
        step,
        mesh=mesh,
        in_specs=(states, states, cut, cut, cut),
        out_specs=(states, *[P("rep", "s", None)] * THREE),
        check_vma=False,
    )
```
